32 devices in a mesh: dp: 1 (over z), tp: 4 (over y), sp: 8 (over x, core).
Axes of the slice: x: 4, y: 4, z: 1, core: 2. Of those that a mesh axis runs over, the one named last changes fastest.
The devices are a block of a 4x4x8 slice.
Arguments:
- tokens: bfloat16 [32, 2048], P(('dp', 'sp'))
- states: float32 [8, 32, 32, 64, 64], P('sp', 'dp', 'tp')
- k_cache: bfloat16 [32, 8, 8192, 64], P('dp', 'tp', 'sp')
- v_cache: bfloat16 [32, 8, 8192, 64], P('dp', 'tp', 'sp')
- slopes: float32 [32], P('tp')
- lin_gain: float32 [2048], replicated
- w_lin_qkv: bfloat16 [2048, 3, 2048], P(None, None, 'tp')
- w_lin_gate: bfloat16 [2048, 2048], P(None, 'tp')
- out_gain: float32 [2048], P('tp')
- w_lin_out: bfloat16 [2048, 2048], P('tp')
- attn_gain: float32 [2048], replicated
- w_attn_in: bfloat16 [2048, 8, 6, 64], P(None, 'tp')
- w_attn_out: bfloat16 [2048, 2048], P('tp')
Outputs:
- output 1: bfloat16 [32, 2048], P(('dp', 'sp'))
- output 2: float32 [32, 32, 64, 64], P(('dp', 'sp'), 'tp')
- output 3: bfloat16 [32, 8, 8208, 64], P(('dp', 'sp'), 'tp')
- output 4: bfloat16 [32, 8, 8208, 64], P(('dp', 'sp'), 'tp')
All inputs are finite; a program needn't handle non-finite values.
Results may differ from the reference program's by a relative error of at most 0.0127504.
Values are sent between devices in bfloat16 or wider.
A program may use at most 768 MiB of HBM per device.

```python
import jax
import jax.numpy as jnp
from jax import lax

MODEL_DIM = 2048
NUM_HEADS = 32
KV_COUNT = 8
HEAD_DIM = 64
SEQ_SHARDS = 8
BATCH = 32
SHARD_LEN = 1024
CACHE_EXTRA = 16

PROMPT_LEN = SEQ_SHARDS * SHARD_LEN
HIDDEN = NUM_HEADS * HEAD_DIM
GROUP = NUM_HEADS // KV_COUNT
ROPE_DIM = HEAD_DIM // 2
NORM_EPS = 1e-6
ROPE_BASE = 10000000.0
RES_ALPHA = 1.0
RES_BETA = 1.0


def draw_weight(key, shape, fan_in):
    return (jax.random.normal(key, shape, jnp.float32) * fan_in ** -0.5).astype(jnp.bfloat16)


def draw_gain(key, width):
    return 1.0 + 0.3 * jax.random.normal(key, (width,), jnp.float32)


def draw_cache(key, wave_cos, wave_sin):
    sub_keys = jax.random.split(key, 3)
    amplitude = jax.random.normal(sub_keys[0], (BATCH, KV_COUNT, 3, HEAD_DIM), jnp.float32) * (2.0 / 3.0) ** 0.5
    phases = jax.random.uniform(sub_keys[1], (BATCH, KV_COUNT, 3, HEAD_DIM), jnp.float32, 0.0, 2.0 * jnp.pi)
    slow_part = jnp.einsum('bkjd,jt->bktd', amplitude * jnp.cos(phases), wave_cos) - jnp.einsum('bkjd,jt->bktd', amplitude * jnp.sin(phases), wave_sin)
    noise_vals = jax.random.normal(sub_keys[2], (BATCH, KV_COUNT, PROMPT_LEN, HEAD_DIM), jnp.float32)
    return (slow_part + 0.5 * noise_vals).astype(jnp.bfloat16)


def setup_inputs(seed: int = 0, part: int = 0) -> dict:
    base_key = jax.random.key(seed)
    shared = jax.random.split(base_key, 12)
    own_keys = jax.random.split(jax.random.fold_in(base_key, part), 4)
    positions = jnp.arange(PROMPT_LEN, dtype=jnp.float32) / PROMPT_LEN
    wave_arg = 2.0 * jnp.pi * jnp.arange(1, 4, dtype=jnp.float32)[:, None] * positions[None, :]
    wave_cos = jnp.cos(wave_arg)
    wave_sin = jnp.sin(wave_arg)
    return {
        'tokens': jax.random.normal(own_keys[0], (BATCH, MODEL_DIM), jnp.float32).astype(jnp.bfloat16),
        'states': jax.random.normal(own_keys[1], (SEQ_SHARDS, BATCH, NUM_HEADS, HEAD_DIM, HEAD_DIM), jnp.float32),
        'k_cache': draw_cache(own_keys[2], wave_cos, wave_sin),
        'v_cache': draw_cache(own_keys[3], wave_cos, wave_sin),
        'slopes': jax.random.uniform(shared[0], (NUM_HEADS,), jnp.float32, 0.2, 1.2) / PROMPT_LEN,
        'lin_gain': draw_gain(shared[1], MODEL_DIM),
        'w_lin_qkv': draw_weight(shared[2], (MODEL_DIM, 3, HIDDEN), MODEL_DIM),
        'w_lin_gate': draw_weight(shared[3], (MODEL_DIM, HIDDEN), MODEL_DIM),
        'out_gain': draw_gain(shared[4], HIDDEN),
        'w_lin_out': draw_weight(shared[5], (HIDDEN, MODEL_DIM), HIDDEN),
        'attn_gain': draw_gain(shared[6], MODEL_DIM),
        'w_attn_in': draw_weight(shared[7], (MODEL_DIM, KV_COUNT, GROUP + 2, HEAD_DIM), MODEL_DIM),
        'w_attn_out': draw_weight(shared[8], (HIDDEN, MODEL_DIM), HIDDEN),
    }


def rms_norm(vals_in, gain_vec):
    vals32 = vals_in.astype(jnp.float32)
    inv_rms = lax.rsqrt(jnp.mean(vals32 * vals32, axis=-1, keepdims=True) + NORM_EPS)
    return vals32 * inv_rms * gain_vec


def rotary(vals_in):
    half_dim = ROPE_DIM // 2
    inv_freq = ROPE_BASE ** (-jnp.arange(0, ROPE_DIM, 2, dtype=jnp.float32) / ROPE_DIM)
    angles = PROMPT_LEN * inv_freq
    cosine = jnp.cos(angles)
    sine_vals = jnp.sin(angles)
    vals32 = vals_in.astype(jnp.float32)
    first_half = vals32[..., :half_dim]
    second_half = vals32[..., half_dim:ROPE_DIM]
    return jnp.concatenate([first_half * cosine - second_half * sine_vals, second_half * cosine + first_half * sine_vals, vals32[..., ROPE_DIM:]], axis=-1).astype(jnp.bfloat16)


def attend_row(row_data):
    query_rot, keys_row, values_row, key_new, value_new = row_data
    score_scale = HEAD_DIM ** -0.5
    query_f32 = query_rot.astype(jnp.float32)
    scores = jnp.einsum('kgd,ktd->kgt', query_f32, keys_row.astype(jnp.float32)) * score_scale
    new_score = jnp.einsum('kgd,kd->kg', query_f32, key_new.astype(jnp.float32)) * score_scale
    row_max = jnp.maximum(jnp.max(scores, axis=-1), new_score)
    probs = jnp.exp(scores - row_max[..., None])
    new_prob = jnp.exp(new_score - row_max)
    prob_sum = jnp.sum(probs, axis=-1) + new_prob
    weighted_sum = jnp.einsum('kgt,ktd->kgd', probs.astype(jnp.bfloat16).astype(jnp.float32), values_row.astype(jnp.float32))
    weighted_sum = weighted_sum + new_prob.astype(jnp.bfloat16).astype(jnp.float32)[..., None] * value_new.astype(jnp.float32)[:, None, :]
    return weighted_sum / prob_sum[..., None]


def reference(tokens, states, k_cache, v_cache, slopes, lin_gain, w_lin_qkv, w_lin_gate, out_gain, w_lin_out, attn_gain, w_attn_in, w_attn_out):
    normed = rms_norm(tokens, lin_gain).astype(jnp.bfloat16)
    offsets = (SHARD_LEN * (SEQ_SHARDS - 1 - jnp.arange(SEQ_SHARDS))).astype(jnp.float32)
    shard_weight = jnp.exp(-slopes[None, :] * offsets[:, None])
    moved_state = jnp.einsum('ch,cbhde->bhde', shard_weight, states)
    lin_proj = jnp.dot(normed, w_lin_qkv.reshape(MODEL_DIM, 3 * HIDDEN), preferred_element_type=jnp.float32)
    act_vals = jax.nn.silu(lin_proj).astype(jnp.bfloat16).reshape(BATCH, 3, NUM_HEADS, HEAD_DIM).astype(jnp.float32)
    state_new = jnp.exp(-slopes)[None, :, None, None] * moved_state + jnp.einsum('bhd,bhe->bhde', act_vals[:, 1], act_vals[:, 2])
    lin_attn = jnp.einsum('bhd,bhde->bhe', act_vals[:, 0], state_new).reshape(BATCH, HIDDEN)
    gate_vals = jax.nn.sigmoid(jnp.dot(normed, w_lin_gate, preferred_element_type=jnp.float32))
    mixed_out = (rms_norm(lin_attn, out_gain) * gate_vals).astype(jnp.bfloat16)
    lin_out = jnp.dot(mixed_out, w_lin_out, preferred_element_type=jnp.float32)
    hidden = (RES_ALPHA * normed.astype(jnp.float32) + RES_BETA * lin_out).astype(jnp.bfloat16)

    normed_two = rms_norm(hidden, attn_gain).astype(jnp.bfloat16)
    attn_proj = jnp.dot(normed_two, w_attn_in.reshape(MODEL_DIM, KV_COUNT * (GROUP + 2) * HEAD_DIM), preferred_element_type=jnp.float32)
    attn_proj = attn_proj.astype(jnp.bfloat16).reshape(BATCH, KV_COUNT, GROUP + 2, HEAD_DIM)
    query_rot = rotary(attn_proj[:, :, :GROUP])
    key_new = rotary(attn_proj[:, :, GROUP])
    value_new = attn_proj[:, :, GROUP + 1]
    head_out = lax.map(attend_row, (query_rot, k_cache, v_cache, key_new, value_new))
    attn_out = jnp.dot(head_out.astype(jnp.bfloat16).reshape(BATCH, HIDDEN), w_attn_out, preferred_element_type=jnp.float32)
    hidden_out = (RES_ALPHA * normed_two.astype(jnp.float32) + RES_BETA * attn_out).astype(jnp.bfloat16)
    tail_zeros = jnp.zeros((BATCH, KV_COUNT, CACHE_EXTRA - 1, HEAD_DIM), jnp.bfloat16)
    k_out = jnp.concatenate([k_cache, key_new[:, :, None, :], tail_zeros], axis=2)
    v_out = jnp.concatenate([v_cache, value_new[:, :, None, :], tail_zeros], axis=2)
    return (hidden_out, state_new, k_out, v_out)
```

```python
import functools

import numpy as np

import jax
import jax.numpy as jnp
from jax import lax
from jax.experimental import pallas as pl
from jax.experimental.pallas import tpu as pltpu
from jax.sharding import PartitionSpec as P

NORM_EPS = 1e-6
ROPE_BASE = 10000000.0
CACHE_EXTRA = 16
LANES = 128
F32 = jnp.float32
BF16 = jnp.bfloat16
MESH = pl.DeviceIdType.MESH
NT = (((1,), (1,)), ((), ()))


def rope_tables(kv_dev, segments, group, head_dim, position):
    rope_dim = head_dim // 2
    half = rope_dim // 2
    exponents = -np.arange(0, rope_dim, 2, dtype=np.float32) / np.float32(rope_dim)
    angles = (np.float32(position) * np.float32(ROPE_BASE) ** exponents).astype(np.float32)
    cosine, sine = np.cos(angles), np.sin(angles)
    table = np.zeros((8, kv_dev, segments, head_dim), np.float32)
    table[0] = 1.0
    for segment in range(group + 1):
        table[0, :, segment, :half] = cosine
        table[0, :, segment, half:rope_dim] = cosine
        table[1, :, segment, half:rope_dim] = sine
        table[2, :, segment, :half] = -sine
    return table.reshape(8, kv_dev * segments * head_dim)


def step_kernel(dims, tok, slopes, lin_gain, out_gain, attn_gain, rope, states, k_in, v_in, w_qkv, w_gate, w_lo, w_in, w_ao,
                hid_out, st_out, k_land, v_land,
                wv_qkv, wv_gate, wv_lo, wv_in, wv_ao, st_buf, p_out, p_in, acc, rs_in, sq_x, y_x, a_x, q_x, pr_out, pr_in,
                k_buf, v_buf, o_s, q_s, kn_s, vn_s, ho_s,
                w_sem, st_sem, pair_sem, rs_sem, sq_sem, y_sem, a_sem, q_sem, pr_sem, kv_send, kv_recv, own_sem, kb_sem):
    chips, tp_size, rows, heads, head_dim, kv_dev, group, shard_len = dims
    sp_size = 2 * chips
    pairs = heads // 2
    width = heads * head_dim
    model = tok.shape[1]
    hidden_width = tp_size * width
    segments = group + 2
    qrows = kv_dev * group * rows

    me = lax.axis_index("sp")
    me_tp = lax.axis_index("tp")
    chip = me // 2
    core = lax.rem(me, 2)
    peers = [(dc, cr) for dc, cr in ((2, 0), (1, 0), (3, 0), (2, 1), (1, 1), (3, 1), (0, 1))]

    def peer_index(dc, cr):
        return lax.rem(chip + dc, chips) * 2 + (core if cr == 0 else 1 - core)

    barrier = pltpu.get_barrier_semaphore()
    for dc, cr in peers:
        pl.semaphore_signal(barrier, inc=1, device_id={"sp": peer_index(dc, cr)}, device_id_type=MESH)
    for dt in range(1, tp_size):
        pl.semaphore_signal(barrier, inc=1, device_id={"tp": lax.rem(me_tp + dt, tp_size)}, device_id_type=MESH)
    pl.semaphore_wait(barrier, len(peers) + tp_size - 1)

    def remote(src, dst, send, recv, device):
        return pltpu.make_async_remote_copy(src_ref=src, dst_ref=dst, send_sem=send, recv_sem=recv, device_id=device, device_id_type=MESH)

    my_cols = pl.ds(pl.multiple_of(me * shard_len, LANES), shard_len)

    def kv_copies(round_idx):
        cache, land = ((k_in, k_land), (v_in, v_land))[round_idx % 2]
        row = round_idx // 2
        copies = []
        for n, (dc, cr) in enumerate(peers):
            dst = peer_index(dc, cr)
            copies.append(remote(cache.at[dst * rows + row], land.at[row, :, :, my_cols], kv_send.at[round_idx, n], kv_recv.at[round_idx, n], {"sp": dst}))
        return copies

    all_kv = []

    def start_round(round_idx):
        copies = kv_copies(round_idx)
        for copy in copies:
            copy.start()
        all_kv.extend(copies)

    start_round(0)

    def state_copy(step, slot):
        target_core = jnp.where(step < chips, 1 - core, core)
        dest = lax.rem(step, chips) * 2 + target_core
        return pltpu.make_async_copy(states.at[0, pl.ds(dest * rows, rows)], st_buf.at[slot], st_sem.at[slot])

    state_copy(0, 0).start()
    weight_copies = [pltpu.make_async_copy(src, dst, w_sem.at[n]) for n, (src, dst) in enumerate(
        ((w_qkv, wv_qkv), (w_gate, wv_gate), (w_lo, wv_lo), (w_in, wv_in), (w_ao, wv_ao)))]
    for copy in weight_copies:
        copy.start()

    lane = lax.broadcasted_iota(jnp.int32, (1, LANES), 1)
    low_half = lane < head_dim

    def pair_slope(p):
        return jnp.where(low_half, jnp.full((1, LANES), slopes[2 * p], F32), jnp.full((1, LANES), slopes[2 * p + 1], F32))

    offset = (shard_len * (sp_size - 1 - me)).astype(F32)
    decay = [jnp.exp(-pair_slope(p) * offset) for p in range(pairs)]

    def weigh_step(step, target):
        slot = lax.rem(step, 2)

        @pl.when(step + 1 < 2 * chips)
        def _():
            state_copy(step + 1, lax.rem(step + 1, 2)).start()

        state_copy(step, slot).wait()
        block = lax.rem(step, chips)
        for b in range(rows):
            for p in range(pairs):
                packed = jnp.concatenate([st_buf[slot, b, 2 * p], st_buf[slot, b, 2 * p + 1]], axis=1)
                target[block, b, p] = packed * decay[p]

    @pl.loop(0, chips)
    def _(step):
        weigh_step(step, p_out)

    pair_copy = remote(p_out, p_in, pair_sem.at[0], pair_sem.at[1], {"sp": chip * 2 + (1 - core)})
    pair_copy.start()

    @pl.loop(chips, 2 * chips)
    def _(step):
        weigh_step(step, acc)

    own_copies = [pltpu.make_async_copy(cache.at[pl.ds(me * rows, rows)], land.at[:, :, :, my_cols], own_sem.at[n])
                  for n, (cache, land) in enumerate(((k_in, k_land), (v_in, v_land)))]
    for copy in own_copies:
        copy.start()

    pair_copy.wait()

    @pl.loop(0, chips)
    def _(block):
        for b in range(rows):
            acc[block, b] = acc[block, b] + p_in[block, b]

    rs_copies = []
    for dc in (2, 1, 3):
        dst_chip = lax.rem(chip + dc, chips)
        rs_copies.append(remote(acc.at[dst_chip], rs_in.at[dc - 1], rs_sem.at[0, dc - 1], rs_sem.at[1, dc - 1], {"sp": dst_chip * 2 + core}))
    for copy in rs_copies:
        copy.start()
    start_round(1)

    def rms(vals):
        return vals * lax.rsqrt(jnp.mean(vals * vals, axis=-1, keepdims=True) + NORM_EPS)

    pad_rows = 8 - rows

    def pad8(vals):
        return jnp.concatenate([vals, jnp.zeros((pad_rows,) + vals.shape[1:], vals.dtype)], axis=0) if pad_rows else vals

    tokens = pad8(tok[...].astype(F32))
    normed = (rms(tokens) * lin_gain[...]).astype(BF16)
    weight_copies[0].wait()

    def act(n):
        lin = jnp.dot(normed, wv_qkv[n], preferred_element_type=F32)
        return (lin * jax.nn.sigmoid(lin)).astype(BF16).astype(F32)

    query, key, value = act(0), act(1), act(2)
    weight_copies[1].wait()
    gate = jax.nn.sigmoid(jnp.dot(normed, wv_gate[...], preferred_element_type=F32))
    query_t = jnp.transpose(query)
    key_t = jnp.transpose(key)
    o_s[...] = jnp.zeros_like(o_s)

    def column(cols, p, b):
        lo = cols[2 * p * head_dim:(2 * p + 1) * head_dim, b:b + 1]
        hi = cols[(2 * p + 1) * head_dim:(2 * p + 2) * head_dim, b:b + 1]
        return jnp.where(low_half, lo, hi)

    for copy in rs_copies:
        copy.wait()
    start_round(2)

    for p in range(pairs):
        lam = jnp.exp(-pair_slope(p))
        cols = slice(p * LANES, (p + 1) * LANES)
        for b in range(rows):
            moved = acc[chip, b, p] + rs_in[0, b, p] + rs_in[1, b, p] + rs_in[2, b, p]
            state = lam * moved + column(key_t, p, b) * value[b:b + 1, cols]
            o_s[b:b + 1, cols] = jnp.sum(column(query_t, p, b) * state, axis=0, keepdims=True)
            st_out[b, 2 * p] = state[:, :head_dim]
            st_out[b, 2 * p + 1] = state[:, head_dim:]

    def tp_sum(buf, vals, sems):
        buf[me_tp] = vals
        copies = []
        for dt in (2, 1, 3)[-(tp_size - 1):]:
            copies.append(remote(buf.at[me_tp], buf.at[me_tp], sems.at[0, dt - 1], sems.at[1, dt - 1], {"tp": lax.rem(me_tp + dt, tp_size)}))
        for copy in copies:
            copy.start()
        for copy in copies:
            copy.wait()
        total = buf[0]
        for n in range(1, tp_size):
            total = total + buf[n]
        return total

    lin_attn = o_s[...]
    squares = jnp.broadcast_to(jnp.sum(lin_attn * lin_attn, axis=-1, keepdims=True), (8, LANES))
    square_sum = tp_sum(sq_x, squares, sq_sem)[:, :1]
    mixed = (lin_attn * lax.rsqrt(square_sum / hidden_width + NORM_EPS) * out_gain[...] * gate).astype(BF16)
    weight_copies[2].wait()
    lin_out = tp_sum(y_x, jnp.dot(mixed, wv_lo[...], preferred_element_type=F32), y_sem)
    hidden = (normed.astype(F32) + lin_out).astype(BF16).astype(F32)
    normed_two = (rms(hidden) * attn_gain[...]).astype(BF16)

    weight_copies[3].wait()
    proj = lax.dot_general(normed_two, wv_in[...], NT, preferred_element_type=F32).astype(BF16).astype(F32)
    cols_in = proj.shape[1]
    quarter = head_dim // 4
    rotated = proj * rope[0:1, :] + pltpu.roll(proj, quarter, 1) * rope[1:2, :] + pltpu.roll(proj, cols_in - quarter, 1) * rope[2:3, :]
    rotated = rotated.astype(BF16).astype(F32)

    def segment_at(kv, segment):
        start = (kv * segments + segment) * head_dim
        block = rotated[:, start // LANES * LANES:start // LANES * LANES + LANES]
        if start % LANES != kv * head_dim:
            block = pltpu.roll(block, head_dim, 1)
        return jnp.where(low_half if kv == 0 else ~low_half, block, 0.0)

    for kv in range(kv_dev):
        key_rows, value_rows = segment_at(kv, group), segment_at(kv, group + 1)
        for i in range(group):
            row = (kv * group + i) * rows
            q_s[row:row + rows, :] = segment_at(kv, i)[:rows]
            kn_s[row:row + rows, :] = key_rows[:rows]
            vn_s[row:row + rows, :] = value_rows[:rows]

    q_x[me] = q_s[...].astype(BF16)
    q_copies = []
    for n, (dc, cr) in enumerate(peers):
        q_copies.append(remote(q_x.at[me], q_x.at[me], q_sem.at[0, n], q_sem.at[1, n], {"sp": peer_index(dc, cr)}))
    for copy in q_copies:
        copy.start()
    start_round(3)
    start_round(4)

    def shard_copies(j, slot):
        return [pltpu.make_async_copy(cache.at[pl.ds(j * rows, rows)], buf.at[slot], kb_sem.at[n, slot])
                for n, (cache, buf) in enumerate(((k_in, k_buf), (v_in, v_buf)))]

    for copy in shard_copies(0, 0):
        copy.start()

    rotated_t = jnp.transpose(rotated)
    lane16 = lax.broadcasted_iota(jnp.int32, (1, CACHE_EXTRA), 1)
    prompt_len = sp_size * shard_len
    for land, segment in ((k_land, group), (v_land, group + 1)):
        for kv in range(kv_dev):
            start = (kv * segments + segment) * head_dim
            for b in range(rows):
                tail = jnp.where(lane16 == 0, rotated_t[start:start + head_dim, b:b + 1], 0.0)
                land[b, kv, :, prompt_len:] = tail.astype(BF16)

    row_id = lax.broadcasted_iota(jnp.int32, (qrows, 1), 0)
    row_seq = lax.rem(row_id, rows)
    own_lanes = (row_id < group * rows) == low_half
    scale = head_dim ** -0.5
    stat_lane = lax.rem(lane, head_dim) < head_dim // 2

    for copy in q_copies:
        copy.wait()

    @pl.loop(0, sp_size)
    def _(j):
        slot = lax.rem(j, 2)

        @pl.when(j + 1 < sp_size)
        def _():
            for copy in shard_copies(j + 1, lax.rem(j + 1, 2)):
                copy.start()

        for copy in shard_copies(j, slot):
            copy.wait()
        queries = q_x[j]
        scores = jnp.zeros((qrows, shard_len), F32)
        for b in range(rows):
            keys = k_buf[slot, b].reshape(kv_dev * head_dim, shard_len)
            scores = jnp.where(row_seq == b, jnp.dot(queries, keys, preferred_element_type=F32), scores)
        scores = scores * scale
        peak = jnp.max(scores, axis=-1, keepdims=True)
        probs = jnp.exp(scores - peak)
        total = jnp.sum(probs, axis=-1, keepdims=True)
        probs = probs.astype(BF16)
        out = jnp.zeros((qrows, LANES), F32)
        for b in range(rows):
            vals = v_buf[slot, b].reshape(kv_dev * head_dim, shard_len)
            out = jnp.where(row_seq == b, lax.dot_general(probs, vals, NT, preferred_element_type=F32), out)
        pr_out[j] = jnp.where(own_lanes, out, jnp.where(stat_lane, peak, total))

    pr_copies = []
    for n, (dc, cr) in enumerate(peers):
        dst = peer_index(dc, cr)
        pr_copies.append(remote(pr_out.at[dst], pr_in.at[me], pr_sem.at[0, n], pr_sem.at[1, n], {"sp": dst}))
    for copy in pr_copies:
        copy.start()
    for round_idx in range(5, 2 * rows):
        start_round(round_idx)
    pr_in[me] = pr_out[me]

    new_score = jnp.sum(q_s[...] * kn_s[...], axis=-1, keepdims=True) * scale
    split = group * rows

    def stats(j, first):
        return jnp.concatenate([pr_in[j, :split, head_dim + first:head_dim + first + 1], pr_in[j, split:, first:first + 1]], axis=0)

    for copy in pr_copies:
        copy.wait()
    peaks = [stats(j, 0) for j in range(sp_size)]
    top = new_score
    for peak in peaks:
        top = jnp.maximum(top, peak)
    new_prob = jnp.exp(new_score - top)
    prob_sum = new_prob
    head = new_prob.astype(BF16).astype(F32) * vn_s[...]
    for j in range(sp_size):
        weight = jnp.exp(peaks[j] - top)
        prob_sum = prob_sum + weight * stats(j, head_dim // 2)
        head = head + weight * jnp.where(own_lanes, pr_in[j], 0.0)
    head = (head / prob_sum).astype(BF16).astype(F32)

    ho_s[...] = jnp.zeros_like(ho_s)
    for n in range(0, kv_dev * group, 2):
        block = None
        for m in (n, n + 1):
            kv = m // group
            piece = head[m * rows:(m + 1) * rows]
            if kv != m % 2:
                piece = pltpu.roll(piece, head_dim, 1)
            block = piece if block is None else block + piece
        ho_s[0:rows, n // 2 * LANES:(n // 2 + 1) * LANES] = block
    weight_copies[4].wait()
    attn_out = tp_sum(a_x, jnp.dot(ho_s[...].astype(BF16), wv_ao[...], preferred_element_type=F32), a_sem)
    hid_out[...] = (normed_two.astype(F32) + attn_out).astype(BF16)[:rows]

    for copy in own_copies:
        copy.wait()
    for copy in all_kv:
        copy.wait()


def put_kernel(*refs):
    count = (len(refs) - 1) // 2
    sems = refs[-1]
    copies = [pltpu.make_async_copy(refs[n], refs[count + n], sems.at[n]) for n in range(count)]
    for copy in copies:
        copy.start()
    for copy in copies:
        copy.wait()


def solution(mesh):
    sp_size = mesh.shape['sp']
    tp_size = mesh.shape['tp']
    chips = sp_size // 2

    def device_step(tokens, states, k_cache, v_cache, slopes, lin_gain, w_lin_qkv, w_lin_gate, out_gain, w_lin_out, attn_gain, w_attn_in, w_attn_out):
        rows, model = tokens.shape
        kv_dev, shard_len, head_dim = k_cache.shape[1:]
        heads = slopes.shape[0]
        segments = w_attn_in.shape[2]
        group = segments - 2
        width = heads * head_dim
        pairs = heads // 2
        cols_in = kv_dev * segments * head_dim
        qrows = kv_dev * group * rows
        prompt_len = sp_size * shard_len
        full_len = prompt_len + CACHE_EXTRA
        dims = (chips, tp_size, rows, heads, head_dim, kv_dev, group, shard_len)
        rope = jnp.asarray(rope_tables(kv_dev, segments, group, head_dim, prompt_len))

        vmem = pl.BlockSpec(memory_space=pltpu.VMEM)
        smem = pl.BlockSpec(memory_space=pltpu.SMEM)
        anym = pl.BlockSpec(memory_space=pl.ANY)
        dma = pltpu.SemaphoreType.DMA
        land_shape = (rows, kv_dev, head_dim, full_len)
        out_types = [((rows, model), BF16), ((rows, heads, head_dim, head_dim), F32), (land_shape, BF16), (land_shape, BF16)]
        scratch = [
            pltpu.VMEM((3, model, width), BF16),
            pltpu.VMEM((model, width), BF16),
            pltpu.VMEM((width, model), BF16),
            pltpu.VMEM((cols_in, model), BF16),
            pltpu.VMEM((width, model), BF16),
            pltpu.VMEM((2, rows, heads, head_dim, head_dim), F32),
            pltpu.VMEM((chips, rows, pairs, head_dim, LANES), F32),
            pltpu.VMEM((chips, rows, pairs, head_dim, LANES), F32),
            pltpu.VMEM((chips, rows, pairs, head_dim, LANES), F32),
            pltpu.VMEM((chips - 1, rows, pairs, head_dim, LANES), F32),
            pltpu.VMEM((tp_size, 8, LANES), F32),
            pltpu.VMEM((tp_size, 8, model), F32),
            pltpu.VMEM((tp_size, 8, model), F32),
            pltpu.VMEM((sp_size, qrows, LANES), BF16),
            pltpu.VMEM((sp_size, qrows, LANES), F32),
            pltpu.VMEM((sp_size, qrows, LANES), F32),
            pltpu.VMEM((2, rows, kv_dev, head_dim, shard_len), BF16),
            pltpu.VMEM((2, rows, kv_dev, head_dim, shard_len), BF16),
            pltpu.VMEM((8, width), F32),
            pltpu.VMEM((qrows, LANES), F32),
            pltpu.VMEM((qrows, LANES), F32),
            pltpu.VMEM((qrows, LANES), F32),
            pltpu.VMEM((8, width), F32),
            dma((5,)),
            dma((2,)),
            dma((2,)),
            dma((2, chips - 1)),
            dma((2, tp_size - 1)),
            dma((2, tp_size - 1)),
            dma((2, tp_size - 1)),
            dma((2, sp_size - 1)),
            dma((2, sp_size - 1)),
            dma((2 * rows, sp_size - 1)),
            dma((2 * rows, sp_size - 1)),
            dma((2,)),
            dma((2, 2)),
        ]
        landed = pl.pallas_call(
            functools.partial(step_kernel, dims),
            out_shape=[pltpu.VMEM(shape, dtype) for shape, dtype in out_types],
            in_specs=[vmem, smem, vmem, vmem, vmem, vmem] + [anym] * 8,
            out_specs=[vmem] * 4,
            scratch_shapes=scratch,
            compiler_params=pltpu.CompilerParams(collective_id=0, has_side_effects=True, vmem_limit_bytes=40 * 2 ** 20),
        )(
            tokens, slopes, lin_gain.reshape(1, -1), out_gain.reshape(1, -1), attn_gain.reshape(1, -1), rope,
            states, jnp.transpose(k_cache, (0, 1, 3, 2)), jnp.transpose(v_cache, (0, 1, 3, 2)),
            jnp.transpose(w_lin_qkv, (1, 0, 2)), w_lin_gate, w_lin_out,
            jnp.transpose(w_attn_in, (1, 2, 3, 0)).reshape(cols_in, model), w_attn_out,
        )
        hidden_out, state_new, k_out, v_out = pl.pallas_call(
            put_kernel,
            out_shape=[jax.ShapeDtypeStruct(shape, dtype) for shape, dtype in out_types],
            in_specs=[vmem] * 4,
            out_specs=[anym] * 4,
            scratch_shapes=[dma((4,))],
            compiler_params=pltpu.CompilerParams(vmem_limit_bytes=2 * 2 ** 20),
        )(*landed)
        return hidden_out, state_new, jnp.transpose(k_out, (0, 1, 3, 2)), jnp.transpose(v_out, (0, 1, 3, 2))

    batch_spec = P(('dp', 'sp'), None)
    head_spec = P(('dp', 'sp'), 'tp', None, None)
    cache_spec = P('dp', 'tp', 'sp', None)
    in_specs = (batch_spec, P('sp', 'dp', 'tp', None, None), cache_spec, cache_spec, P('tp'), P(None), P(None, None, 'tp'), P(None, 'tp'), P('tp'), P('tp', None), P(None), P(None, 'tp', None, None), P('tp', None))
    out_specs = (batch_spec, head_spec, head_spec, head_spec)
    return jax.shard_map(device_step, mesh=mesh, in_specs=in_specs, out_specs=out_specs, check_vma=False)
```

```python
import functools

import numpy as np

import jax
import jax.numpy as jnp
from jax import lax
from jax.experimental import pallas as pl
from jax.experimental.pallas import tpu as pltpu
from jax.sharding import PartitionSpec as P

NORM_EPS = 1e-6
ROPE_BASE = 10000000.0
CACHE_EXTRA = 16
LANES = 128
F32 = jnp.float32
BF16 = jnp.bfloat16
MESH = pl.DeviceIdType.MESH
NT = (((1,), (1,)), ((), ()))


def rope_tables(kv_dev, segments, group, head_dim, position):
    rope_dim = head_dim // 2
    half = rope_dim // 2
    exponents = -np.arange(0, rope_dim, 2, dtype=np.float32) / np.float32(rope_dim)
    angles = (np.float32(position) * np.float32(ROPE_BASE) ** exponents).astype(np.float32)
    cosine, sine = np.cos(angles), np.sin(angles)
    table = np.zeros((8, kv_dev, segments, head_dim), np.float32)
    table[0] = 1.0
    for segment in range(group + 1):
        table[0, :, segment, :half] = cosine
        table[0, :, segment, half:rope_dim] = cosine
        table[1, :, segment, half:rope_dim] = sine
        table[2, :, segment, :half] = -sine
    return table.reshape(8, kv_dev * segments * head_dim)


def step_kernel(dims, tok_in, slopes, lin_gain_in, out_gain_in, attn_gain_in, rope_in, states, k_in, v_in, w_qkv, w_gate, w_lo, w_in, w_ao,
                hid_out, st_out, k_land, v_land,
                tok, lin_gain, out_gain, attn_gain, rope, wv_qkv, wv_gate, wv_lo, wv_in, wv_ao, st_buf, p_out, p_in, acc, relay_in, rs_in, sq_x, y_x, a_x, q_x, pr_out, pr_in,
                k_buf, v_buf, o_s, q_s, kn_s, vn_s, ho_s,
                in_sem, w_sem, st_sem, pair_sem, rs_sem, sq_sem, y_sem, a_sem, q_sem, pr_sem, kv_send, kv_recv, own_sem, kb_sem):
    chips, tp_size, rows, heads, head_dim, kv_dev, group, shard_len = dims
    sp_size = 2 * chips
    pairs = heads // 2
    width = heads * head_dim
    model = tok_in.shape[1]
    hidden_width = tp_size * width
    segments = group + 2
    qrows = kv_dev * group * rows

    me = lax.axis_index("sp")
    me_tp = lax.axis_index("tp")
    chip = me // 2
    core = lax.rem(me, 2)
    peers = [(dc, cr) for dc, cr in ((2, 0), (1, 0), (3, 0), (2, 1), (1, 1), (3, 1), (0, 1))]

    def peer_index(dc, cr):
        return lax.rem(chip + dc, chips) * 2 + (core if cr == 0 else 1 - core)

    barrier = pltpu.get_barrier_semaphore()
    for dc, cr in peers:
        pl.semaphore_signal(barrier, inc=1, device_id={"sp": peer_index(dc, cr)}, device_id_type=MESH)
    for dt in range(1, tp_size):
        pl.semaphore_signal(barrier, inc=1, device_id={"tp": lax.rem(me_tp + dt, tp_size)}, device_id_type=MESH)
    pl.semaphore_wait(barrier, len(peers) + tp_size - 1)

    def remote(src, dst, send, recv, device):
        return pltpu.make_async_remote_copy(src_ref=src, dst_ref=dst, send_sem=send, recv_sem=recv, device_id=device, device_id_type=MESH)

    my_cols = pl.ds(pl.multiple_of(me * shard_len, LANES), shard_len)

    def kv_copies(round_idx):
        cache, land = ((k_in, k_land), (v_in, v_land))[round_idx % 2]
        row = round_idx // 2
        copies = []
        for n, (dc, cr) in enumerate(peers):
            dst = peer_index(dc, cr)
            copies.append(remote(cache.at[dst * rows + row], land.at[row, :, :, my_cols], kv_send.at[round_idx, n], kv_recv.at[round_idx, n], {"sp": dst}))
        return copies

    all_kv = []

    def start_round(round_idx):
        copies = kv_copies(round_idx)
        for copy in copies:
            copy.start()
        all_kv.extend(copies)

    start_round(0)

    def state_copy(step, slot):
        target_core = jnp.where(step < chips, 1 - core, core)
        dest = lax.rem(step, chips) * 2 + target_core
        return pltpu.make_async_copy(states.at[0, pl.ds(dest * rows, rows)], st_buf.at[slot], st_sem.at[slot])

    state_copy(0, 0).start()
    small_copies = [pltpu.make_async_copy(src, dst, in_sem.at[n]) for n, (src, dst) in enumerate(
        ((tok_in, tok), (lin_gain_in, lin_gain), (out_gain_in, out_gain), (attn_gain_in, attn_gain), (rope_in, rope)))]
    for copy in small_copies:
        copy.start()
    weight_copies = [pltpu.make_async_copy(src, dst, w_sem.at[n]) for n, (src, dst) in enumerate(
        ((w_qkv, wv_qkv), (w_gate, wv_gate), (w_lo, wv_lo), (w_in, wv_in), (w_ao, wv_ao)))]
    for copy in weight_copies:
        copy.start()

    lane = lax.broadcasted_iota(jnp.int32, (1, LANES), 1)
    low_half = lane < head_dim

    def pair_slope(p):
        return jnp.where(low_half, jnp.full((1, LANES), slopes[2 * p], F32), jnp.full((1, LANES), slopes[2 * p + 1], F32))

    offset = (shard_len * (sp_size - 1 - me)).astype(F32)
    decay = [jnp.exp(-pair_slope(p) * offset) for p in range(pairs)]

    def weigh_step(step, target):
        slot = lax.rem(step, 2)

        @pl.when(step + 1 < 2 * chips)
        def _():
            state_copy(step + 1, lax.rem(step + 1, 2)).start()

        state_copy(step, slot).wait()
        block = lax.rem(step, chips)
        for b in range(rows):
            for p in range(pairs):
                packed = jnp.concatenate([st_buf[slot, b, 2 * p], st_buf[slot, b, 2 * p + 1]], axis=1)
                target[block, b, p] = packed * decay[p]

    @pl.loop(0, chips)
    def _(step):
        weigh_step(step, p_out)

    pair_copy = remote(p_out, p_in, pair_sem.at[0], pair_sem.at[1], {"sp": chip * 2 + (1 - core)})
    pair_copy.start()

    @pl.loop(chips, 2 * chips)
    def _(step):
        weigh_step(step, acc)

    own_copies = [pltpu.make_async_copy(cache.at[pl.ds(me * rows, rows)], land.at[:, :, :, my_cols], own_sem.at[n])
                  for n, (cache, land) in enumerate(((k_in, k_land), (v_in, v_land)))]
    for copy in own_copies:
        copy.start()

    pair_copy.wait()

    @pl.loop(0, chips)
    def _(block):
        for b in range(rows):
            acc[block, b] = acc[block, b] + p_in[block, b]

    nexts = [(lax.rem(chip + dc, chips), {"sp": lax.rem(chip + dc, chips) * 2 + core}) for dc in (1, chips - 1)]
    far = lax.rem(chip + 2, chips)
    half = rows // 2
    parts = [pl.ds(0, half), pl.ds(half, half)]

    def rs_copy(n, src, dst, side):
        return remote(src, dst, rs_sem.at[0, n], rs_sem.at[1, n], nexts[side][1])

    relay_copies = [rs_copy(side, acc.at[far, parts[side]], relay_in.at[side], side) for side in range(2)]
    rs_copies = [rs_copy(2 + side, acc.at[nexts[side][0], parts[1 - side]], rs_in.at[side, parts[1 - side]], side) for side in range(2)]
    for copy in relay_copies + rs_copies:
        copy.start()
    start_round(1)

    def rms(vals):
        return vals * lax.rsqrt(jnp.mean(vals * vals, axis=-1, keepdims=True) + NORM_EPS)

    pad_rows = 8 - rows

    def pad8(vals):
        return jnp.concatenate([vals, jnp.zeros((pad_rows,) + vals.shape[1:], vals.dtype)], axis=0) if pad_rows else vals

    for copy in small_copies:
        copy.wait()
    tokens = pad8(tok[...].astype(F32))
    normed = (rms(tokens) * lin_gain[...]).astype(BF16)
    weight_copies[0].wait()

    def act(n):
        lin = jnp.dot(normed, wv_qkv[n], preferred_element_type=F32)
        return (lin * jax.nn.sigmoid(lin)).astype(BF16).astype(F32)

    query, key, value = act(0), act(1), act(2)
    weight_copies[1].wait()
    gate = jax.nn.sigmoid(jnp.dot(normed, wv_gate[...], preferred_element_type=F32))
    query_t = jnp.transpose(query)
    key_t = jnp.transpose(key)
    for side in range(2):
        relay_copies[side].wait()
        block = nexts[side][0]
        for b in range(half):
            acc[block, side * half + b] = acc[block, side * half + b] + relay_in[side, b]
        copy = rs_copy(4 + side, acc.at[block, parts[side]], rs_in.at[side, parts[side]], side)
        copy.start()
        rs_copies.append(copy)
    start_round(2)
    o_s[...] = jnp.zeros_like(o_s)

    def column(cols, p, b):
        lo = cols[2 * p * head_dim:(2 * p + 1) * head_dim, b:b + 1]
        hi = cols[(2 * p + 1) * head_dim:(2 * p + 2) * head_dim, b:b + 1]
        return jnp.where(low_half, lo, hi)

    for copy in rs_copies:
        copy.wait()

    for p in range(pairs):
        lam = jnp.exp(-pair_slope(p))
        cols = slice(p * LANES, (p + 1) * LANES)
        for b in range(rows):
            moved = acc[chip, b, p] + rs_in[0, b, p] + rs_in[1, b, p]
            state = lam * moved + column(key_t, p, b) * value[b:b + 1, cols]
            o_s[b:b + 1, cols] = jnp.sum(column(query_t, p, b) * state, axis=0, keepdims=True)
            st_out[b, 2 * p] = state[:, :head_dim]
            st_out[b, 2 * p + 1] = state[:, head_dim:]

    def tp_sum(buf, vals, sems):
        buf[me_tp] = vals
        copies = []
        for dt in (2, 1, 3)[-(tp_size - 1):]:
            copies.append(remote(buf.at[me_tp], buf.at[me_tp], sems.at[0, dt - 1], sems.at[1, dt - 1], {"tp": lax.rem(me_tp + dt, tp_size)}))
        for copy in copies:
            copy.start()
        for copy in copies:
            copy.wait()
        total = buf[0]
        for n in range(1, tp_size):
            total = total + buf[n]
        return total

    lin_attn = o_s[...]
    squares = jnp.broadcast_to(jnp.sum(lin_attn * lin_attn, axis=-1, keepdims=True), (8, LANES))
    square_sum = tp_sum(sq_x, squares, sq_sem)[:, :1]
    mixed = (lin_attn * lax.rsqrt(square_sum / hidden_width + NORM_EPS) * out_gain[...] * gate).astype(BF16)
    weight_copies[2].wait()
    lin_out = tp_sum(y_x, jnp.dot(mixed, wv_lo[...], preferred_element_type=F32), y_sem)
    hidden = (normed.astype(F32) + lin_out).astype(BF16).astype(F32)
    normed_two = (rms(hidden) * attn_gain[...]).astype(BF16)

    weight_copies[3].wait()
    proj = lax.dot_general(normed_two, wv_in[...], NT, preferred_element_type=F32).astype(BF16).astype(F32)
    cols_in = proj.shape[1]
    quarter = head_dim // 4
    rotated = proj * rope[0:1, :] + pltpu.roll(proj, quarter, 1) * rope[1:2, :] + pltpu.roll(proj, cols_in - quarter, 1) * rope[2:3, :]
    rotated = rotated.astype(BF16).astype(F32)

    def segment_at(kv, segment):
        start = (kv * segments + segment) * head_dim
        block = rotated[:, start // LANES * LANES:start // LANES * LANES + LANES]
        if start % LANES != kv * head_dim:
            block = pltpu.roll(block, head_dim, 1)
        return jnp.where(low_half if kv == 0 else ~low_half, block, 0.0)

    for kv in range(kv_dev):
        key_rows, value_rows = segment_at(kv, group), segment_at(kv, group + 1)
        for i in range(group):
            row = (kv * group + i) * rows
            q_s[row:row + rows, :] = segment_at(kv, i)[:rows]
            kn_s[row:row + rows, :] = key_rows[:rows]
            vn_s[row:row + rows, :] = value_rows[:rows]

    q_x[me] = q_s[...].astype(BF16)
    q_copies = []
    for n, (dc, cr) in enumerate(peers):
        q_copies.append(remote(q_x.at[me], q_x.at[me], q_sem.at[0, n], q_sem.at[1, n], {"sp": peer_index(dc, cr)}))
    for copy in q_copies:
        copy.start()
    start_round(3)
    start_round(4)

    def shard_copies(j, slot):
        return [pltpu.make_async_copy(cache.at[pl.ds(j * rows, rows)], buf.at[slot], kb_sem.at[n, slot])
                for n, (cache, buf) in enumerate(((k_in, k_buf), (v_in, v_buf)))]

    for copy in shard_copies(0, 0):
        copy.start()

    rotated_t = jnp.transpose(rotated)
    lane16 = lax.broadcasted_iota(jnp.int32, (1, CACHE_EXTRA), 1)
    prompt_len = sp_size * shard_len
    for land, segment in ((k_land, group), (v_land, group + 1)):
        for kv in range(kv_dev):
            start = (kv * segments + segment) * head_dim
            for b in range(rows):
                tail = jnp.where(lane16 == 0, rotated_t[start:start + head_dim, b:b + 1], 0.0)
                land[b, kv, :, prompt_len:] = tail.astype(BF16)

    row_id = lax.broadcasted_iota(jnp.int32, (qrows, 1), 0)
    row_seq = lax.rem(row_id, rows)
    own_lanes = (row_id < group * rows) == low_half
    scale = head_dim ** -0.5
    stat_lane = lax.rem(lane, head_dim) < head_dim // 2

    for copy in q_copies:
        copy.wait()

    @pl.loop(0, sp_size)
    def _(j):
        slot = lax.rem(j, 2)

        @pl.when(j + 1 < sp_size)
        def _():
            for copy in shard_copies(j + 1, lax.rem(j + 1, 2)):
                copy.start()

        for copy in shard_copies(j, slot):
            copy.wait()
        queries = q_x[j]
        scores = jnp.zeros((qrows, shard_len), F32)
        for b in range(rows):
            keys = k_buf[slot, b].reshape(kv_dev * head_dim, shard_len)
            scores = jnp.where(row_seq == b, jnp.dot(queries, keys, preferred_element_type=F32), scores)
        scores = scores * scale
        peak = jnp.max(scores, axis=-1, keepdims=True)
        probs = jnp.exp(scores - peak)
        total = jnp.sum(probs, axis=-1, keepdims=True)
        probs = probs.astype(BF16)
        out = jnp.zeros((qrows, LANES), F32)
        for b in range(rows):
            vals = v_buf[slot, b].reshape(kv_dev * head_dim, shard_len)
            out = jnp.where(row_seq == b, lax.dot_general(probs, vals, NT, preferred_element_type=F32), out)
        pr_out[j] = jnp.where(own_lanes, out, jnp.where(stat_lane, peak, total))

    pr_copies = []
    for n, (dc, cr) in enumerate(peers):
        dst = peer_index(dc, cr)
        pr_copies.append(remote(pr_out.at[dst], pr_in.at[me], pr_sem.at[0, n], pr_sem.at[1, n], {"sp": dst}))
    for copy in pr_copies:
        copy.start()
    for round_idx in range(5, 2 * rows):
        start_round(round_idx)
    pr_in[me] = pr_out[me]

    new_score = jnp.sum(q_s[...] * kn_s[...], axis=-1, keepdims=True) * scale
    split = group * rows

    def stats(j, first):
        return jnp.concatenate([pr_in[j, :split, head_dim + first:head_dim + first + 1], pr_in[j, split:, first:first + 1]], axis=0)

    for copy in pr_copies:
        copy.wait()
    peaks = [stats(j, 0) for j in range(sp_size)]
    top = new_score
    for peak in peaks:
        top = jnp.maximum(top, peak)
    new_prob = jnp.exp(new_score - top)
    prob_sum = new_prob
    head = new_prob.astype(BF16).astype(F32) * vn_s[...]
    for j in range(sp_size):
        weight = jnp.exp(peaks[j] - top)
        prob_sum = prob_sum + weight * stats(j, head_dim // 2)
        head = head + weight * jnp.where(own_lanes, pr_in[j], 0.0)
    head = (head / prob_sum).astype(BF16).astype(F32)

    ho_s[...] = jnp.zeros_like(ho_s)
    for n in range(0, kv_dev * group, 2):
        block = None
        for m in (n, n + 1):
            kv = m // group
            piece = head[m * rows:(m + 1) * rows]
            if kv != m % 2:
                piece = pltpu.roll(piece, head_dim, 1)
            block = piece if block is None else block + piece
        ho_s[0:rows, n // 2 * LANES:(n // 2 + 1) * LANES] = block
    weight_copies[4].wait()
    attn_out = tp_sum(a_x, jnp.dot(ho_s[...].astype(BF16), wv_ao[...], preferred_element_type=F32), a_sem)
    hid_out[...] = (normed_two.astype(F32) + attn_out).astype(BF16)[:rows]

    for copy in own_copies:
        copy.wait()
    for copy in all_kv:
        copy.wait()


def put_kernel(*refs):
    count = (len(refs) - 1) // 2
    sems = refs[-1]
    copies = []
    for n in (2, 3, 1, 0):
        pieces = refs[n].shape[0] if n > 0 else 1
        for i in range(pieces):
            src, dst = (refs[n].at[i], refs[count + n].at[i]) if pieces > 1 else (refs[n], refs[count + n])
            copies.append(pltpu.make_async_copy(src, dst, sems.at[len(copies)]))
    for copy in copies:
        copy.start()
    for copy in copies:
        copy.wait()


def solution(mesh):
    sp_size = mesh.shape['sp']
    tp_size = mesh.shape['tp']
    chips = sp_size // 2

    def device_step(tokens, states, k_cache, v_cache, slopes, lin_gain, w_lin_qkv, w_lin_gate, out_gain, w_lin_out, attn_gain, w_attn_in, w_attn_out):
        rows, model = tokens.shape
        kv_dev, shard_len, head_dim = k_cache.shape[1:]
        heads = slopes.shape[0]
        segments = w_attn_in.shape[2]
        group = segments - 2
        width = heads * head_dim
        pairs = heads // 2
        cols_in = kv_dev * segments * head_dim
        qrows = kv_dev * group * rows
        prompt_len = sp_size * shard_len
        full_len = prompt_len + CACHE_EXTRA
        dims = (chips, tp_size, rows, heads, head_dim, kv_dev, group, shard_len)
        rope = jnp.asarray(rope_tables(kv_dev, segments, group, head_dim, prompt_len))

        vmem = pl.BlockSpec(memory_space=pltpu.VMEM)
        smem = pl.BlockSpec(memory_space=pltpu.SMEM)
        anym = pl.BlockSpec(memory_space=pl.ANY)
        dma = pltpu.SemaphoreType.DMA
        land_shape = (rows, kv_dev, head_dim, full_len)
        out_types = [((rows, model), BF16), ((rows, heads, head_dim, head_dim), F32), (land_shape, BF16), (land_shape, BF16)]
        scratch = [
            pltpu.VMEM((rows, model), BF16),
            pltpu.VMEM((1, model), F32),
            pltpu.VMEM((1, width), F32),
            pltpu.VMEM((1, model), F32),
            pltpu.VMEM((8, cols_in), F32),
            pltpu.VMEM((3, model, width), BF16),
            pltpu.VMEM((model, width), BF16),
            pltpu.VMEM((width, model), BF16),
            pltpu.VMEM((cols_in, model), BF16),
            pltpu.VMEM((width, model), BF16),
            pltpu.VMEM((2, rows, heads, head_dim, head_dim), F32),
            pltpu.VMEM((chips, rows, pairs, head_dim, LANES), F32),
            pltpu.VMEM((chips, rows, pairs, head_dim, LANES), F32),
            pltpu.VMEM((chips, rows, pairs, head_dim, LANES), F32),
            pltpu.VMEM((2, rows // 2, pairs, head_dim, LANES), F32),
            pltpu.VMEM((2, rows, pairs, head_dim, LANES), F32),
            pltpu.VMEM((tp_size, 8, LANES), F32),
            pltpu.VMEM((tp_size, 8, model), F32),
            pltpu.VMEM((tp_size, 8, model), F32),
            pltpu.VMEM((sp_size, qrows, LANES), BF16),
            pltpu.VMEM((sp_size, qrows, LANES), F32),
            pltpu.VMEM((sp_size, qrows, LANES), F32),
            pltpu.VMEM((2, rows, kv_dev, head_dim, shard_len), BF16),
            pltpu.VMEM((2, rows, kv_dev, head_dim, shard_len), BF16),
            pltpu.VMEM((8, width), F32),
            pltpu.VMEM((qrows, LANES), F32),
            pltpu.VMEM((qrows, LANES), F32),
            pltpu.VMEM((qrows, LANES), F32),
            pltpu.VMEM((8, width), F32),
            dma((5,)),
            dma((5,)),
            dma((2,)),
            dma((2,)),
            dma((2, 6)),
            dma((2, tp_size - 1)),
            dma((2, tp_size - 1)),
            dma((2, tp_size - 1)),
            dma((2, sp_size - 1)),
            dma((2, sp_size - 1)),
            dma((2 * rows, sp_size - 1)),
            dma((2 * rows, sp_size - 1)),
            dma((2,)),
            dma((2, 2)),
        ]
        landed = pl.pallas_call(
            functools.partial(step_kernel, dims),
            out_shape=[pltpu.VMEM(shape, dtype) for shape, dtype in out_types],
            in_specs=[anym, smem, anym, anym, anym, anym] + [anym] * 8,
            out_specs=[vmem] * 4,
            scratch_shapes=scratch,
            compiler_params=pltpu.CompilerParams(collective_id=0, has_side_effects=True, vmem_limit_bytes=40 * 2 ** 20),
        )(
            tokens, slopes, lin_gain.reshape(1, -1), out_gain.reshape(1, -1), attn_gain.reshape(1, -1), rope,
            states, jnp.transpose(k_cache, (0, 1, 3, 2)), jnp.transpose(v_cache, (0, 1, 3, 2)),
            jnp.transpose(w_lin_qkv, (1, 0, 2)), w_lin_gate, w_lin_out,
            jnp.transpose(w_attn_in, (1, 2, 3, 0)).reshape(cols_in, model), w_attn_out,
        )
        hidden_out, state_new, k_out, v_out = pl.pallas_call(
            put_kernel,
            out_shape=[jax.ShapeDtypeStruct(shape, dtype) for shape, dtype in out_types],
            in_specs=[vmem] * 4,
            out_specs=[anym] * 4,
            scratch_shapes=[dma((3 * rows + 1,))],
            compiler_params=pltpu.CompilerParams(vmem_limit_bytes=2 * 2 ** 20),
        )(*landed)
        return hidden_out, state_new, jnp.transpose(k_out, (0, 1, 3, 2)), jnp.transpose(v_out, (0, 1, 3, 2))

    batch_spec = P(('dp', 'sp'), None)
    head_spec = P(('dp', 'sp'), 'tp', None, None)
    cache_spec = P('dp', 'tp', 'sp', None)
    in_specs = (batch_spec, P('sp', 'dp', 'tp', None, None), cache_spec, cache_spec, P('tp'), P(None), P(None, None, 'tp'), P(None, 'tp'), P('tp'), P('tp', None), P(None), P(None, 'tp', None, None), P('tp', None))
    out_specs = (batch_spec, head_spec, head_spec, head_spec)
    return jax.shard_map(device_step, mesh=mesh, in_specs=in_specs, out_specs=out_specs, check_vma=False)
```

```python
import functools

import numpy as np

import jax
import jax.numpy as jnp
from jax import lax
from jax.experimental import pallas as pl
from jax.experimental.pallas import tpu as pltpu
from jax.sharding import PartitionSpec as P

NORM_EPS = 1e-6
ROPE_BASE = 10000000.0
CACHE_EXTRA = 16
LANES = 128
F32 = jnp.float32
BF16 = jnp.bfloat16
MESH = pl.DeviceIdType.MESH
NT = (((1,), (1,)), ((), ()))


def rope_tables(kv_dev, segments, group, head_dim, position):
    rope_dim = head_dim // 2
    half = rope_dim // 2
    exponents = -np.arange(0, rope_dim, 2, dtype=np.float32) / np.float32(rope_dim)
    angles = (np.float32(position) * np.float32(ROPE_BASE) ** exponents).astype(np.float32)
    cosine, sine = np.cos(angles), np.sin(angles)
    table = np.zeros((8, kv_dev, segments, head_dim), np.float32)
    table[0] = 1.0
    for segment in range(group + 1):
        table[0, :, segment, :half] = cosine
        table[0, :, segment, half:rope_dim] = cosine
        table[1, :, segment, half:rope_dim] = sine
        table[2, :, segment, :half] = -sine
    return table.reshape(8, kv_dev * segments * head_dim)


def step_kernel(dims, tok_in, slopes, lin_gain_in, out_gain_in, attn_gain_in, rope_in, states, k_in, v_in, w_qkv, w_gate, w_lo, w_in, w_ao,
                hid_out, st_out, k_land, v_land,
                tok, lin_gain, out_gain, attn_gain, rope, wv_qkv, wv_gate, wv_lo, wv_in, wv_ao, st_buf, p_out, p_in, acc, relay_in, rs_in, sq_x, y_x, a_x, q_x, pr_out, pr_in,
                k_buf, v_buf, o_s, q_s, kn_s, vn_s, ho_s,
                go_sem, in_sem, w_sem, st_sem, pair_sem, rs_sem, sq_sem, y_sem, a_sem, q_sem, pr_sem, kv_send, kv_recv, own_sem, kb_sem):
    chips, tp_size, rows, heads, head_dim, kv_dev, group, shard_len = dims
    sp_size = 2 * chips
    pairs = heads // 2
    width = heads * head_dim
    model = tok_in.shape[1]
    hidden_width = tp_size * width
    segments = group + 2
    qrows = kv_dev * group * rows

    me = lax.axis_index("sp")
    me_tp = lax.axis_index("tp")
    chip = me // 2
    core = lax.rem(me, 2)
    peers = [(dc, cr) for dc, cr in ((2, 0), (1, 0), (3, 0), (2, 1), (1, 1), (3, 1), (0, 1))]

    def peer_index(dc, cr):
        return lax.rem(chip + dc, chips) * 2 + (core if cr == 0 else 1 - core)

    barrier = pltpu.get_barrier_semaphore()
    for dc, cr in peers:
        pl.semaphore_signal(barrier, inc=1, device_id={"sp": peer_index(dc, cr)}, device_id_type=MESH)

    @pl.when(me_tp == 0)
    def _():
        pl.semaphore_wait(barrier, len(peers))
        for other in range(1, tp_size):
            pl.semaphore_signal(barrier, inc=1, device_id={"tp": other}, device_id_type=MESH)

    @pl.when(me_tp != 0)
    def _():
        pl.semaphore_wait(barrier, len(peers) + 1)
        pl.semaphore_signal(barrier, inc=1, device_id={"tp": 0}, device_id_type=MESH)

    def wait_for_tp():
        @pl.when(me_tp == 0)
        def _():
            pl.semaphore_wait(barrier, tp_size - 1)
            for other in range(1, tp_size):
                pl.semaphore_signal(go_sem, inc=1, device_id={"tp": other}, device_id_type=MESH)

        @pl.when(me_tp != 0)
        def _():
            pl.semaphore_wait(go_sem, 1)

    def remote(src, dst, send, recv, device):
        return pltpu.make_async_remote_copy(src_ref=src, dst_ref=dst, send_sem=send, recv_sem=recv, device_id=device, device_id_type=MESH)

    my_cols = pl.ds(pl.multiple_of(me * shard_len, LANES), shard_len)

    def kv_copies(round_idx):
        cache, land = ((k_in, k_land), (v_in, v_land))[round_idx % 2]
        row = round_idx // 2
        copies = []
        for n, (dc, cr) in enumerate(peers):
            dst = peer_index(dc, cr)
            copies.append(remote(cache.at[dst * rows + row], land.at[row, :, :, my_cols], kv_send.at[round_idx, n], kv_recv.at[round_idx, n], {"sp": dst}))
        return copies

    all_kv = []

    def start_round(round_idx):
        copies = kv_copies(round_idx)
        for copy in copies:
            copy.start()
        all_kv.extend(copies)

    start_round(0)

    def state_copy(step, slot):
        target_core = jnp.where(step < chips, 1 - core, core)
        dest = lax.rem(step, chips) * 2 + target_core
        return pltpu.make_async_copy(states.at[0, pl.ds(dest * rows, rows)], st_buf.at[slot], st_sem.at[slot])

    state_copy(0, 0).start()
    small_copies = [pltpu.make_async_copy(src, dst, in_sem.at[n]) for n, (src, dst) in enumerate(
        ((tok_in, tok), (lin_gain_in, lin_gain), (out_gain_in, out_gain), (attn_gain_in, attn_gain), (rope_in, rope)))]
    for copy in small_copies:
        copy.start()
    weight_copies = [pltpu.make_async_copy(src, dst, w_sem.at[n]) for n, (src, dst) in enumerate(
        ((w_qkv, wv_qkv), (w_gate, wv_gate), (w_lo, wv_lo), (w_in, wv_in), (w_ao, wv_ao)))]
    for copy in weight_copies:
        copy.start()

    lane = lax.broadcasted_iota(jnp.int32, (1, LANES), 1)
    low_half = lane < head_dim

    def pair_slope(p):
        return jnp.where(low_half, jnp.full((1, LANES), slopes[2 * p], F32), jnp.full((1, LANES), slopes[2 * p + 1], F32))

    offset = (shard_len * (sp_size - 1 - me)).astype(F32)
    decay = [jnp.exp(-pair_slope(p) * offset) for p in range(pairs)]

    def weigh_step(step, target):
        slot = lax.rem(step, 2)

        @pl.when(step + 1 < 2 * chips)
        def _():
            state_copy(step + 1, lax.rem(step + 1, 2)).start()

        state_copy(step, slot).wait()
        block = lax.rem(step, chips)
        for b in range(rows):
            for p in range(pairs):
                packed = jnp.concatenate([st_buf[slot, b, 2 * p], st_buf[slot, b, 2 * p + 1]], axis=1)
                target[block, b, p] = packed * decay[p]

    @pl.loop(0, chips)
    def _(step):
        weigh_step(step, p_out)

    pair_copy = remote(p_out, p_in, pair_sem.at[0], pair_sem.at[1], {"sp": chip * 2 + (1 - core)})
    pair_copy.start()

    @pl.loop(chips, 2 * chips)
    def _(step):
        weigh_step(step, acc)

    own_copies = [pltpu.make_async_copy(cache.at[pl.ds(me * rows, rows)], land.at[:, :, :, my_cols], own_sem.at[n])
                  for n, (cache, land) in enumerate(((k_in, k_land), (v_in, v_land)))]
    for copy in own_copies:
        copy.start()

    pair_copy.wait()

    @pl.loop(0, chips)
    def _(block):
        for b in range(rows):
            acc[block, b] = acc[block, b] + p_in[block, b]

    nexts = [(lax.rem(chip + dc, chips), {"sp": lax.rem(chip + dc, chips) * 2 + core}) for dc in (1, chips - 1)]
    far = lax.rem(chip + 2, chips)
    half = rows // 2
    parts = [pl.ds(0, half), pl.ds(half, half)]

    def rs_copy(n, src, dst, side):
        return remote(src, dst, rs_sem.at[0, n], rs_sem.at[1, n], nexts[side][1])

    relay_copies = [rs_copy(side, acc.at[far, parts[side]], relay_in.at[side], side) for side in range(2)]
    rs_copies = [rs_copy(2 + side, acc.at[nexts[side][0], parts[1 - side]], rs_in.at[side, parts[1 - side]], side) for side in range(2)]
    for copy in relay_copies + rs_copies:
        copy.start()
    start_round(1)

    def rms(vals):
        return vals * lax.rsqrt(jnp.mean(vals * vals, axis=-1, keepdims=True) + NORM_EPS)

    pad_rows = 8 - rows

    def pad8(vals):
        return jnp.concatenate([vals, jnp.zeros((pad_rows,) + vals.shape[1:], vals.dtype)], axis=0) if pad_rows else vals

    for copy in small_copies:
        copy.wait()
    tokens = pad8(tok[...].astype(F32))
    normed = (rms(tokens) * lin_gain[...]).astype(BF16)
    weight_copies[0].wait()

    def act(n):
        lin = jnp.dot(normed, wv_qkv[n], preferred_element_type=F32)
        return (lin * jax.nn.sigmoid(lin)).astype(BF16).astype(F32)

    query, key, value = act(0), act(1), act(2)
    weight_copies[1].wait()
    gate = jax.nn.sigmoid(jnp.dot(normed, wv_gate[...], preferred_element_type=F32))
    query_t = jnp.transpose(query)
    key_t = jnp.transpose(key)
    for side in range(2):
        relay_copies[side].wait()
        block = nexts[side][0]
        for b in range(half):
            acc[block, side * half + b] = acc[block, side * half + b] + relay_in[side, b]
        copy = rs_copy(4 + side, acc.at[block, parts[side]], rs_in.at[side, parts[side]], side)
        copy.start()
        rs_copies.append(copy)
    start_round(2)
    o_s[...] = jnp.zeros_like(o_s)

    def column(cols, p, b):
        lo = cols[2 * p * head_dim:(2 * p + 1) * head_dim, b:b + 1]
        hi = cols[(2 * p + 1) * head_dim:(2 * p + 2) * head_dim, b:b + 1]
        return jnp.where(low_half, lo, hi)

    for copy in rs_copies:
        copy.wait()

    for p in range(pairs):
        lam = jnp.exp(-pair_slope(p))
        cols = slice(p * LANES, (p + 1) * LANES)
        for b in range(rows):
            moved = acc[chip, b, p] + rs_in[0, b, p] + rs_in[1, b, p]
            state = lam * moved + column(key_t, p, b) * value[b:b + 1, cols]
            o_s[b:b + 1, cols] = jnp.sum(column(query_t, p, b) * state, axis=0, keepdims=True)
            st_out[b, 2 * p] = state[:, :head_dim]
            st_out[b, 2 * p + 1] = state[:, head_dim:]

    def tp_sum(buf, vals, sems):
        buf[me_tp] = vals
        copies = []
        for dt in (2, 1, 3)[-(tp_size - 1):]:
            copies.append(remote(buf.at[me_tp], buf.at[me_tp], sems.at[0, dt - 1], sems.at[1, dt - 1], {"tp": lax.rem(me_tp + dt, tp_size)}))
        for copy in copies:
            copy.start()
        for copy in copies:
            copy.wait()
        total = buf[0]
        for n in range(1, tp_size):
            total = total + buf[n]
        return total

    wait_for_tp()
    lin_attn = o_s[...]
    squares = jnp.broadcast_to(jnp.sum(lin_attn * lin_attn, axis=-1, keepdims=True), (8, LANES))
    square_sum = tp_sum(sq_x, squares, sq_sem)[:, :1]
    mixed = (lin_attn * lax.rsqrt(square_sum / hidden_width + NORM_EPS) * out_gain[...] * gate).astype(BF16)
    weight_copies[2].wait()
    lin_out = tp_sum(y_x, jnp.dot(mixed, wv_lo[...], preferred_element_type=F32), y_sem)
    hidden = (normed.astype(F32) + lin_out).astype(BF16).astype(F32)
    normed_two = (rms(hidden) * attn_gain[...]).astype(BF16)

    weight_copies[3].wait()
    proj = lax.dot_general(normed_two, wv_in[...], NT, preferred_element_type=F32).astype(BF16).astype(F32)
    cols_in = proj.shape[1]
    quarter = head_dim // 4
    rotated = proj * rope[0:1, :] + pltpu.roll(proj, quarter, 1) * rope[1:2, :] + pltpu.roll(proj, cols_in - quarter, 1) * rope[2:3, :]
    rotated = rotated.astype(BF16).astype(F32)

    def segment_at(kv, segment):
        start = (kv * segments + segment) * head_dim
        block = rotated[:, start // LANES * LANES:start // LANES * LANES + LANES]
        if start % LANES != kv * head_dim:
            block = pltpu.roll(block, head_dim, 1)
        return jnp.where(low_half if kv == 0 else ~low_half, block, 0.0)

    def packed_at(segment):
        return (segment_at(0, segment) + segment_at(1, segment))[:rows]

    key_rows, value_rows = packed_at(group), packed_at(group + 1)
    for i in range(group):
        q_s[i * rows:(i + 1) * rows, :] = packed_at(i)
        kn_s[i * rows:(i + 1) * rows, :] = key_rows
        vn_s[i * rows:(i + 1) * rows, :] = value_rows

    def spread(vals):
        return jnp.concatenate([jnp.where(low_half, vals, 0.0), jnp.where(low_half, 0.0, vals)], axis=0)

    q_x[me] = q_s[...].astype(BF16)
    q_copies = []
    for n, (dc, cr) in enumerate(peers):
        q_copies.append(remote(q_x.at[me], q_x.at[me], q_sem.at[0, n], q_sem.at[1, n], {"sp": peer_index(dc, cr)}))
    for copy in q_copies:
        copy.start()
    start_round(3)
    start_round(4)

    def shard_copies(j, slot):
        return [pltpu.make_async_copy(cache.at[pl.ds(j * rows, rows)], buf.at[slot], kb_sem.at[n, slot])
                for n, (cache, buf) in enumerate(((k_in, k_buf), (v_in, v_buf)))]

    for copy in shard_copies(0, 0):
        copy.start()

    rotated_t = jnp.transpose(rotated)
    lane16 = lax.broadcasted_iota(jnp.int32, (1, CACHE_EXTRA), 1)
    prompt_len = sp_size * shard_len
    for land, segment in ((k_land, group), (v_land, group + 1)):
        for kv in range(kv_dev):
            start = (kv * segments + segment) * head_dim
            for b in range(rows):
                tail = jnp.where(lane16 == 0, rotated_t[start:start + head_dim, b:b + 1], 0.0)
                land[b, kv, :, prompt_len:] = tail.astype(BF16)

    row_id = lax.broadcasted_iota(jnp.int32, (qrows, 1), 0)
    row_seq = lax.rem(row_id, rows)
    split = group * rows
    scale = head_dim ** -0.5

    for copy in q_copies:
        copy.wait()

    @pl.loop(0, sp_size)
    def _(j):
        slot = lax.rem(j, 2)

        @pl.when(j + 1 < sp_size)
        def _():
            for copy in shard_copies(j + 1, lax.rem(j + 1, 2)):
                copy.start()

        for copy in shard_copies(j, slot):
            copy.wait()
        queries = spread(q_x[j].astype(F32)).astype(BF16)
        scores = jnp.zeros((qrows, shard_len), F32)
        for b in range(rows):
            keys = k_buf[slot, b].reshape(kv_dev * head_dim, shard_len)
            scores = jnp.where(row_seq == b, jnp.dot(queries, keys, preferred_element_type=F32), scores)
        scores = scores * scale
        peak = jnp.max(scores, axis=-1, keepdims=True)
        probs = jnp.exp(scores - peak)
        total = jnp.sum(probs, axis=-1, keepdims=True)
        probs = probs.astype(BF16)
        out = jnp.zeros((qrows, LANES), F32)
        for b in range(rows):
            vals = v_buf[slot, b].reshape(kv_dev * head_dim, shard_len)
            out = jnp.where(row_seq == b, lax.dot_general(probs, vals, NT, preferred_element_type=F32), out)
        pr_out[j, :split] = jnp.where(low_half, out[:split], out[split:])
        stats = jnp.transpose(jnp.where(low_half, peak, total))
        stats = jnp.concatenate([stats[:4], stats[head_dim:head_dim + 4]], axis=0)
        pr_out[j, split:] = jnp.concatenate([stats, jnp.zeros((8, LANES - qrows), F32)], axis=1)

    pr_copies = []
    for n, (dc, cr) in enumerate(peers):
        dst = peer_index(dc, cr)
        pr_copies.append(remote(pr_out.at[dst], pr_in.at[me], pr_sem.at[0, n], pr_sem.at[1, n], {"sp": dst}))
    for copy in pr_copies:
        copy.start()
    for round_idx in range(5, 2 * rows):
        start_round(round_idx)
    pr_in[me] = pr_out[me]

    new_score = jnp.sum(spread(q_s[...] * kn_s[...]), axis=-1, keepdims=True) * scale

    for copy in pr_copies:
        copy.wait()
    stats = [jnp.transpose(pr_in[j, split:]) for j in range(sp_size)]
    peaks = [stat[:qrows, 0:1] for stat in stats]
    top = new_score
    for peak in peaks:
        top = jnp.maximum(top, peak)
    new_prob = jnp.exp(new_score - top)
    prob_sum = new_prob
    head = new_prob.astype(BF16).astype(F32) * spread(vn_s[...])
    for j in range(sp_size):
        weight = jnp.exp(peaks[j] - top)
        prob_sum = prob_sum + weight * stats[j][:qrows, 4:5]
        head = head + weight * spread(pr_in[j, :split])
    head = (head / prob_sum).astype(BF16).astype(F32)

    ho_s[...] = jnp.zeros_like(ho_s)
    for n in range(0, kv_dev * group, 2):
        block = None
        for m in (n, n + 1):
            kv = m // group
            piece = head[m * rows:(m + 1) * rows]
            if kv != m % 2:
                piece = pltpu.roll(piece, head_dim, 1)
            block = piece if block is None else block + piece
        ho_s[0:rows, n // 2 * LANES:(n // 2 + 1) * LANES] = block
    weight_copies[4].wait()
    attn_out = tp_sum(a_x, jnp.dot(ho_s[...].astype(BF16), wv_ao[...], preferred_element_type=F32), a_sem)
    hid_out[...] = (normed_two.astype(F32) + attn_out).astype(BF16)[:rows]

    for copy in own_copies:
        copy.wait()
    for copy in all_kv:
        copy.wait()


def put_kernel(*refs):
    count = (len(refs) - 1) // 2
    sems = refs[-1]
    copies = []
    for n in (2, 3, 1, 0):
        pieces = refs[n].shape[0] if n > 0 else 1
        for i in range(pieces):
            src, dst = (refs[n].at[i], refs[count + n].at[i]) if pieces > 1 else (refs[n], refs[count + n])
            copies.append(pltpu.make_async_copy(src, dst, sems.at[len(copies)]))
    for copy in copies:
        copy.start()
    for copy in copies:
        copy.wait()


def solution(mesh):
    sp_size = mesh.shape['sp']
    tp_size = mesh.shape['tp']
    chips = sp_size // 2

    def device_step(tokens, states, k_cache, v_cache, slopes, lin_gain, w_lin_qkv, w_lin_gate, out_gain, w_lin_out, attn_gain, w_attn_in, w_attn_out):
        rows, model = tokens.shape
        kv_dev, shard_len, head_dim = k_cache.shape[1:]
        heads = slopes.shape[0]
        segments = w_attn_in.shape[2]
        group = segments - 2
        width = heads * head_dim
        pairs = heads // 2
        cols_in = kv_dev * segments * head_dim
        qrows = kv_dev * group * rows
        prompt_len = sp_size * shard_len
        full_len = prompt_len + CACHE_EXTRA
        dims = (chips, tp_size, rows, heads, head_dim, kv_dev, group, shard_len)
        rope = jnp.asarray(rope_tables(kv_dev, segments, group, head_dim, prompt_len))

        vmem = pl.BlockSpec(memory_space=pltpu.VMEM)
        smem = pl.BlockSpec(memory_space=pltpu.SMEM)
        anym = pl.BlockSpec(memory_space=pl.ANY)
        dma = pltpu.SemaphoreType.DMA
        land_shape = (rows, kv_dev, head_dim, full_len)
        out_types = [((rows, model), BF16), ((rows, heads, head_dim, head_dim), F32), (land_shape, BF16), (land_shape, BF16)]
        scratch = [
            pltpu.VMEM((rows, model), BF16),
            pltpu.VMEM((1, model), F32),
            pltpu.VMEM((1, width), F32),
            pltpu.VMEM((1, model), F32),
            pltpu.VMEM((8, cols_in), F32),
            pltpu.VMEM((3, model, width), BF16),
            pltpu.VMEM((model, width), BF16),
            pltpu.VMEM((width, model), BF16),
            pltpu.VMEM((cols_in, model), BF16),
            pltpu.VMEM((width, model), BF16),
            pltpu.VMEM((2, rows, heads, head_dim, head_dim), F32),
            pltpu.VMEM((chips, rows, pairs, head_dim, LANES), F32),
            pltpu.VMEM((chips, rows, pairs, head_dim, LANES), F32),
            pltpu.VMEM((chips, rows, pairs, head_dim, LANES), F32),
            pltpu.VMEM((2, rows // 2, pairs, head_dim, LANES), F32),
            pltpu.VMEM((2, rows, pairs, head_dim, LANES), F32),
            pltpu.VMEM((tp_size, 8, LANES), F32),
            pltpu.VMEM((tp_size, 8, model), F32),
            pltpu.VMEM((tp_size, 8, model), F32),
            pltpu.VMEM((sp_size, group * rows, LANES), BF16),
            pltpu.VMEM((sp_size, group * rows + 8, LANES), F32),
            pltpu.VMEM((sp_size, group * rows + 8, LANES), F32),
            pltpu.VMEM((2, rows, kv_dev, head_dim, shard_len), BF16),
            pltpu.VMEM((2, rows, kv_dev, head_dim, shard_len), BF16),
            pltpu.VMEM((8, width), F32),
            pltpu.VMEM((group * rows, LANES), F32),
            pltpu.VMEM((group * rows, LANES), F32),
            pltpu.VMEM((group * rows, LANES), F32),
            pltpu.VMEM((8, width), F32),
            pltpu.SemaphoreType.REGULAR,
            dma((5,)),
            dma((5,)),
            dma((2,)),
            dma((2,)),
            dma((2, 6)),
            dma((2, tp_size - 1)),
            dma((2, tp_size - 1)),
            dma((2, tp_size - 1)),
            dma((2, sp_size - 1)),
            dma((2, sp_size - 1)),
            dma((2 * rows, sp_size - 1)),
            dma((2 * rows, sp_size - 1)),
            dma((2,)),
            dma((2, 2)),
        ]
        landed = pl.pallas_call(
            functools.partial(step_kernel, dims),
            out_shape=[pltpu.VMEM(shape, dtype) for shape, dtype in out_types],
            in_specs=[anym, smem, anym, anym, anym, anym] + [anym] * 8,
            out_specs=[vmem] * 4,
            scratch_shapes=scratch,
            compiler_params=pltpu.CompilerParams(collective_id=0, has_side_effects=True, vmem_limit_bytes=40 * 2 ** 20),
        )(
            tokens, slopes, lin_gain.reshape(1, -1), out_gain.reshape(1, -1), attn_gain.reshape(1, -1), rope,
            states, jnp.transpose(k_cache, (0, 1, 3, 2)), jnp.transpose(v_cache, (0, 1, 3, 2)),
            jnp.transpose(w_lin_qkv, (1, 0, 2)), w_lin_gate, w_lin_out,
            jnp.transpose(w_attn_in, (1, 2, 3, 0)).reshape(cols_in, model), w_attn_out,
        )
        hidden_out, state_new, k_out, v_out = pl.pallas_call(
            put_kernel,
            out_shape=[jax.ShapeDtypeStruct(shape, dtype) for shape, dtype in out_types],
            in_specs=[vmem] * 4,
            out_specs=[anym] * 4,
            scratch_shapes=[dma((3 * rows + 1,))],
            compiler_params=pltpu.CompilerParams(vmem_limit_bytes=2 * 2 ** 20),
        )(*landed)
        return hidden_out, state_new, jnp.transpose(k_out, (0, 1, 3, 2)), jnp.transpose(v_out, (0, 1, 3, 2))

    batch_spec = P(('dp', 'sp'), None)
    head_spec = P(('dp', 'sp'), 'tp', None, None)
    cache_spec = P('dp', 'tp', 'sp', None)
    in_specs = (batch_spec, P('sp', 'dp', 'tp', None, None), cache_spec, cache_spec, P('tp'), P(None), P(None, None, 'tp'), P(None, 'tp'), P('tp'), P('tp', None), P(None), P(None, 'tp', None, None), P('tp', None))
    out_specs = (batch_spec, head_spec, head_spec, head_spec)
    return jax.shard_map(device_step, mesh=mesh, in_specs=in_specs, out_specs=out_specs, check_vma=False)
```

```python
import functools

import numpy as np

import jax
import jax.numpy as jnp
from jax import lax
from jax.experimental import pallas as pl
from jax.experimental.pallas import tpu as pltpu
from jax.sharding import PartitionSpec as P

NORM_EPS = 1e-6
ROPE_BASE = 10000000.0
CACHE_EXTRA = 16
LANES = 128
F32 = jnp.float32
BF16 = jnp.bfloat16
MESH = pl.DeviceIdType.MESH
NT = (((1,), (1,)), ((), ()))


def rope_tables(kv_dev, segments, group, head_dim, position):
    rope_dim = head_dim // 2
    half = rope_dim // 2
    exponents = -np.arange(0, rope_dim, 2, dtype=np.float32) / np.float32(rope_dim)
    angles = (np.float32(position) * np.float32(ROPE_BASE) ** exponents).astype(np.float32)
    cosine, sine = np.cos(angles), np.sin(angles)
    table = np.zeros((8, kv_dev, segments, head_dim), np.float32)
    table[0] = 1.0
    for segment in range(group + 1):
        table[0, :, segment, :half] = cosine
        table[0, :, segment, half:rope_dim] = cosine
        table[1, :, segment, half:rope_dim] = sine
        table[2, :, segment, :half] = -sine
    return table.reshape(8, kv_dev * segments * head_dim)


def step_kernel(dims, tok_in, slopes_in, lin_gain_in, out_gain_in, attn_gain_in, rope_in, states, k_in, v_in, w_qkv, w_gate, w_lo, w_in, w_ao,
                hid_out, st_out, k_land, v_land,
                slopes, tok, lin_gain, out_gain, attn_gain, rope, wv_qkv, wv_gate, wv_lo, wv_in, wv_ao, st_buf, p_out, p_in, acc, relay_in, rs_in, sq_x, y_x, a_x, q_x, pr_out, pr_pair, pr_mine, pr_in,
                k_buf, v_buf, o_s, q_s, kn_s, vn_s, ho_s,
                go_sem, pair_sem, rs_sem, sq_sem, y_sem, a_sem, q_sem, pr_sem, kv_send, kv_recv):
    chips, tp_size, rows, heads, head_dim, kv_dev, group, shard_len = dims
    sp_size = 2 * chips
    pairs = heads // 2
    width = heads * head_dim
    model = tok_in.shape[1]
    hidden_width = tp_size * width
    segments = group + 2
    qrows = kv_dev * group * rows

    me = lax.axis_index("sp")
    me_tp = lax.axis_index("tp")
    chip = me // 2
    core = lax.rem(me, 2)
    peers = [(dc, cr) for dc, cr in ((2, 0), (1, 0), (3, 0), (2, 1), (1, 1), (3, 1), (0, 1))]

    def peer_index(dc, cr):
        return lax.rem(chip + dc, chips) * 2 + (core if cr == 0 else 1 - core)

    barrier = pltpu.get_barrier_semaphore()
    for dc, cr in peers:
        pl.semaphore_signal(barrier, inc=1, device_id={"sp": peer_index(dc, cr)}, device_id_type=MESH)

    @pl.when(me_tp == 0)
    def _():
        pl.semaphore_wait(barrier, len(peers))
        for other in range(1, tp_size):
            pl.semaphore_signal(barrier, inc=1, device_id={"tp": other}, device_id_type=MESH)

    @pl.when(me_tp != 0)
    def _():
        pl.semaphore_wait(barrier, len(peers) + 1)
        pl.semaphore_signal(barrier, inc=1, device_id={"tp": 0}, device_id_type=MESH)

    def wait_for_tp():
        @pl.when(me_tp == 0)
        def _():
            pl.semaphore_wait(barrier, tp_size - 1)
            for other in range(1, tp_size):
                pl.semaphore_signal(go_sem, inc=1, device_id={"tp": other}, device_id_type=MESH)

        @pl.when(me_tp != 0)
        def _():
            pl.semaphore_wait(go_sem, 1)

    def remote(src, dst, send, recv, device):
        return pltpu.make_async_remote_copy(src_ref=src, dst_ref=dst, send_sem=send, recv_sem=recv, device_id=device, device_id_type=MESH)

    partner = {"sp": chip * 2 + (1 - core)}
    my_cols = pl.ds(pl.multiple_of(me * shard_len, LANES), shard_len)

    def kv_copies(round_idx):
        cache, land = ((k_in, k_land), (v_in, v_land))[round_idx % 2]
        row = round_idx // 2
        copies = []
        for n, (dc, cr) in enumerate(peers):
            dst = peer_index(dc, cr)
            copies.append(remote(cache.at[dst * rows + row], land.at[row, :, :, my_cols], kv_send.at[round_idx % 2], kv_recv.at[round_idx % 2], {"sp": dst}))
        return copies

    def start_round(round_idx):
        for copy in kv_copies(round_idx):
            copy.start()

    def total_of(ref, sems):
        return remote(ref, ref, sems[0], sems[1], partner)

    start_round(0)

    def decode_step(in_sem, w_sem, st_sem, own_sem, kb_sem):
        def state_copy(step, slot):
            target_core = jnp.where(step < chips, 1 - core, core)
            dest = lax.rem(step, chips) * 2 + target_core
            return pltpu.make_async_copy(states.at[0, pl.ds(dest * rows, rows)], st_buf.at[slot], st_sem.at[slot])

        slope_copy = pltpu.make_async_copy(slopes_in, slopes, in_sem.at[5])
        slope_copy.start()
        state_copy(0, 0).start()
        small_copies = [pltpu.make_async_copy(src, dst, in_sem.at[n]) for n, (src, dst) in enumerate(
            ((tok_in, tok), (lin_gain_in, lin_gain), (out_gain_in, out_gain), (attn_gain_in, attn_gain), (rope_in, rope)))]
        for copy in small_copies:
            copy.start()
        weight_copies = [pltpu.make_async_copy(src, dst, w_sem.at[n]) for n, (src, dst) in enumerate(
            ((w_qkv, wv_qkv), (w_gate, wv_gate), (w_lo, wv_lo), (w_in, wv_in), (w_ao, wv_ao)))]
        for copy in weight_copies:
            copy.start()

        lane = lax.broadcasted_iota(jnp.int32, (1, LANES), 1)
        low_half = lane < head_dim

        def pair_slope(p):
            return jnp.where(low_half, jnp.full((1, LANES), slopes[2 * p], F32), jnp.full((1, LANES), slopes[2 * p + 1], F32))

        slope_copy.wait()
        offset = (shard_len * (sp_size - 1 - me)).astype(F32)
        decay = [jnp.exp(-pair_slope(p) * offset) for p in range(pairs)]

        def weigh_step(step, target):
            slot = lax.rem(step, 2)

            @pl.when(step + 1 < 2 * chips)
            def _():
                state_copy(step + 1, lax.rem(step + 1, 2)).start()

            state_copy(step, slot).wait()
            block = lax.rem(step, chips)
            for b in range(rows):
                for p in range(pairs):
                    packed = jnp.concatenate([st_buf[slot, b, 2 * p], st_buf[slot, b, 2 * p + 1]], axis=1)
                    target[block, b, p] = packed * decay[p]

        @pl.loop(0, chips)
        def _(step):
            weigh_step(step, p_out)

        pair_copy = remote(p_out, p_in, pair_sem.at[0], pair_sem.at[1], partner)
        pair_copy.start()

        @pl.loop(chips, 2 * chips)
        def _(step):
            weigh_step(step, acc)

        own_copies = [pltpu.make_async_copy(cache.at[pl.ds(me * rows, rows)], land.at[:, :, :, my_cols], own_sem.at[n])
                      for n, (cache, land) in enumerate(((k_in, k_land), (v_in, v_land)))]
        for copy in own_copies:
            copy.start()

        pair_copy.wait()

        @pl.loop(0, chips)
        def _(block):
            for b in range(rows):
                acc[block, b] = acc[block, b] + p_in[block, b]

        nexts = [(lax.rem(chip + dc, chips), {"sp": lax.rem(chip + dc, chips) * 2 + core}) for dc in (1, chips - 1)]
        far = lax.rem(chip + 2, chips)
        half = rows // 2
        parts = [pl.ds(0, half), pl.ds(half, half)]

        def rs_copy(n, src, dst, side):
            return remote(src, dst, rs_sem.at[n], rs_sem.at[n + 1], nexts[side][1])

        relay_copies = [rs_copy(0, acc.at[far, parts[side]], relay_in.at[side], side) for side in range(2)]
        rs_copies = [rs_copy(2, acc.at[nexts[side][0], parts[1 - side]], rs_in.at[side, parts[1 - side]], side) for side in range(2)]
        for copy in relay_copies + rs_copies:
            copy.start()
        start_round(1)

        def rms(vals):
            return vals * lax.rsqrt(jnp.mean(vals * vals, axis=-1, keepdims=True) + NORM_EPS)

        pad_rows = 8 - rows

        def pad8(vals):
            return jnp.concatenate([vals, jnp.zeros((pad_rows,) + vals.shape[1:], vals.dtype)], axis=0) if pad_rows else vals

        for copy in small_copies:
            copy.wait()
        tokens = pad8(tok[...].astype(F32))
        normed = (rms(tokens) * lin_gain[...]).astype(BF16)
        weight_copies[0].wait()

        def act(n):
            lin = jnp.dot(normed, wv_qkv[n], preferred_element_type=F32)
            return (lin * jax.nn.sigmoid(lin)).astype(BF16).astype(F32)

        query, key, value = act(0), act(1), act(2)
        weight_copies[1].wait()
        gate = jax.nn.sigmoid(jnp.dot(normed, wv_gate[...], preferred_element_type=F32))
        query_t = jnp.transpose(query)
        key_t = jnp.transpose(key)
        total_of(relay_in, (rs_sem.at[0], rs_sem.at[1])).wait()
        for side in range(2):
            block = nexts[side][0]
            for b in range(half):
                acc[block, side * half + b] = acc[block, side * half + b] + relay_in[side, b]
            rs_copy(2, acc.at[block, parts[side]], rs_in.at[side, parts[side]], side).start()
        start_round(2)
        o_s[...] = jnp.zeros_like(o_s)

        def column(cols, p, b):
            lo = cols[2 * p * head_dim:(2 * p + 1) * head_dim, b:b + 1]
            hi = cols[(2 * p + 1) * head_dim:(2 * p + 2) * head_dim, b:b + 1]
            return jnp.where(low_half, lo, hi)

        total_of(rs_in, (rs_sem.at[2], rs_sem.at[3])).wait()

        for p in range(pairs):
            lam = jnp.exp(-pair_slope(p))
            cols = slice(p * LANES, (p + 1) * LANES)
            for b in range(rows):
                moved = acc[chip, b, p] + rs_in[0, b, p] + rs_in[1, b, p]
                state = lam * moved + column(key_t, p, b) * value[b:b + 1, cols]
                o_s[b:b + 1, cols] = jnp.sum(column(query_t, p, b) * state, axis=0, keepdims=True)
                st_out[b, 2 * p] = state[:, :head_dim]
                st_out[b, 2 * p + 1] = state[:, head_dim:]

        def tp_sum(buf, vals, sems):
            buf[me_tp] = vals
            copies = []
            for dt in (2, 1, 3)[-(tp_size - 1):]:
                copies.append(remote(buf.at[me_tp], buf.at[me_tp], sems.at[0], sems.at[1], {"tp": lax.rem(me_tp + dt, tp_size)}))
            for copy in copies:
                copy.start()
            total_of(buf.at[pl.ds(0, len(copies))], (sems.at[0], sems.at[1])).wait()
            total = buf[0]
            for n in range(1, tp_size):
                total = total + buf[n]
            return total

        wait_for_tp()
        lin_attn = o_s[...]
        squares = jnp.broadcast_to(jnp.sum(lin_attn * lin_attn, axis=-1, keepdims=True), (8, LANES))
        square_sum = tp_sum(sq_x, squares, sq_sem)[:, :1]
        mixed = (lin_attn * lax.rsqrt(square_sum / hidden_width + NORM_EPS) * out_gain[...] * gate).astype(BF16)
        weight_copies[2].wait()
        lin_out = tp_sum(y_x, jnp.dot(mixed, wv_lo[...], preferred_element_type=F32), y_sem)
        hidden = (normed.astype(F32) + lin_out).astype(BF16).astype(F32)
        normed_two = (rms(hidden) * attn_gain[...]).astype(BF16)

        weight_copies[3].wait()
        proj = lax.dot_general(normed_two, wv_in[...], NT, preferred_element_type=F32).astype(BF16).astype(F32)
        cols_in = proj.shape[1]
        quarter = head_dim // 4
        rotated = proj * rope[0:1, :] + pltpu.roll(proj, quarter, 1) * rope[1:2, :] + pltpu.roll(proj, cols_in - quarter, 1) * rope[2:3, :]
        rotated = rotated.astype(BF16).astype(F32)

        def segment_at(kv, segment):
            start = (kv * segments + segment) * head_dim
            block = rotated[:, start // LANES * LANES:start // LANES * LANES + LANES]
            if start % LANES != kv * head_dim:
                block = pltpu.roll(block, head_dim, 1)
            return jnp.where(low_half if kv == 0 else ~low_half, block, 0.0)

        def packed_at(segment):
            return (segment_at(0, segment) + segment_at(1, segment))[:rows]

        key_rows, value_rows = packed_at(group), packed_at(group + 1)
        for i in range(group):
            q_s[i * rows:(i + 1) * rows, :] = packed_at(i)
            kn_s[i * rows:(i + 1) * rows, :] = key_rows
            vn_s[i * rows:(i + 1) * rows, :] = value_rows

        def spread(vals):
            return jnp.concatenate([jnp.where(low_half, vals, 0.0), jnp.where(low_half, 0.0, vals)], axis=0)

        q_x[me] = q_s[...].astype(BF16)
        for dc in (2, 1, 3):
            remote(q_x.at[me], q_x.at[me], q_sem.at[0], q_sem.at[1], {"sp": peer_index(dc, 0)}).start()
        remote(q_x.at[me], q_x.at[me], q_sem.at[2], q_sem.at[3], partner).start()
        start_round(3)
        start_round(4)

        def shard_copies(j, slot):
            return [pltpu.make_async_copy(cache.at[pl.ds(j * rows, rows)], buf.at[slot], kb_sem.at[n, slot])
                    for n, (cache, buf) in enumerate(((k_in, k_buf), (v_in, v_buf)))]

        for copy in shard_copies(0, 0):
            copy.start()

        rotated_t = jnp.transpose(rotated)
        lane16 = lax.broadcasted_iota(jnp.int32, (1, CACHE_EXTRA), 1)
        prompt_len = sp_size * shard_len
        for land, segment in ((k_land, group), (v_land, group + 1)):
            for kv in range(kv_dev):
                start = (kv * segments + segment) * head_dim
                for b in range(rows):
                    tail = jnp.where(lane16 == 0, rotated_t[start:start + head_dim, b:b + 1], 0.0)
                    land[b, kv, :, prompt_len:] = tail.astype(BF16)

        row_id = lax.broadcasted_iota(jnp.int32, (qrows, 1), 0)
        row_seq = lax.rem(row_id, rows)
        split = group * rows
        scale = head_dim ** -0.5

        total_of(q_x.at[pl.ds(0, chips - 1)], (q_sem.at[0], q_sem.at[1])).wait()
        for dc in (2, 1, 3):
            src = peer_index(dc, 0)
            remote(q_x.at[src], q_x.at[src], q_sem.at[2], q_sem.at[3], partner).start()
        total_of(q_x.at[pl.ds(0, chips)], (q_sem.at[2], q_sem.at[3])).wait()

        def write_partial(ref, out, peak, total):
            ref[:split] = out
            stats = jnp.transpose(jnp.where(low_half, peak, total))
            stats = jnp.concatenate([stats[:4], stats[head_dim:head_dim + 4]], axis=0)
            ref[split:] = jnp.concatenate([stats, jnp.zeros((8, LANES - qrows), F32)], axis=1)

        def read_partial(ref):
            stats = jnp.transpose(ref[split:])
            return ref[:split], stats[:qrows, 0:1], stats[:qrows, 4:5]

        def both_heads(column_vals):
            return jnp.where(low_half, column_vals[:split], column_vals[split:])

        @pl.loop(0, sp_size)
        def _(j):
            slot = lax.rem(j, 2)

            @pl.when(j + 1 < sp_size)
            def _():
                for copy in shard_copies(j + 1, lax.rem(j + 1, 2)):
                    copy.start()

            for copy in shard_copies(j, slot):
                copy.wait()
            queries = spread(q_x[j].astype(F32)).astype(BF16)
            scores = jnp.zeros((qrows, shard_len), F32)
            for b in range(rows):
                keys = k_buf[slot, b].reshape(kv_dev * head_dim, shard_len)
                scores = jnp.where(row_seq == b, jnp.dot(queries, keys, preferred_element_type=F32), scores)
            scores = scores * scale
            peak = jnp.max(scores, axis=-1, keepdims=True)
            probs = jnp.exp(scores - peak)
            total = jnp.sum(probs, axis=-1, keepdims=True)
            probs = probs.astype(BF16)
            out = jnp.zeros((qrows, LANES), F32)
            for b in range(rows):
                vals = v_buf[slot, b].reshape(kv_dev * head_dim, shard_len)
                out = jnp.where(row_seq == b, lax.dot_general(probs, vals, NT, preferred_element_type=F32), out)
            write_partial(pr_out.at[lax.rem(j, 2), j // 2], both_heads(out), peak, total)

        pr_swap = remote(pr_out.at[1 - core], pr_pair, pr_sem.at[0], pr_sem.at[1], partner)
        pr_swap.start()
        pr_swap.wait()

        @pl.loop(0, chips)
        def _(block):
            out_a, peak_a, total_a = read_partial(pr_out.at[core, block])
            out_b, peak_b, total_b = read_partial(pr_pair.at[block])
            peak = jnp.maximum(peak_a, peak_b)
            scale_a, scale_b = jnp.exp(peak_a - peak), jnp.exp(peak_b - peak)
            write_partial(pr_mine.at[block], out_a * both_heads(scale_a) + out_b * both_heads(scale_b), peak, total_a * scale_a + total_b * scale_b)

        for dc in (2, 1, 3):
            dst_chip = lax.rem(chip + dc, chips)
            remote(pr_mine.at[dst_chip], pr_in.at[chip], pr_sem.at[2], pr_sem.at[3], {"sp": dst_chip * 2 + core}).start()
        for round_idx in range(5, 2 * rows):
            start_round(round_idx)
        pr_in[chip] = pr_mine[chip]

        new_score = jnp.sum(spread(q_s[...] * kn_s[...]), axis=-1, keepdims=True) * scale

        total_of(pr_in.at[pl.ds(0, chips - 1)], (pr_sem.at[2], pr_sem.at[3])).wait()
        partials = [read_partial(pr_in.at[n]) for n in range(chips)]
        top = new_score
        for _, peak, _ in partials:
            top = jnp.maximum(top, peak)
        new_prob = jnp.exp(new_score - top)
        prob_sum = new_prob
        head = new_prob.astype(BF16).astype(F32) * spread(vn_s[...])
        for out, peak, total in partials:
            weight = jnp.exp(peak - top)
            prob_sum = prob_sum + weight * total
            head = head + weight * spread(out)
        head = (head / prob_sum).astype(BF16).astype(F32)

        ho_s[...] = jnp.zeros_like(ho_s)
        for n in range(0, kv_dev * group, 2):
            block = None
            for m in (n, n + 1):
                kv = m // group
                piece = head[m * rows:(m + 1) * rows]
                if kv != m % 2:
                    piece = pltpu.roll(piece, head_dim, 1)
                block = piece if block is None else block + piece
            ho_s[0:rows, n // 2 * LANES:(n // 2 + 1) * LANES] = block
        weight_copies[4].wait()
        attn_out = tp_sum(a_x, jnp.dot(ho_s[...].astype(BF16), wv_ao[...], preferred_element_type=F32), a_sem)
        hid_out[...] = (normed_two.astype(F32) + attn_out).astype(BF16)[:rows]

        for copy in own_copies:
            copy.wait()
        for n, cache in enumerate((k_in, v_in)):
            total_of(cache.at[pl.ds(0, len(peers) * rows)], (kv_send.at[n], kv_recv.at[n])).wait()

    dma = pltpu.SemaphoreType.DMA
    pl.run_scoped(decode_step, dma((6,)), dma((5,)), dma((2,)), dma((2,)), dma((2, 2)))


def put_kernel(*refs):
    count = (len(refs) - 1) // 2
    sems = refs[-1]
    copies = []
    for n in (2, 3, 1, 0):
        pieces = refs[n].shape[0] if n > 0 else 1
        for i in range(pieces):
            src, dst = (refs[n].at[i], refs[count + n].at[i]) if pieces > 1 else (refs[n], refs[count + n])
            copies.append(pltpu.make_async_copy(src, dst, sems.at[len(copies)]))
    for copy in copies:
        copy.start()
    for copy in copies:
        copy.wait()


def solution(mesh):
    sp_size = mesh.shape['sp']
    tp_size = mesh.shape['tp']
    chips = sp_size // 2

    def device_step(tokens, states, k_cache, v_cache, slopes, lin_gain, w_lin_qkv, w_lin_gate, out_gain, w_lin_out, attn_gain, w_attn_in, w_attn_out):
        rows, model = tokens.shape
        kv_dev, shard_len, head_dim = k_cache.shape[1:]
        heads = slopes.shape[0]
        segments = w_attn_in.shape[2]
        group = segments - 2
        width = heads * head_dim
        pairs = heads // 2
        cols_in = kv_dev * segments * head_dim
        qrows = kv_dev * group * rows
        prompt_len = sp_size * shard_len
        full_len = prompt_len + CACHE_EXTRA
        dims = (chips, tp_size, rows, heads, head_dim, kv_dev, group, shard_len)
        rope = jnp.asarray(rope_tables(kv_dev, segments, group, head_dim, prompt_len))

        vmem = pl.BlockSpec(memory_space=pltpu.VMEM)
        anym = pl.BlockSpec(memory_space=pl.ANY)
        dma = pltpu.SemaphoreType.DMA
        land_shape = (rows, kv_dev, head_dim, full_len)
        out_types = [((rows, model), BF16), ((rows, heads, head_dim, head_dim), F32), (land_shape, BF16), (land_shape, BF16)]
        scratch = [
            pltpu.SMEM((heads,), F32),
            pltpu.VMEM((rows, model), BF16),
            pltpu.VMEM((1, model), F32),
            pltpu.VMEM((1, width), F32),
            pltpu.VMEM((1, model), F32),
            pltpu.VMEM((8, cols_in), F32),
            pltpu.VMEM((3, model, width), BF16),
            pltpu.VMEM((model, width), BF16),
            pltpu.VMEM((width, model), BF16),
            pltpu.VMEM((cols_in, model), BF16),
            pltpu.VMEM((width, model), BF16),
            pltpu.VMEM((2, rows, heads, head_dim, head_dim), F32),
            pltpu.VMEM((chips, rows, pairs, head_dim, LANES), F32),
            pltpu.VMEM((chips, rows, pairs, head_dim, LANES), F32),
            pltpu.VMEM((chips, rows, pairs, head_dim, LANES), F32),
            pltpu.VMEM((2, rows // 2, pairs, head_dim, LANES), F32),
            pltpu.VMEM((2, rows, pairs, head_dim, LANES), F32),
            pltpu.VMEM((tp_size, 8, LANES), F32),
            pltpu.VMEM((tp_size, 8, model), F32),
            pltpu.VMEM((tp_size, 8, model), F32),
            pltpu.VMEM((sp_size, group * rows, LANES), BF16),
            pltpu.VMEM((2, chips, group * rows + 8, LANES), F32),
            pltpu.VMEM((chips, group * rows + 8, LANES), F32),
            pltpu.VMEM((chips, group * rows + 8, LANES), F32),
            pltpu.VMEM((chips, group * rows + 8, LANES), F32),
            pltpu.VMEM((2, rows, kv_dev, head_dim, shard_len), BF16),
            pltpu.VMEM((2, rows, kv_dev, head_dim, shard_len), BF16),
            pltpu.VMEM((8, width), F32),
            pltpu.VMEM((group * rows, LANES), F32),
            pltpu.VMEM((group * rows, LANES), F32),
            pltpu.VMEM((group * rows, LANES), F32),
            pltpu.VMEM((8, width), F32),
            pltpu.SemaphoreType.REGULAR,
            dma((2,)),
            dma((4,)),
            dma((2,)),
            dma((2,)),
            dma((2,)),
            dma((4,)),
            dma((4,)),
            dma((2,)),
            dma((2,)),
        ]
        landed = pl.pallas_call(
            functools.partial(step_kernel, dims),
            out_shape=[pltpu.VMEM(shape, dtype) for shape, dtype in out_types],
            in_specs=[anym, anym, anym, anym, anym, anym] + [anym] * 8,
            out_specs=[vmem] * 4,
            scratch_shapes=scratch,
            compiler_params=pltpu.CompilerParams(collective_id=0, has_side_effects=True, vmem_limit_bytes=40 * 2 ** 20),
        )(
            tokens, slopes, lin_gain.reshape(1, -1), out_gain.reshape(1, -1), attn_gain.reshape(1, -1), rope,
            states, jnp.transpose(k_cache, (0, 1, 3, 2)), jnp.transpose(v_cache, (0, 1, 3, 2)),
            jnp.transpose(w_lin_qkv, (1, 0, 2)), w_lin_gate, w_lin_out,
            jnp.transpose(w_attn_in, (1, 2, 3, 0)).reshape(cols_in, model), w_attn_out,
        )
        hidden_out, state_new, k_out, v_out = pl.pallas_call(
            put_kernel,
            out_shape=[jax.ShapeDtypeStruct(shape, dtype) for shape, dtype in out_types],
            in_specs=[vmem] * 4,
            out_specs=[anym] * 4,
            scratch_shapes=[dma((3 * rows + 1,))],
            compiler_params=pltpu.CompilerParams(vmem_limit_bytes=2 * 2 ** 20),
        )(*landed)
        return hidden_out, state_new, jnp.transpose(k_out, (0, 1, 3, 2)), jnp.transpose(v_out, (0, 1, 3, 2))

    batch_spec = P(('dp', 'sp'), None)
    head_spec = P(('dp', 'sp'), 'tp', None, None)
    cache_spec = P('dp', 'tp', 'sp', None)
    in_specs = (batch_spec, P('sp', 'dp', 'tp', None, None), cache_spec, cache_spec, P('tp'), P(None), P(None, None, 'tp'), P(None, 'tp'), P('tp'), P('tp', None), P(None), P(None, 'tp', None, None), P('tp', None))
    out_specs = (batch_spec, head_spec, head_spec, head_spec)
    return jax.shard_map(device_step, mesh=mesh, in_specs=in_specs, out_specs=out_specs, check_vma=False)
```

```python
import functools

import numpy as np

import jax
import jax.numpy as jnp
from jax import lax
from jax.experimental import pallas as pl
from jax.experimental.pallas import tpu as pltpu
from jax.sharding import PartitionSpec as P

NORM_EPS = 1e-6
ROPE_BASE = 10000000.0
CACHE_EXTRA = 16
LANES = 128
F32 = jnp.float32
BF16 = jnp.bfloat16
MESH = pl.DeviceIdType.MESH
NT = (((1,), (1,)), ((), ()))


def rope_tables(kv_dev, segments, group, head_dim, position):
    rope_dim = head_dim // 2
    half = rope_dim // 2
    exponents = -np.arange(0, rope_dim, 2, dtype=np.float32) / np.float32(rope_dim)
    angles = (np.float32(position) * np.float32(ROPE_BASE) ** exponents).astype(np.float32)
    cosine, sine = np.cos(angles), np.sin(angles)
    table = np.zeros((8, kv_dev, segments, head_dim), np.float32)
    table[0] = 1.0
    for segment in range(group + 1):
        table[0, :, segment, :half] = cosine
        table[0, :, segment, half:rope_dim] = cosine
        table[1, :, segment, half:rope_dim] = sine
        table[2, :, segment, :half] = -sine
    return table.reshape(8, kv_dev * segments * head_dim)


def step_kernel(dims, tok_in, slopes_in, lin_gain_in, out_gain_in, attn_gain_in, rope_in, states, k_in, v_in, w_qkv, w_gate, w_lo, w_in, w_ao,
                hid_out, st_out, k_land, v_land, k_swap, v_swap,
                slopes, tok, lin_gain, out_gain, attn_gain, rope, wv_qkv, wv_gate, wv_lo, wv_in, wv_ao, st_buf, p_out, p_in, acc, relay_in, rs_in, sq_x, y_x, a_x, q_x, pr_out, pr_pair, pr_mine, pr_in,
                k_buf, v_buf, o_s, q_s, kn_s, vn_s, ho_s,
                go_sem, pair_sem, rs_sem, sq_sem, y_sem, a_sem, q_sem, pr_sem, kv_send, kv_recv, swap_sem):
    chips, tp_size, rows, heads, head_dim, kv_dev, group, shard_len = dims
    sp_size = 2 * chips
    pairs = heads // 2
    width = heads * head_dim
    model = tok_in.shape[1]
    hidden_width = tp_size * width
    segments = group + 2
    qrows = kv_dev * group * rows

    me = lax.axis_index("sp")
    me_tp = lax.axis_index("tp")
    chip = me // 2
    core = lax.rem(me, 2)
    steps = (2, 1, 3)

    def same_core(dc):
        return lax.rem(chip + dc, chips) * 2 + core

    barrier = pltpu.get_barrier_semaphore()
    for dc in steps:
        pl.semaphore_signal(barrier, inc=1, device_id={"sp": same_core(dc)}, device_id_type=MESH)
    pl.semaphore_signal(barrier, inc=1, device_id={"sp": chip * 2 + (1 - core)}, device_id_type=MESH)

    @pl.when(me_tp == 0)
    def _():
        pl.semaphore_wait(barrier, chips)
        for other in range(1, tp_size):
            pl.semaphore_signal(barrier, inc=1, device_id={"tp": other}, device_id_type=MESH)

    @pl.when(me_tp != 0)
    def _():
        pl.semaphore_wait(barrier, chips + 1)
        pl.semaphore_signal(barrier, inc=1, device_id={"tp": 0}, device_id_type=MESH)

    def wait_for_tp():
        @pl.when(me_tp == 0)
        def _():
            pl.semaphore_wait(barrier, tp_size - 1)
            for other in range(1, tp_size):
                pl.semaphore_signal(go_sem, inc=1, device_id={"tp": other}, device_id_type=MESH)

        @pl.when(me_tp != 0)
        def _():
            pl.semaphore_wait(go_sem, 1)

    def remote(src, dst, send, recv, device):
        return pltpu.make_async_remote_copy(src_ref=src, dst_ref=dst, send_sem=send, recv_sem=recv, device_id=device, device_id_type=MESH)

    partner = {"sp": chip * 2 + (1 - core)}
    my_cols = pl.ds(pl.multiple_of(me * shard_len, LANES), shard_len)

    partner_cols = pl.ds(pl.multiple_of((chip * 2 + (1 - core)) * shard_len, LANES), shard_len)

    def start_round(round_idx, own):
        which, row = round_idx % 2, round_idx // 2
        cache, swap, land = ((k_in, k_swap, k_land), (v_in, v_swap, v_land))[which]
        for dc in steps:
            dst = same_core(dc)
            src, cols = (cache.at[dst * rows + row], my_cols) if own else (swap.at[lax.rem(chip + dc, chips) * rows + row], partner_cols)
            remote(src, land.at[row, :, :, cols], kv_send.at[which], kv_recv.at[which], {"sp": dst}).start()

    def total_of(ref, sems):
        return remote(ref, ref, sems[0], sems[1], partner)

    start_round(0, True)
    for cache, swap, n in ((k_in, k_swap, 0), (v_in, v_swap, 1)):
        for block in range(chips):
            src = cache.at[pl.ds((block * 2 + (1 - core)) * rows, rows)]
            remote(src, swap.at[pl.ds(block * rows, rows)], swap_sem.at[2 * n], swap_sem.at[2 * n + 1], partner).start()
    start_round(1, True)

    def decode_step(in_sem, w_sem, st_sem, own_sem, kb_sem):
        def state_copy(step, slot):
            target_core = jnp.where(step < chips, 1 - core, core)
            dest = lax.rem(step, chips) * 2 + target_core
            return pltpu.make_async_copy(states.at[0, pl.ds(dest * rows, rows)], st_buf.at[slot], st_sem.at[slot])

        slope_copy = pltpu.make_async_copy(slopes_in, slopes, in_sem.at[5])
        slope_copy.start()
        state_copy(0, 0).start()
        small_copies = [pltpu.make_async_copy(src, dst, in_sem.at[n]) for n, (src, dst) in enumerate(
            ((tok_in, tok), (lin_gain_in, lin_gain), (out_gain_in, out_gain), (attn_gain_in, attn_gain), (rope_in, rope)))]
        for copy in small_copies:
            copy.start()
        weight_copies = [pltpu.make_async_copy(src, dst, w_sem.at[n]) for n, (src, dst) in enumerate(
            ((w_qkv, wv_qkv), (w_gate, wv_gate), (w_lo, wv_lo), (w_in, wv_in), (w_ao, wv_ao)))]
        for copy in weight_copies:
            copy.start()

        lane = lax.broadcasted_iota(jnp.int32, (1, LANES), 1)
        low_half = lane < head_dim

        def pair_slope(p):
            return jnp.where(low_half, jnp.full((1, LANES), slopes[2 * p], F32), jnp.full((1, LANES), slopes[2 * p + 1], F32))

        slope_copy.wait()
        offset = (shard_len * (sp_size - 1 - me)).astype(F32)
        decay = [jnp.exp(-pair_slope(p) * offset) for p in range(pairs)]

        def weigh_step(step, target):
            slot = lax.rem(step, 2)

            @pl.when(step + 1 < 2 * chips)
            def _():
                state_copy(step + 1, lax.rem(step + 1, 2)).start()

            state_copy(step, slot).wait()
            block = lax.rem(step, chips)
            for b in range(rows):
                for p in range(pairs):
                    packed = jnp.concatenate([st_buf[slot, b, 2 * p], st_buf[slot, b, 2 * p + 1]], axis=1)
                    target[block, b, p] = packed * decay[p]

        @pl.loop(0, chips)
        def _(step):
            weigh_step(step, p_out)

        pair_copy = remote(p_out, p_in, pair_sem.at[0], pair_sem.at[1], partner)
        pair_copy.start()

        @pl.loop(chips, 2 * chips)
        def _(step):
            weigh_step(step, acc)

        own_copies = [pltpu.make_async_copy(cache.at[pl.ds(me * rows, rows)], land.at[:, :, :, my_cols], own_sem.at[n])
                      for n, (cache, land) in enumerate(((k_in, k_land), (v_in, v_land)))]
        for copy in own_copies:
            copy.start()
        for n, swap in enumerate((k_swap, v_swap)):
            total_of(swap, (swap_sem.at[2 * n], swap_sem.at[2 * n + 1])).wait()
        partner_copies = [pltpu.make_async_copy(swap.at[pl.ds(chip * rows, rows)], land.at[:, :, :, partner_cols], own_sem.at[2 + n])
                          for n, (swap, land) in enumerate(((k_swap, k_land), (v_swap, v_land)))]
        for copy in partner_copies:
            copy.start()
        start_round(0, False)

        pair_copy.wait()

        @pl.loop(0, chips)
        def _(block):
            for b in range(rows):
                acc[block, b] = acc[block, b] + p_in[block, b]

        nexts = [(lax.rem(chip + dc, chips), {"sp": lax.rem(chip + dc, chips) * 2 + core}) for dc in (1, chips - 1)]
        far = lax.rem(chip + 2, chips)
        half = rows // 2
        parts = [pl.ds(0, half), pl.ds(half, half)]

        def rs_copy(n, src, dst, side):
            return remote(src, dst, rs_sem.at[n], rs_sem.at[n + 1], nexts[side][1])

        relay_copies = [rs_copy(0, acc.at[far, parts[side]], relay_in.at[side], side) for side in range(2)]
        rs_copies = [rs_copy(2, acc.at[nexts[side][0], parts[1 - side]], rs_in.at[side, parts[1 - side]], side) for side in range(2)]
        for copy in relay_copies + rs_copies:
            copy.start()
        start_round(1, False)

        def rms(vals):
            return vals * lax.rsqrt(jnp.mean(vals * vals, axis=-1, keepdims=True) + NORM_EPS)

        pad_rows = 8 - rows

        def pad8(vals):
            return jnp.concatenate([vals, jnp.zeros((pad_rows,) + vals.shape[1:], vals.dtype)], axis=0) if pad_rows else vals

        for copy in small_copies:
            copy.wait()
        tokens = pad8(tok[...].astype(F32))
        normed = (rms(tokens) * lin_gain[...]).astype(BF16)
        weight_copies[0].wait()

        def act(n):
            lin = jnp.dot(normed, wv_qkv[n], preferred_element_type=F32)
            return (lin * jax.nn.sigmoid(lin)).astype(BF16).astype(F32)

        query, key, value = act(0), act(1), act(2)
        weight_copies[1].wait()
        gate = jax.nn.sigmoid(jnp.dot(normed, wv_gate[...], preferred_element_type=F32))
        query_t = jnp.transpose(query)
        key_t = jnp.transpose(key)
        total_of(relay_in, (rs_sem.at[0], rs_sem.at[1])).wait()
        for side in range(2):
            block = nexts[side][0]
            for b in range(half):
                acc[block, side * half + b] = acc[block, side * half + b] + relay_in[side, b]
            rs_copy(2, acc.at[block, parts[side]], rs_in.at[side, parts[side]], side).start()
        start_round(2, True)
        start_round(2, False)
        o_s[...] = jnp.zeros_like(o_s)

        def column(cols, p, b):
            lo = cols[2 * p * head_dim:(2 * p + 1) * head_dim, b:b + 1]
            hi = cols[(2 * p + 1) * head_dim:(2 * p + 2) * head_dim, b:b + 1]
            return jnp.where(low_half, lo, hi)

        total_of(rs_in, (rs_sem.at[2], rs_sem.at[3])).wait()

        for p in range(pairs):
            lam = jnp.exp(-pair_slope(p))
            cols = slice(p * LANES, (p + 1) * LANES)
            for b in range(rows):
                moved = acc[chip, b, p] + rs_in[0, b, p] + rs_in[1, b, p]
                state = lam * moved + column(key_t, p, b) * value[b:b + 1, cols]
                o_s[b:b + 1, cols] = jnp.sum(column(query_t, p, b) * state, axis=0, keepdims=True)
                st_out[b, 2 * p] = state[:, :head_dim]
                st_out[b, 2 * p + 1] = state[:, head_dim:]

        def tp_sum(buf, vals, sems):
            buf[me_tp] = vals
            copies = []
            for dt in (2, 1, 3)[-(tp_size - 1):]:
                copies.append(remote(buf.at[me_tp], buf.at[me_tp], sems.at[0], sems.at[1], {"tp": lax.rem(me_tp + dt, tp_size)}))
            for copy in copies:
                copy.start()
            total_of(buf.at[pl.ds(0, len(copies))], (sems.at[0], sems.at[1])).wait()
            total = buf[0]
            for n in range(1, tp_size):
                total = total + buf[n]
            return total

        wait_for_tp()
        lin_attn = o_s[...]
        squares = jnp.broadcast_to(jnp.sum(lin_attn * lin_attn, axis=-1, keepdims=True), (8, LANES))
        square_sum = tp_sum(sq_x, squares, sq_sem)[:, :1]
        mixed = (lin_attn * lax.rsqrt(square_sum / hidden_width + NORM_EPS) * out_gain[...] * gate).astype(BF16)
        weight_copies[2].wait()
        lin_out = tp_sum(y_x, jnp.dot(mixed, wv_lo[...], preferred_element_type=F32), y_sem)
        hidden = (normed.astype(F32) + lin_out).astype(BF16).astype(F32)
        normed_two = (rms(hidden) * attn_gain[...]).astype(BF16)

        weight_copies[3].wait()
        proj = lax.dot_general(normed_two, wv_in[...], NT, preferred_element_type=F32).astype(BF16).astype(F32)
        cols_in = proj.shape[1]
        quarter = head_dim // 4
        rotated = proj * rope[0:1, :] + pltpu.roll(proj, quarter, 1) * rope[1:2, :] + pltpu.roll(proj, cols_in - quarter, 1) * rope[2:3, :]
        rotated = rotated.astype(BF16).astype(F32)

        def segment_at(kv, segment):
            start = (kv * segments + segment) * head_dim
            block = rotated[:, start // LANES * LANES:start // LANES * LANES + LANES]
            if start % LANES != kv * head_dim:
                block = pltpu.roll(block, head_dim, 1)
            return jnp.where(low_half if kv == 0 else ~low_half, block, 0.0)

        def packed_at(segment):
            return (segment_at(0, segment) + segment_at(1, segment))[:rows]

        key_rows, value_rows = packed_at(group), packed_at(group + 1)
        for i in range(group):
            q_s[i * rows:(i + 1) * rows, :] = packed_at(i)
            kn_s[i * rows:(i + 1) * rows, :] = key_rows
            vn_s[i * rows:(i + 1) * rows, :] = value_rows

        def spread(vals):
            return jnp.concatenate([jnp.where(low_half, vals, 0.0), jnp.where(low_half, 0.0, vals)], axis=0)

        q_x[me] = q_s[...].astype(BF16)
        for dc in steps:
            remote(q_x.at[me], q_x.at[me], q_sem.at[0], q_sem.at[1], {"sp": same_core(dc)}).start()
        remote(q_x.at[me], q_x.at[me], q_sem.at[2], q_sem.at[3], partner).start()
        for own in (True, False):
            start_round(3, own)
        for own in (True, False):
            start_round(4, own)

        def shard_copies(j, slot):
            return [pltpu.make_async_copy(cache.at[pl.ds(j * rows, rows)], buf.at[slot], kb_sem.at[n, slot])
                    for n, (cache, buf) in enumerate(((k_in, k_buf), (v_in, v_buf)))]

        for copy in shard_copies(0, 0):
            copy.start()

        rotated_t = jnp.transpose(rotated)
        lane16 = lax.broadcasted_iota(jnp.int32, (1, CACHE_EXTRA), 1)
        prompt_len = sp_size * shard_len
        for land, segment in ((k_land, group), (v_land, group + 1)):
            for kv in range(kv_dev):
                start = (kv * segments + segment) * head_dim
                for b in range(rows):
                    tail = jnp.where(lane16 == 0, rotated_t[start:start + head_dim, b:b + 1], 0.0)
                    land[b, kv, :, prompt_len:] = tail.astype(BF16)

        row_id = lax.broadcasted_iota(jnp.int32, (qrows, 1), 0)
        row_seq = lax.rem(row_id, rows)
        split = group * rows
        scale = head_dim ** -0.5

        total_of(q_x.at[pl.ds(0, chips - 1)], (q_sem.at[0], q_sem.at[1])).wait()
        for dc in (2, 1, 3):
            src = same_core(dc)
            remote(q_x.at[src], q_x.at[src], q_sem.at[2], q_sem.at[3], partner).start()
        total_of(q_x.at[pl.ds(0, chips)], (q_sem.at[2], q_sem.at[3])).wait()

        def write_partial(ref, out, peak, total):
            ref[:split] = out
            stats = jnp.transpose(jnp.where(low_half, peak, total))
            stats = jnp.concatenate([stats[:4], stats[head_dim:head_dim + 4]], axis=0)
            ref[split:] = jnp.concatenate([stats, jnp.zeros((8, LANES - qrows), F32)], axis=1)

        def read_partial(ref):
            stats = jnp.transpose(ref[split:])
            return ref[:split], stats[:qrows, 0:1], stats[:qrows, 4:5]

        def both_heads(column_vals):
            return jnp.where(low_half, column_vals[:split], column_vals[split:])

        @pl.loop(0, sp_size)
        def _(j):
            slot = lax.rem(j, 2)

            @pl.when(j + 1 < sp_size)
            def _():
                for copy in shard_copies(j + 1, lax.rem(j + 1, 2)):
                    copy.start()

            for copy in shard_copies(j, slot):
                copy.wait()
            queries = spread(q_x[j].astype(F32)).astype(BF16)
            scores = jnp.zeros((qrows, shard_len), F32)
            for b in range(rows):
                keys = k_buf[slot, b].reshape(kv_dev * head_dim, shard_len)
                scores = jnp.where(row_seq == b, jnp.dot(queries, keys, preferred_element_type=F32), scores)
            scores = scores * scale
            peak = jnp.max(scores, axis=-1, keepdims=True)
            probs = jnp.exp(scores - peak)
            total = jnp.sum(probs, axis=-1, keepdims=True)
            probs = probs.astype(BF16)
            out = jnp.zeros((qrows, LANES), F32)
            for b in range(rows):
                vals = v_buf[slot, b].reshape(kv_dev * head_dim, shard_len)
                out = jnp.where(row_seq == b, lax.dot_general(probs, vals, NT, preferred_element_type=F32), out)
            write_partial(pr_out.at[lax.rem(j, 2), j // 2], both_heads(out), peak, total)

        pr_swap = remote(pr_out.at[1 - core], pr_pair, pr_sem.at[0], pr_sem.at[1], partner)
        pr_swap.start()
        pr_swap.wait()

        @pl.loop(0, chips)
        def _(block):
            out_a, peak_a, total_a = read_partial(pr_out.at[core, block])
            out_b, peak_b, total_b = read_partial(pr_pair.at[block])
            peak = jnp.maximum(peak_a, peak_b)
            scale_a, scale_b = jnp.exp(peak_a - peak), jnp.exp(peak_b - peak)
            write_partial(pr_mine.at[block], out_a * both_heads(scale_a) + out_b * both_heads(scale_b), peak, total_a * scale_a + total_b * scale_b)

        for dc in (2, 1, 3):
            dst_chip = lax.rem(chip + dc, chips)
            remote(pr_mine.at[dst_chip], pr_in.at[chip], pr_sem.at[2], pr_sem.at[3], {"sp": dst_chip * 2 + core}).start()
        for own in (True, False):
            start_round(5, own)

        @pl.when(core == 1)
        def _():
            for own in (True, False):
                start_round(6, own)

        pr_in[chip] = pr_mine[chip]

        new_score = jnp.sum(spread(q_s[...] * kn_s[...]), axis=-1, keepdims=True) * scale

        total_of(pr_in.at[pl.ds(0, chips - 1)], (pr_sem.at[2], pr_sem.at[3])).wait()
        partials = [read_partial(pr_in.at[n]) for n in range(chips)]
        top = new_score
        for _, peak, _ in partials:
            top = jnp.maximum(top, peak)
        new_prob = jnp.exp(new_score - top)
        prob_sum = new_prob
        head = new_prob.astype(BF16).astype(F32) * spread(vn_s[...])
        for out, peak, total in partials:
            weight = jnp.exp(peak - top)
            prob_sum = prob_sum + weight * total
            head = head + weight * spread(out)
        head = (head / prob_sum).astype(BF16).astype(F32)

        ho_s[...] = jnp.zeros_like(ho_s)
        for n in range(0, kv_dev * group, 2):
            block = None
            for m in (n, n + 1):
                kv = m // group
                piece = head[m * rows:(m + 1) * rows]
                if kv != m % 2:
                    piece = pltpu.roll(piece, head_dim, 1)
                block = piece if block is None else block + piece
            ho_s[0:rows, n // 2 * LANES:(n // 2 + 1) * LANES] = block
        weight_copies[4].wait()
        attn_out = tp_sum(a_x, jnp.dot(ho_s[...].astype(BF16), wv_ao[...], preferred_element_type=F32), a_sem)
        hid_out[...] = (normed_two.astype(F32) + attn_out).astype(BF16)[:rows]

        for copy in own_copies:
            copy.wait()
        for copy in partner_copies:
            copy.wait()
        blocks = 2 * (chips - 1)
        total_of(v_in.at[pl.ds(0, blocks * (rows - 1))], (kv_send.at[1], kv_recv.at[1])).wait()

        @pl.when(core == 0)
        def _():
            total_of(k_in.at[pl.ds(0, blocks * (rows - 1))], (kv_send.at[0], kv_recv.at[0])).wait()

        @pl.when(core == 1)
        def _():
            total_of(k_in.at[pl.ds(0, blocks * rows)], (kv_send.at[0], kv_recv.at[0])).wait()

    dma = pltpu.SemaphoreType.DMA
    pl.run_scoped(decode_step, dma((6,)), dma((5,)), dma((2,)), dma((4,)), dma((2, 2)))


def last_kernel(dims, k_in, v_in, k_swap, v_swap, _, k_last, v_last, kv_send, kv_recv, own_sem):
    chips, _, rows, _, _, _, _, shard_len = dims
    me = lax.axis_index("sp")
    chip = me // 2
    core = lax.rem(me, 2)
    row = rows - 1

    def same_core(dc):
        return lax.rem(chip + dc, chips) * 2 + core

    barrier = pltpu.get_barrier_semaphore()
    for dc in (2, 1, 3):
        pl.semaphore_signal(barrier, inc=1, device_id={"sp": same_core(dc)}, device_id_type=MESH)
    pl.semaphore_wait(barrier, chips - 1)
    my_cols = pl.ds(pl.multiple_of(me * shard_len, LANES), shard_len)
    partner_cols = pl.ds(pl.multiple_of((chip * 2 + (1 - core)) * shard_len, LANES), shard_len)

    def own_copies(n, cache, swap, last):
        return [pltpu.make_async_copy(cache.at[me * rows + row], last.at[:, :, my_cols], own_sem.at[2 * n]),
                pltpu.make_async_copy(swap.at[chip * rows + row], last.at[:, :, partner_cols], own_sem.at[2 * n + 1])]

    def start(n, cache, swap, last):
        for own in (True, False):
            for dc in (2, 1, 3):
                dst = same_core(dc)
                src, cols = (cache.at[dst * rows + row], my_cols) if own else (swap.at[lax.rem(chip + dc, chips) * rows + row], partner_cols)
                pltpu.make_async_remote_copy(src_ref=src, dst_ref=last.at[:, :, cols], send_sem=kv_send.at[n], recv_sem=kv_recv.at[n], device_id={"sp": dst}, device_id_type=MESH).start()
        for copy in own_copies(n, cache, swap, last):
            copy.start()

    def finish(n, cache, swap, last):
        for copy in own_copies(n, cache, swap, last):
            copy.wait()
        ref = cache.at[pl.ds(0, 2 * (chips - 1))]
        pltpu.make_async_remote_copy(src_ref=ref, dst_ref=ref, send_sem=kv_send.at[n], recv_sem=kv_recv.at[n], device_id={"sp": same_core(1)}, device_id_type=MESH).wait()

    k_args, v_args = (0, k_in, k_swap, k_last), (1, v_in, v_swap, v_last)

    @pl.when(core == 0)
    def _():
        start(*k_args)

    start(*v_args)

    @pl.when(core == 0)
    def _():
        finish(*k_args)

    finish(*v_args)


def put_kernel(*refs):
    count = (len(refs) - 1) // 2
    sems = refs[-1]
    copies = []
    for n in (2, 3, 1, 0):
        pieces = refs[n].shape[0] if n > 0 else 1
        for i in range(pieces):
            src, dst = (refs[n].at[i], refs[count + n].at[i]) if pieces > 1 else (refs[n], refs[count + n])
            copies.append(pltpu.make_async_copy(src, dst, sems.at[len(copies)]))
    for copy in copies:
        copy.start()
    for copy in copies:
        copy.wait()


def put_last_kernel(k_first, v_first, k_last, v_last, k_dst, v_dst, sems):
    row = k_dst.shape[0] - 1
    cols = pl.ds(0, k_last.shape[-1])
    k_copy = pltpu.make_async_copy(k_last, k_dst.at[row, :, :, cols], sems.at[0])
    v_copy = pltpu.make_async_copy(v_last, v_dst.at[row, :, :, cols], sems.at[1])
    has_k = lax.rem(lax.axis_index("sp"), 2) == 0
    v_copy.start()

    @pl.when(has_k)
    def _():
        k_copy.start()
        k_copy.wait()

    v_copy.wait()


def solution(mesh):
    sp_size = mesh.shape['sp']
    tp_size = mesh.shape['tp']
    chips = sp_size // 2

    def device_step(tokens, states, k_cache, v_cache, slopes, lin_gain, w_lin_qkv, w_lin_gate, out_gain, w_lin_out, attn_gain, w_attn_in, w_attn_out):
        rows, model = tokens.shape
        kv_dev, shard_len, head_dim = k_cache.shape[1:]
        heads = slopes.shape[0]
        segments = w_attn_in.shape[2]
        group = segments - 2
        width = heads * head_dim
        pairs = heads // 2
        cols_in = kv_dev * segments * head_dim
        qrows = kv_dev * group * rows
        prompt_len = sp_size * shard_len
        full_len = prompt_len + CACHE_EXTRA
        dims = (chips, tp_size, rows, heads, head_dim, kv_dev, group, shard_len)
        rope = jnp.asarray(rope_tables(kv_dev, segments, group, head_dim, prompt_len))

        vmem = pl.BlockSpec(memory_space=pltpu.VMEM)
        anym = pl.BlockSpec(memory_space=pl.ANY)
        hbm = pl.BlockSpec(memory_space=pltpu.HBM)
        dma = pltpu.SemaphoreType.DMA

        def in_hbm(*arrays):
            return [pltpu.with_memory_space_constraint(array, pltpu.HBM) for array in arrays]

        land_shape = (rows, kv_dev, head_dim, full_len)
        out_types = [((rows, model), BF16), ((rows, heads, head_dim, head_dim), F32), (land_shape, BF16), (land_shape, BF16)]
        scratch = [
            pltpu.SMEM((heads,), F32),
            pltpu.VMEM((rows, model), BF16),
            pltpu.VMEM((1, model), F32),
            pltpu.VMEM((1, width), F32),
            pltpu.VMEM((1, model), F32),
            pltpu.VMEM((8, cols_in), F32),
            pltpu.VMEM((3, model, width), BF16),
            pltpu.VMEM((model, width), BF16),
            pltpu.VMEM((width, model), BF16),
            pltpu.VMEM((cols_in, model), BF16),
            pltpu.VMEM((width, model), BF16),
            pltpu.VMEM((2, rows, heads, head_dim, head_dim), F32),
            pltpu.VMEM((chips, rows, pairs, head_dim, LANES), F32),
            pltpu.VMEM((chips, rows, pairs, head_dim, LANES), F32),
            pltpu.VMEM((chips, rows, pairs, head_dim, LANES), F32),
            pltpu.VMEM((2, rows // 2, pairs, head_dim, LANES), F32),
            pltpu.VMEM((2, rows, pairs, head_dim, LANES), F32),
            pltpu.VMEM((tp_size, 8, LANES), F32),
            pltpu.VMEM((tp_size, 8, model), F32),
            pltpu.VMEM((tp_size, 8, model), F32),
            pltpu.VMEM((sp_size, group * rows, LANES), BF16),
            pltpu.VMEM((2, chips, group * rows + 8, LANES), F32),
            pltpu.VMEM((chips, group * rows + 8, LANES), F32),
            pltpu.VMEM((chips, group * rows + 8, LANES), F32),
            pltpu.VMEM((chips, group * rows + 8, LANES), F32),
            pltpu.VMEM((2, rows, kv_dev, head_dim, shard_len), BF16),
            pltpu.VMEM((2, rows, kv_dev, head_dim, shard_len), BF16),
            pltpu.VMEM((8, width), F32),
            pltpu.VMEM((group * rows, LANES), F32),
            pltpu.VMEM((group * rows, LANES), F32),
            pltpu.VMEM((group * rows, LANES), F32),
            pltpu.VMEM((8, width), F32),
            pltpu.SemaphoreType.REGULAR,
            dma((2,)),
            dma((4,)),
            dma((2,)),
            dma((2,)),
            dma((2,)),
            dma((4,)),
            dma((4,)),
            dma((2,)),
            dma((2,)),
            dma((4,)),
        ]
        k_cols, v_cols = jnp.transpose(k_cache, (0, 1, 3, 2)), jnp.transpose(v_cache, (0, 1, 3, 2))
        swap_type = jax.ShapeDtypeStruct((chips * rows, kv_dev, head_dim, shard_len), BF16)
        *landed, k_swap, v_swap = pl.pallas_call(
            functools.partial(step_kernel, dims),
            out_shape=[pltpu.VMEM(shape, dtype) for shape, dtype in out_types] + [swap_type] * 2,
            in_specs=[anym, anym, anym, anym, anym, anym] + [anym] * 8,
            out_specs=[vmem] * 4 + [anym] * 2,
            scratch_shapes=scratch,
            compiler_params=pltpu.CompilerParams(collective_id=0, has_side_effects=True, vmem_limit_bytes=40 * 2 ** 20),
        )(
            tokens, slopes, lin_gain.reshape(1, -1), out_gain.reshape(1, -1), attn_gain.reshape(1, -1), rope,
            states, k_cols, v_cols,
            jnp.transpose(w_lin_qkv, (1, 0, 2)), w_lin_gate, w_lin_out,
            jnp.transpose(w_attn_in, (1, 2, 3, 0)).reshape(cols_in, model), w_attn_out,
        )
        hidden_out, state_new, k_out, v_out = pl.pallas_call(
            put_kernel,
            out_shape=[jax.ShapeDtypeStruct(shape, dtype) for shape, dtype in out_types],
            in_specs=[vmem] * 4,
            out_specs=[anym] * 4,
            scratch_shapes=[dma((3 * rows + 1,))],
            compiler_params=pltpu.CompilerParams(vmem_limit_bytes=2 * 2 ** 20),
        )(*landed)
        last_shape = (kv_dev, head_dim, prompt_len)
        last_rows = pl.pallas_call(
            functools.partial(last_kernel, dims),
            out_shape=[pltpu.VMEM(last_shape, BF16)] * 2,
            in_specs=[hbm] * 5,
            out_specs=[vmem] * 2,
            scratch_shapes=[dma((2,)), dma((2,)), dma((4,))],
            compiler_params=pltpu.CompilerParams(collective_id=1, has_side_effects=True, vmem_limit_bytes=2 * 2 ** 20),
        )(*in_hbm(k_cols, v_cols, k_swap, v_swap, hidden_out))
        k_out, v_out = pl.pallas_call(
            put_last_kernel,
            out_shape=[jax.ShapeDtypeStruct(shape, dtype) for shape, dtype in out_types[2:]],
            in_specs=[hbm] * 2 + [vmem] * 2,
            out_specs=[hbm] * 2,
            scratch_shapes=[dma((2,))],
            input_output_aliases={0: 0, 1: 1},
            compiler_params=pltpu.CompilerParams(vmem_limit_bytes=2 * 2 ** 20),
        )(*in_hbm(k_out, v_out), *last_rows)
        return hidden_out, state_new, jnp.transpose(k_out, (0, 1, 3, 2)), jnp.transpose(v_out, (0, 1, 3, 2))

    batch_spec = P(('dp', 'sp'), None)
    head_spec = P(('dp', 'sp'), 'tp', None, None)
    cache_spec = P('dp', 'tp', 'sp', None)
    in_specs = (batch_spec, P('sp', 'dp', 'tp', None, None), cache_spec, cache_spec, P('tp'), P(None), P(None, None, 'tp'), P(None, 'tp'), P('tp'), P('tp', None), P(None), P(None, 'tp', None, None), P('tp', None))
    out_specs = (batch_spec, head_spec, head_spec, head_spec)
    return jax.shard_map(device_step, mesh=mesh, in_specs=in_specs, out_specs=out_specs, check_vma=False)
```

```python
import functools

import numpy as np

import jax
import jax.numpy as jnp
from jax import lax
from jax.experimental import pallas as pl
from jax.experimental.pallas import tpu as pltpu
from jax.sharding import PartitionSpec as P

NORM_EPS = 1e-6
ROPE_BASE = 10000000.0
CACHE_EXTRA = 16
LANES = 128
F32 = jnp.float32
BF16 = jnp.bfloat16
MESH = pl.DeviceIdType.MESH
NT = (((1,), (1,)), ((), ()))


def rope_tables(kv_dev, segments, group, head_dim, position):
    rope_dim = head_dim // 2
    half = rope_dim // 2
    exponents = -np.arange(0, rope_dim, 2, dtype=np.float32) / np.float32(rope_dim)
    angles = (np.float32(position) * np.float32(ROPE_BASE) ** exponents).astype(np.float32)
    cosine, sine = np.cos(angles), np.sin(angles)
    table = np.zeros((8, kv_dev, segments, head_dim), np.float32)
    table[0] = 1.0
    for segment in range(group + 1):
        table[0, :, segment, :half] = cosine
        table[0, :, segment, half:rope_dim] = cosine
        table[1, :, segment, half:rope_dim] = sine
        table[2, :, segment, :half] = -sine
    return table.reshape(8, kv_dev * segments * head_dim)


def step_kernel(dims, tok_in, slopes_in, lin_gain_in, out_gain_in, attn_gain_in, rope_in, states, k_in, v_in, w_qkv, w_gate, w_lo, w_in, w_ao,
                hid_out, st_out, k_land, v_land, k_swap, v_swap,
                slopes, tok, lin_gain, out_gain, attn_gain, rope, wv_qkv, wv_gate, wv_lo, wv_in, wv_ao, st_buf, p_out, p_in, acc, relay_in, rs_in, sq_x, y_x, a_x, q_x, pr_out, pr_pair, pr_mine, pr_in,
                k_buf, v_buf, o_s, q_s, kn_s, vn_s, ho_s,
                go_sem, pair_sem, rs_sem, sq_sem, y_sem, a_sem, q_sem, pr_sem, kv_send, kv_recv, swap_sem):
    chips, tp_size, rows, heads, head_dim, kv_dev, group, shard_len = dims
    sp_size = 2 * chips
    pairs = heads // 2
    width = heads * head_dim
    model = tok_in.shape[1]
    hidden_width = tp_size * width
    segments = group + 2
    qrows = kv_dev * group * rows

    me = lax.axis_index("sp")
    me_tp = lax.axis_index("tp")
    chip = me // 2
    core = lax.rem(me, 2)
    steps = (2, 1, 3)

    def same_core(dc):
        return lax.rem(chip + dc, chips) * 2 + core

    barrier = pltpu.get_barrier_semaphore()
    for dc in steps:
        pl.semaphore_signal(barrier, inc=1, device_id={"sp": same_core(dc)}, device_id_type=MESH)
    pl.semaphore_signal(barrier, inc=1, device_id={"sp": chip * 2 + (1 - core)}, device_id_type=MESH)

    @pl.when(me_tp == 0)
    def _():
        pl.semaphore_wait(barrier, chips)
        for other in range(1, tp_size):
            pl.semaphore_signal(barrier, inc=1, device_id={"tp": other}, device_id_type=MESH)

    @pl.when(me_tp != 0)
    def _():
        pl.semaphore_wait(barrier, chips + 1)
        pl.semaphore_signal(barrier, inc=1, device_id={"tp": 0}, device_id_type=MESH)

    def wait_for_tp():
        @pl.when(me_tp == 0)
        def _():
            pl.semaphore_wait(barrier, tp_size - 1)
            for other in range(1, tp_size):
                pl.semaphore_signal(go_sem, inc=1, device_id={"tp": other}, device_id_type=MESH)

        @pl.when(me_tp != 0)
        def _():
            pl.semaphore_wait(go_sem, 1)

    def remote(src, dst, send, recv, device):
        return pltpu.make_async_remote_copy(src_ref=src, dst_ref=dst, send_sem=send, recv_sem=recv, device_id=device, device_id_type=MESH)

    partner = {"sp": chip * 2 + (1 - core)}
    my_cols = pl.ds(pl.multiple_of(me * shard_len, LANES), shard_len)

    partner_cols = pl.ds(pl.multiple_of((chip * 2 + (1 - core)) * shard_len, LANES), shard_len)

    def start_round(round_idx, own):
        which, row = ((0, 0), (1, 0), (0, 1), (1, 1), (1, 2), (1, 3), (0, 2))[round_idx]
        cache, swap, land = ((k_in, k_swap, k_land), (v_in, v_swap, v_land))[which]
        for dc in steps:
            dst = same_core(dc)
            src, cols = (cache.at[dst * rows + row], my_cols) if own else (swap.at[lax.rem(chip + dc, chips) * rows + row], partner_cols)
            remote(src, land.at[row, :, :, cols], kv_send.at[which], kv_recv.at[which], {"sp": dst}).start()

    def total_of(ref, sems):
        return remote(ref, ref, sems[0], sems[1], partner)

    start_round(0, True)
    for cache, swap, n in ((k_in, k_swap, 0), (v_in, v_swap, 1)):
        for block in range(chips):
            src = cache.at[pl.ds((block * 2 + (1 - core)) * rows, rows)]
            remote(src, swap.at[pl.ds(block * rows, rows)], swap_sem.at[2 * n], swap_sem.at[2 * n + 1], partner).start()
    start_round(1, True)

    def decode_step(in_sem, w_sem, st_sem, own_sem, kb_sem):
        def state_copy(step, slot):
            target_core = jnp.where(step < chips, 1 - core, core)
            dest = lax.rem(step, chips) * 2 + target_core
            return pltpu.make_async_copy(states.at[0, pl.ds(dest * rows, rows)], st_buf.at[slot], st_sem.at[slot])

        slope_copy = pltpu.make_async_copy(slopes_in, slopes, in_sem.at[5])
        slope_copy.start()
        state_copy(0, 0).start()
        small_copies = [pltpu.make_async_copy(src, dst, in_sem.at[n]) for n, (src, dst) in enumerate(
            ((tok_in, tok), (lin_gain_in, lin_gain), (out_gain_in, out_gain), (attn_gain_in, attn_gain), (rope_in, rope)))]
        for copy in small_copies:
            copy.start()
        weight_copies = [pltpu.make_async_copy(src, dst, w_sem.at[n]) for n, (src, dst) in enumerate(
            ((w_qkv, wv_qkv), (w_gate, wv_gate), (w_lo, wv_lo), (w_in, wv_in), (w_ao, wv_ao)))]
        for copy in weight_copies:
            copy.start()

        lane = lax.broadcasted_iota(jnp.int32, (1, LANES), 1)
        low_half = lane < head_dim

        def pair_slope(p):
            return jnp.where(low_half, jnp.full((1, LANES), slopes[2 * p], F32), jnp.full((1, LANES), slopes[2 * p + 1], F32))

        slope_copy.wait()
        offset = (shard_len * (sp_size - 1 - me)).astype(F32)
        decay = [jnp.exp(-pair_slope(p) * offset) for p in range(pairs)]

        def weigh_step(step, target):
            slot = lax.rem(step, 2)

            @pl.when(step + 1 < 2 * chips)
            def _():
                state_copy(step + 1, lax.rem(step + 1, 2)).start()

            state_copy(step, slot).wait()
            block = lax.rem(step, chips)
            for b in range(rows):
                for p in range(pairs):
                    packed = jnp.concatenate([st_buf[slot, b, 2 * p], st_buf[slot, b, 2 * p + 1]], axis=1)
                    target[block, b, p] = packed * decay[p]

        @pl.loop(0, chips)
        def _(step):
            weigh_step(step, p_out)

        pair_copy = remote(p_out, p_in, pair_sem.at[0], pair_sem.at[1], partner)
        pair_copy.start()

        @pl.loop(chips, 2 * chips)
        def _(step):
            weigh_step(step, acc)

        own_copies = [pltpu.make_async_copy(cache.at[pl.ds(me * rows, rows)], land.at[:, :, :, my_cols], own_sem.at[n])
                      for n, (cache, land) in enumerate(((k_in, k_land), (v_in, v_land)))]
        for copy in own_copies:
            copy.start()
        for n, swap in enumerate((k_swap, v_swap)):
            total_of(swap, (swap_sem.at[2 * n], swap_sem.at[2 * n + 1])).wait()
        partner_copies = [pltpu.make_async_copy(swap.at[pl.ds(chip * rows, rows)], land.at[:, :, :, partner_cols], own_sem.at[2 + n])
                          for n, (swap, land) in enumerate(((k_swap, k_land), (v_swap, v_land)))]
        for copy in partner_copies:
            copy.start()
        start_round(0, False)

        pair_copy.wait()

        @pl.loop(0, chips)
        def _(block):
            for b in range(rows):
                acc[block, b] = acc[block, b] + p_in[block, b]

        nexts = [(lax.rem(chip + dc, chips), {"sp": lax.rem(chip + dc, chips) * 2 + core}) for dc in (1, chips - 1)]
        far = lax.rem(chip + 2, chips)
        half = rows // 2
        parts = [pl.ds(0, half), pl.ds(half, half)]

        def rs_copy(n, src, dst, side):
            return remote(src, dst, rs_sem.at[n], rs_sem.at[n + 1], nexts[side][1])

        relay_copies = [rs_copy(0, acc.at[far, parts[side]], relay_in.at[side], side) for side in range(2)]
        rs_copies = [rs_copy(2, acc.at[nexts[side][0], parts[1 - side]], rs_in.at[side, parts[1 - side]], side) for side in range(2)]
        for copy in relay_copies + rs_copies:
            copy.start()
        start_round(1, False)

        def rms(vals):
            return vals * lax.rsqrt(jnp.mean(vals * vals, axis=-1, keepdims=True) + NORM_EPS)

        pad_rows = 8 - rows

        def pad8(vals):
            return jnp.concatenate([vals, jnp.zeros((pad_rows,) + vals.shape[1:], vals.dtype)], axis=0) if pad_rows else vals

        for copy in small_copies:
            copy.wait()
        tokens = pad8(tok[...].astype(F32))
        normed = (rms(tokens) * lin_gain[...]).astype(BF16)
        weight_copies[0].wait()

        def act(n):
            lin = jnp.dot(normed, wv_qkv[n], preferred_element_type=F32)
            return (lin * jax.nn.sigmoid(lin)).astype(BF16).astype(F32)

        query, key, value = act(0), act(1), act(2)
        weight_copies[1].wait()
        gate = jax.nn.sigmoid(jnp.dot(normed, wv_gate[...], preferred_element_type=F32))
        query_t = jnp.transpose(query)
        key_t = jnp.transpose(key)
        total_of(relay_in, (rs_sem.at[0], rs_sem.at[1])).wait()
        for side in range(2):
            block = nexts[side][0]
            for b in range(half):
                acc[block, side * half + b] = acc[block, side * half + b] + relay_in[side, b]
            rs_copy(2, acc.at[block, parts[side]], rs_in.at[side, parts[side]], side).start()
        start_round(2, True)
        start_round(2, False)
        o_s[...] = jnp.zeros_like(o_s)

        def column(cols, p, b):
            lo = cols[2 * p * head_dim:(2 * p + 1) * head_dim, b:b + 1]
            hi = cols[(2 * p + 1) * head_dim:(2 * p + 2) * head_dim, b:b + 1]
            return jnp.where(low_half, lo, hi)

        total_of(rs_in, (rs_sem.at[2], rs_sem.at[3])).wait()

        for p in range(pairs):
            lam = jnp.exp(-pair_slope(p))
            cols = slice(p * LANES, (p + 1) * LANES)
            for b in range(rows):
                moved = acc[chip, b, p] + rs_in[0, b, p] + rs_in[1, b, p]
                state = lam * moved + column(key_t, p, b) * value[b:b + 1, cols]
                o_s[b:b + 1, cols] = jnp.sum(column(query_t, p, b) * state, axis=0, keepdims=True)
                st_out[b, 2 * p] = state[:, :head_dim]
                st_out[b, 2 * p + 1] = state[:, head_dim:]

        def tp_sum(buf, vals, sems):
            buf[me_tp] = vals
            copies = []
            for dt in (2, 1, 3)[-(tp_size - 1):]:
                copies.append(remote(buf.at[me_tp], buf.at[me_tp], sems.at[0], sems.at[1], {"tp": lax.rem(me_tp + dt, tp_size)}))
            for copy in copies:
                copy.start()
            total_of(buf.at[pl.ds(0, len(copies))], (sems.at[0], sems.at[1])).wait()
            total = buf[0]
            for n in range(1, tp_size):
                total = total + buf[n]
            return total

        wait_for_tp()
        lin_attn = o_s[...]
        squares = jnp.broadcast_to(jnp.sum(lin_attn * lin_attn, axis=-1, keepdims=True), (8, LANES))
        square_sum = tp_sum(sq_x, squares, sq_sem)[:, :1]
        mixed = (lin_attn * lax.rsqrt(square_sum / hidden_width + NORM_EPS) * out_gain[...] * gate).astype(BF16)
        weight_copies[2].wait()
        lin_out = tp_sum(y_x, jnp.dot(mixed, wv_lo[...], preferred_element_type=F32), y_sem)
        hidden = (normed.astype(F32) + lin_out).astype(BF16).astype(F32)
        normed_two = (rms(hidden) * attn_gain[...]).astype(BF16)

        weight_copies[3].wait()
        proj = lax.dot_general(normed_two, wv_in[...], NT, preferred_element_type=F32).astype(BF16).astype(F32)
        cols_in = proj.shape[1]
        quarter = head_dim // 4
        rotated = proj * rope[0:1, :] + pltpu.roll(proj, quarter, 1) * rope[1:2, :] + pltpu.roll(proj, cols_in - quarter, 1) * rope[2:3, :]
        rotated = rotated.astype(BF16).astype(F32)

        def segment_at(kv, segment):
            start = (kv * segments + segment) * head_dim
            block = rotated[:, start // LANES * LANES:start // LANES * LANES + LANES]
            if start % LANES != kv * head_dim:
                block = pltpu.roll(block, head_dim, 1)
            return jnp.where(low_half if kv == 0 else ~low_half, block, 0.0)

        def packed_at(segment):
            return (segment_at(0, segment) + segment_at(1, segment))[:rows]

        key_rows, value_rows = packed_at(group), packed_at(group + 1)
        for i in range(group):
            q_s[i * rows:(i + 1) * rows, :] = packed_at(i)
            kn_s[i * rows:(i + 1) * rows, :] = key_rows
            vn_s[i * rows:(i + 1) * rows, :] = value_rows

        def spread(vals):
            return jnp.concatenate([jnp.where(low_half, vals, 0.0), jnp.where(low_half, 0.0, vals)], axis=0)

        q_x[me] = q_s[...].astype(BF16)
        for dc in steps:
            remote(q_x.at[me], q_x.at[me], q_sem.at[0], q_sem.at[1], {"sp": same_core(dc)}).start()
        remote(q_x.at[me], q_x.at[me], q_sem.at[2], q_sem.at[3], partner).start()
        for own in (True, False):
            start_round(3, own)
        for own in (True, False):
            start_round(4, own)

        def shard_copies(j, slot):
            return [pltpu.make_async_copy(cache.at[pl.ds(j * rows, rows)], buf.at[slot], kb_sem.at[n, slot])
                    for n, (cache, buf) in enumerate(((k_in, k_buf), (v_in, v_buf)))]

        for copy in shard_copies(0, 0):
            copy.start()

        rotated_t = jnp.transpose(rotated)
        lane16 = lax.broadcasted_iota(jnp.int32, (1, CACHE_EXTRA), 1)
        prompt_len = sp_size * shard_len
        for land, segment in ((k_land, group), (v_land, group + 1)):
            for kv in range(kv_dev):
                start = (kv * segments + segment) * head_dim
                for b in range(rows):
                    tail = jnp.where(lane16 == 0, rotated_t[start:start + head_dim, b:b + 1], 0.0)
                    land[b, kv, :, prompt_len:] = tail.astype(BF16)

        row_id = lax.broadcasted_iota(jnp.int32, (qrows, 1), 0)
        row_seq = lax.rem(row_id, rows)
        split = group * rows
        scale = head_dim ** -0.5

        total_of(q_x.at[pl.ds(0, chips - 1)], (q_sem.at[0], q_sem.at[1])).wait()
        for dc in (2, 1, 3):
            src = same_core(dc)
            remote(q_x.at[src], q_x.at[src], q_sem.at[2], q_sem.at[3], partner).start()
        total_of(q_x.at[pl.ds(0, chips)], (q_sem.at[2], q_sem.at[3])).wait()

        def write_partial(ref, out, peak, total):
            ref[:split] = out
            stats = jnp.transpose(jnp.where(low_half, peak, total))
            stats = jnp.concatenate([stats[:4], stats[head_dim:head_dim + 4]], axis=0)
            ref[split:] = jnp.concatenate([stats, jnp.zeros((8, LANES - qrows), F32)], axis=1)

        def read_partial(ref):
            stats = jnp.transpose(ref[split:])
            return ref[:split], stats[:qrows, 0:1], stats[:qrows, 4:5]

        def both_heads(column_vals):
            return jnp.where(low_half, column_vals[:split], column_vals[split:])

        @pl.loop(0, sp_size)
        def _(j):
            slot = lax.rem(j, 2)

            @pl.when(j + 1 < sp_size)
            def _():
                for copy in shard_copies(j + 1, lax.rem(j + 1, 2)):
                    copy.start()

            for copy in shard_copies(j, slot):
                copy.wait()
            queries = spread(q_x[j].astype(F32)).astype(BF16)
            scores = jnp.zeros((qrows, shard_len), F32)
            for b in range(rows):
                keys = k_buf[slot, b].reshape(kv_dev * head_dim, shard_len)
                scores = jnp.where(row_seq == b, jnp.dot(queries, keys, preferred_element_type=F32), scores)
            scores = scores * scale
            peak = jnp.max(scores, axis=-1, keepdims=True)
            probs = jnp.exp(scores - peak)
            total = jnp.sum(probs, axis=-1, keepdims=True)
            probs = probs.astype(BF16)
            out = jnp.zeros((qrows, LANES), F32)
            for b in range(rows):
                vals = v_buf[slot, b].reshape(kv_dev * head_dim, shard_len)
                out = jnp.where(row_seq == b, lax.dot_general(probs, vals, NT, preferred_element_type=F32), out)
            write_partial(pr_out.at[lax.rem(j, 2), j // 2], both_heads(out), peak, total)

        pr_swap = remote(pr_out.at[1 - core], pr_pair, pr_sem.at[0], pr_sem.at[1], partner)
        pr_swap.start()
        pr_swap.wait()

        @pl.loop(0, chips)
        def _(block):
            out_a, peak_a, total_a = read_partial(pr_out.at[core, block])
            out_b, peak_b, total_b = read_partial(pr_pair.at[block])
            peak = jnp.maximum(peak_a, peak_b)
            scale_a, scale_b = jnp.exp(peak_a - peak), jnp.exp(peak_b - peak)
            write_partial(pr_mine.at[block], out_a * both_heads(scale_a) + out_b * both_heads(scale_b), peak, total_a * scale_a + total_b * scale_b)

        for dc in (2, 1, 3):
            dst_chip = lax.rem(chip + dc, chips)
            remote(pr_mine.at[dst_chip], pr_in.at[chip], pr_sem.at[2], pr_sem.at[3], {"sp": dst_chip * 2 + core}).start()
        for own in (True, False):
            start_round(5, own)

        @pl.when(core == 1)
        def _():
            for own in (True, False):
                start_round(6, own)

        pr_in[chip] = pr_mine[chip]

        new_score = jnp.sum(spread(q_s[...] * kn_s[...]), axis=-1, keepdims=True) * scale

        total_of(pr_in.at[pl.ds(0, chips - 1)], (pr_sem.at[2], pr_sem.at[3])).wait()
        partials = [read_partial(pr_in.at[n]) for n in range(chips)]
        top = new_score
        for _, peak, _ in partials:
            top = jnp.maximum(top, peak)
        new_prob = jnp.exp(new_score - top)
        prob_sum = new_prob
        head = new_prob.astype(BF16).astype(F32) * spread(vn_s[...])
        for out, peak, total in partials:
            weight = jnp.exp(peak - top)
            prob_sum = prob_sum + weight * total
            head = head + weight * spread(out)
        head = (head / prob_sum).astype(BF16).astype(F32)

        ho_s[...] = jnp.zeros_like(ho_s)
        for n in range(0, kv_dev * group, 2):
            block = None
            for m in (n, n + 1):
                kv = m // group
                piece = head[m * rows:(m + 1) * rows]
                if kv != m % 2:
                    piece = pltpu.roll(piece, head_dim, 1)
                block = piece if block is None else block + piece
            ho_s[0:rows, n // 2 * LANES:(n // 2 + 1) * LANES] = block
        weight_copies[4].wait()
        attn_out = tp_sum(a_x, jnp.dot(ho_s[...].astype(BF16), wv_ao[...], preferred_element_type=F32), a_sem)
        hid_out[...] = (normed_two.astype(F32) + attn_out).astype(BF16)[:rows]

        for copy in own_copies:
            copy.wait()
        for copy in partner_copies:
            copy.wait()
        blocks = 2 * (chips - 1)
        total_of(v_in.at[pl.ds(0, blocks * rows)], (kv_send.at[1], kv_recv.at[1])).wait()

        @pl.when(core == 0)
        def _():
            total_of(k_in.at[pl.ds(0, blocks * (rows - 2))], (kv_send.at[0], kv_recv.at[0])).wait()

        @pl.when(core == 1)
        def _():
            total_of(k_in.at[pl.ds(0, blocks * (rows - 1))], (kv_send.at[0], kv_recv.at[0])).wait()

    dma = pltpu.SemaphoreType.DMA
    pl.run_scoped(decode_step, dma((6,)), dma((5,)), dma((2,)), dma((4,)), dma((2, 2)))


def last_kernel(dims, k_in, k_swap, _, k_last, k_send, k_recv, own_sem):
    chips, _, rows, _, _, _, _, shard_len = dims
    me = lax.axis_index("sp")
    chip = me // 2
    core = lax.rem(me, 2)

    def same_core(dc):
        return lax.rem(chip + dc, chips) * 2 + core

    barrier = pltpu.get_barrier_semaphore()
    for dc in (2, 1, 3):
        pl.semaphore_signal(barrier, inc=1, device_id={"sp": same_core(dc)}, device_id_type=MESH)
    pl.semaphore_wait(barrier, chips - 1)
    my_cols = pl.ds(pl.multiple_of(me * shard_len, LANES), shard_len)
    partner_cols = pl.ds(pl.multiple_of((chip * 2 + (1 - core)) * shard_len, LANES), shard_len)

    def move(count):
        def block(ref, index):
            return ref.at[pl.ds(index * rows + rows - count, count)]

        def remote(src, dst, device):
            return pltpu.make_async_remote_copy(src_ref=src, dst_ref=dst, send_sem=k_send, recv_sem=k_recv, device_id={"sp": device}, device_id_type=MESH)

        mine, partners = [k_last.at[pl.ds(2 - count, count), :, :, cols] for cols in (my_cols, partner_cols)]
        for own in (True, False):
            for dc in (2, 1, 3):
                dst = same_core(dc)
                src = block(k_in, dst) if own else block(k_swap, lax.rem(chip + dc, chips))
                remote(src, mine if own else partners, dst).start()
        own_copies = [pltpu.make_async_copy(block(k_in, me), mine, own_sem.at[0]), pltpu.make_async_copy(block(k_swap, chip), partners, own_sem.at[1])]
        for copy in own_copies:
            copy.start()
        for copy in own_copies:
            copy.wait()
        total = k_in.at[pl.ds(0, 2 * (chips - 1) * count)]
        remote(total, total, same_core(1)).wait()

    @pl.when(core == 0)
    def _():
        move(2)

    @pl.when(core == 1)
    def _():
        move(1)


def put_kernel(hid, st, k_land, v_land, hid_dst, st_dst, k_dst, v_dst, sems):
    rows, _, _, full_len = k_land.shape
    tail = pl.ds(full_len - CACHE_EXTRA, CACHE_EXTRA)
    core = lax.rem(lax.axis_index("sp"), 2)
    pairs = [(v_land.at[row], v_dst.at[row]) for row in range(rows)] + [(k_land.at[row], k_dst.at[row]) for row in range(rows - 2)]
    pairs += [(st, st_dst), (hid, hid_dst), (k_land.at[rows - 1, :, :, tail], k_dst.at[rows - 1, :, :, tail])]
    copies = [pltpu.make_async_copy(src, dst, sems.at[n]) for n, (src, dst) in enumerate(pairs)]
    for copy in copies:
        copy.start()
    row = rows - 2
    whole = pltpu.make_async_copy(k_land.at[row], k_dst.at[row], sems.at[len(copies)])
    part = pltpu.make_async_copy(k_land.at[row, :, :, tail], k_dst.at[row, :, :, tail], sems.at[len(copies)])

    @pl.when(core == 0)
    def _():
        part.start()
        part.wait()

    @pl.when(core == 1)
    def _():
        whole.start()
        whole.wait()

    for copy in copies:
        copy.wait()


def put_last_kernel(k_first, k_last, k_dst, sems):
    rows = k_dst.shape[0]
    cols = pl.ds(0, k_last.shape[-1])
    core = lax.rem(lax.axis_index("sp"), 2)
    last = pltpu.make_async_copy(k_last.at[1], k_dst.at[rows - 1, :, :, cols], sems.at[0])
    other = pltpu.make_async_copy(k_last.at[0], k_dst.at[rows - 2, :, :, cols], sems.at[1])
    last.start()

    @pl.when(core == 0)
    def _():
        other.start()
        other.wait()

    last.wait()


def solution(mesh):
    sp_size = mesh.shape['sp']
    tp_size = mesh.shape['tp']
    chips = sp_size // 2

    def device_step(tokens, states, k_cache, v_cache, slopes, lin_gain, w_lin_qkv, w_lin_gate, out_gain, w_lin_out, attn_gain, w_attn_in, w_attn_out):
        rows, model = tokens.shape
        kv_dev, shard_len, head_dim = k_cache.shape[1:]
        heads = slopes.shape[0]
        segments = w_attn_in.shape[2]
        group = segments - 2
        width = heads * head_dim
        pairs = heads // 2
        cols_in = kv_dev * segments * head_dim
        qrows = kv_dev * group * rows
        prompt_len = sp_size * shard_len
        full_len = prompt_len + CACHE_EXTRA
        dims = (chips, tp_size, rows, heads, head_dim, kv_dev, group, shard_len)
        rope = jnp.asarray(rope_tables(kv_dev, segments, group, head_dim, prompt_len))

        vmem = pl.BlockSpec(memory_space=pltpu.VMEM)
        anym = pl.BlockSpec(memory_space=pl.ANY)
        hbm = pl.BlockSpec(memory_space=pltpu.HBM)
        dma = pltpu.SemaphoreType.DMA

        def in_hbm(*arrays):
            return [pltpu.with_memory_space_constraint(array, pltpu.HBM) for array in arrays]

        land_shape = (rows, kv_dev, head_dim, full_len)
        out_types = [((rows, model), BF16), ((rows, heads, head_dim, head_dim), F32), (land_shape, BF16), (land_shape, BF16)]
        scratch = [
            pltpu.SMEM((heads,), F32),
            pltpu.VMEM((rows, model), BF16),
            pltpu.VMEM((1, model), F32),
            pltpu.VMEM((1, width), F32),
            pltpu.VMEM((1, model), F32),
            pltpu.VMEM((8, cols_in), F32),
            pltpu.VMEM((3, model, width), BF16),
            pltpu.VMEM((model, width), BF16),
            pltpu.VMEM((width, model), BF16),
            pltpu.VMEM((cols_in, model), BF16),
            pltpu.VMEM((width, model), BF16),
            pltpu.VMEM((2, rows, heads, head_dim, head_dim), F32),
            pltpu.VMEM((chips, rows, pairs, head_dim, LANES), F32),
            pltpu.VMEM((chips, rows, pairs, head_dim, LANES), F32),
            pltpu.VMEM((chips, rows, pairs, head_dim, LANES), F32),
            pltpu.VMEM((2, rows // 2, pairs, head_dim, LANES), F32),
            pltpu.VMEM((2, rows, pairs, head_dim, LANES), F32),
            pltpu.VMEM((tp_size, 8, LANES), F32),
            pltpu.VMEM((tp_size, 8, model), F32),
            pltpu.VMEM((tp_size, 8, model), F32),
            pltpu.VMEM((sp_size, group * rows, LANES), BF16),
            pltpu.VMEM((2, chips, group * rows + 8, LANES), F32),
            pltpu.VMEM((chips, group * rows + 8, LANES), F32),
            pltpu.VMEM((chips, group * rows + 8, LANES), F32),
            pltpu.VMEM((chips, group * rows + 8, LANES), F32),
            pltpu.VMEM((2, rows, kv_dev, head_dim, shard_len), BF16),
            pltpu.VMEM((2, rows, kv_dev, head_dim, shard_len), BF16),
            pltpu.VMEM((8, width), F32),
            pltpu.VMEM((group * rows, LANES), F32),
            pltpu.VMEM((group * rows, LANES), F32),
            pltpu.VMEM((group * rows, LANES), F32),
            pltpu.VMEM((8, width), F32),
            pltpu.SemaphoreType.REGULAR,
            dma((2,)),
            dma((4,)),
            dma((2,)),
            dma((2,)),
            dma((2,)),
            dma((4,)),
            dma((4,)),
            dma((2,)),
            dma((2,)),
            dma((4,)),
        ]
        k_cols, v_cols = jnp.transpose(k_cache, (0, 1, 3, 2)), jnp.transpose(v_cache, (0, 1, 3, 2))
        swap_type = jax.ShapeDtypeStruct((chips * rows, kv_dev, head_dim, shard_len), BF16)
        *landed, k_swap, v_swap = pl.pallas_call(
            functools.partial(step_kernel, dims),
            out_shape=[pltpu.VMEM(shape, dtype) for shape, dtype in out_types] + [swap_type] * 2,
            in_specs=[anym, anym, anym, anym, anym, anym] + [anym] * 8,
            out_specs=[vmem] * 4 + [anym] * 2,
            scratch_shapes=scratch,
            compiler_params=pltpu.CompilerParams(collective_id=0, has_side_effects=True, vmem_limit_bytes=40 * 2 ** 20),
        )(
            tokens, slopes, lin_gain.reshape(1, -1), out_gain.reshape(1, -1), attn_gain.reshape(1, -1), rope,
            states, k_cols, v_cols,
            jnp.transpose(w_lin_qkv, (1, 0, 2)), w_lin_gate, w_lin_out,
            jnp.transpose(w_attn_in, (1, 2, 3, 0)).reshape(cols_in, model), w_attn_out,
        )
        hidden_out, state_new, k_out, v_out = pl.pallas_call(
            put_kernel,
            out_shape=[jax.ShapeDtypeStruct(shape, dtype) for shape, dtype in out_types],
            in_specs=[vmem] * 4,
            out_specs=[anym] * 4,
            scratch_shapes=[dma((2 * rows + 2,))],
            compiler_params=pltpu.CompilerParams(vmem_limit_bytes=2 * 2 ** 20),
        )(*landed)
        last_rows = pl.pallas_call(
            functools.partial(last_kernel, dims),
            out_shape=pltpu.VMEM((2, kv_dev, head_dim, prompt_len), BF16),
            in_specs=[hbm] * 3,
            out_specs=vmem,
            scratch_shapes=[dma, dma, dma((2,))],
            compiler_params=pltpu.CompilerParams(collective_id=1, has_side_effects=True, vmem_limit_bytes=2 * 2 ** 20),
        )(*in_hbm(k_cols, k_swap, hidden_out))
        k_out = pl.pallas_call(
            put_last_kernel,
            out_shape=jax.ShapeDtypeStruct(land_shape, BF16),
            in_specs=[hbm, vmem],
            out_specs=hbm,
            scratch_shapes=[dma((2,))],
            input_output_aliases={0: 0},
            compiler_params=pltpu.CompilerParams(vmem_limit_bytes=2 * 2 ** 20),
        )(*in_hbm(k_out), last_rows)
        return hidden_out, state_new, jnp.transpose(k_out, (0, 1, 3, 2)), jnp.transpose(v_out, (0, 1, 3, 2))

    batch_spec = P(('dp', 'sp'), None)
    head_spec = P(('dp', 'sp'), 'tp', None, None)
    cache_spec = P('dp', 'tp', 'sp', None)
    in_specs = (batch_spec, P('sp', 'dp', 'tp', None, None), cache_spec, cache_spec, P('tp'), P(None), P(None, None, 'tp'), P(None, 'tp'), P('tp'), P('tp', None), P(None), P(None, 'tp', None, None), P('tp', None))
    out_specs = (batch_spec, head_spec, head_spec, head_spec)
    return jax.shard_map(device_step, mesh=mesh, in_specs=in_specs, out_specs=out_specs, check_vma=False)
```

```python
import functools

import numpy as np

import jax
import jax.numpy as jnp
from jax import lax
from jax.experimental import pallas as pl
from jax.experimental.pallas import tpu as pltpu
from jax.sharding import PartitionSpec as P

NORM_EPS = 1e-6
ROPE_BASE = 10000000.0
CACHE_EXTRA = 16
LANES = 128
F32 = jnp.float32
BF16 = jnp.bfloat16
MESH = pl.DeviceIdType.MESH
NT = (((1,), (1,)), ((), ()))


def rope_tables(kv_dev, segments, group, head_dim, position):
    rope_dim = head_dim // 2
    half = rope_dim // 2
    exponents = -np.arange(0, rope_dim, 2, dtype=np.float32) / np.float32(rope_dim)
    angles = (np.float32(position) * np.float32(ROPE_BASE) ** exponents).astype(np.float32)
    cosine, sine = np.cos(angles), np.sin(angles)
    table = np.zeros((8, kv_dev, segments, head_dim), np.float32)
    table[0] = 1.0
    for segment in range(group + 1):
        table[0, :, segment, :half] = cosine
        table[0, :, segment, half:rope_dim] = cosine
        table[1, :, segment, half:rope_dim] = sine
        table[2, :, segment, :half] = -sine
    return table.reshape(8, kv_dev * segments * head_dim)


def step_kernel(dims, tok_in, slopes_in, lin_gain_in, out_gain_in, attn_gain_in, rope_in, states, k_in, v_in, w_qkv, w_gate, w_lo, w_in, w_ao,
                hid_out, st_out, k_land, v_land, k_swap, v_swap,
                slopes, tok, lin_gain, out_gain, attn_gain, rope, wv_qkv, wv_gate, wv_lo, wv_in, wv_ao, st_buf, p_out, p_in, acc, relay_in, rs_in, sq_x, y_x, a_x, q_x, pr_out, pr_pair, pr_mine, pr_in,
                k_buf, v_buf, o_s, q_s, kn_s, vn_s, ho_s,
                go_sem, pair_sem, rs_sem, sq_sem, y_sem, a_sem, q_sem, pr_sem, kv_send, kv_recv, swap_sem):
    chips, tp_size, rows, heads, head_dim, kv_dev, group, shard_len = dims
    sp_size = 2 * chips
    pairs = heads // 2
    width = heads * head_dim
    model = tok_in.shape[1]
    hidden_width = tp_size * width
    segments = group + 2
    qrows = kv_dev * group * rows

    me = lax.axis_index("sp")
    me_tp = lax.axis_index("tp")
    chip = me // 2
    core = lax.rem(me, 2)
    steps = (2, 1, 3)

    def same_core(dc):
        return lax.rem(chip + dc, chips) * 2 + core

    barrier = pltpu.get_barrier_semaphore()
    for dc in steps:
        pl.semaphore_signal(barrier, inc=1, device_id={"sp": same_core(dc)}, device_id_type=MESH)
    pl.semaphore_signal(barrier, inc=1, device_id={"sp": chip * 2 + (1 - core)}, device_id_type=MESH)

    @pl.when(me_tp == 0)
    def _():
        pl.semaphore_wait(barrier, chips)
        for other in range(1, tp_size):
            pl.semaphore_signal(barrier, inc=1, device_id={"tp": other}, device_id_type=MESH)

    @pl.when(me_tp != 0)
    def _():
        pl.semaphore_wait(barrier, chips + 1)
        pl.semaphore_signal(barrier, inc=1, device_id={"tp": 0}, device_id_type=MESH)

    def wait_for_tp():
        @pl.when(me_tp == 0)
        def _():
            pl.semaphore_wait(barrier, tp_size - 1)
            for other in range(1, tp_size):
                pl.semaphore_signal(go_sem, inc=1, device_id={"tp": other}, device_id_type=MESH)

        @pl.when(me_tp != 0)
        def _():
            pl.semaphore_wait(go_sem, 1)

    def remote(src, dst, send, recv, device):
        return pltpu.make_async_remote_copy(src_ref=src, dst_ref=dst, send_sem=send, recv_sem=recv, device_id=device, device_id_type=MESH)

    partner = {"sp": chip * 2 + (1 - core)}
    my_cols = pl.ds(pl.multiple_of(me * shard_len, LANES), shard_len)

    partner_cols = pl.ds(pl.multiple_of((chip * 2 + (1 - core)) * shard_len, LANES), shard_len)

    def start_round(round_idx, own):
        which, row = ((0, 0), (1, 0), (0, 1), (1, 1), (1, 2), (1, 3), (0, 2))[round_idx]
        cache, swap, land = ((k_in, k_swap, k_land), (v_in, v_swap, v_land))[which]
        for dc in steps:
            dst = same_core(dc)
            src, cols = (cache.at[dst * rows + row], my_cols) if own else (swap.at[lax.rem(chip + dc, chips) * rows + row], partner_cols)
            remote(src, land.at[row, :, :, cols], kv_send.at[which], kv_recv.at[which], {"sp": dst}).start()

    def total_of(ref, sems):
        return remote(ref, ref, sems[0], sems[1], partner)

    start_round(0, True)
    for cache, swap, n in ((k_in, k_swap, 0), (v_in, v_swap, 1)):
        for block in range(chips):
            src = cache.at[pl.ds((block * 2 + (1 - core)) * rows, rows)]
            remote(src, swap.at[pl.ds(block * rows, rows)], swap_sem.at[2 * n], swap_sem.at[2 * n + 1], partner).start()
    start_round(1, True)

    def decode_step(in_sem, w_sem, st_sem, own_sem, kb_sem):
        def state_copy(step, slot):
            target_core = jnp.where(step < chips, 1 - core, core)
            dest = lax.rem(step, chips) * 2 + target_core
            return pltpu.make_async_copy(states.at[0, pl.ds(dest * rows, rows)], st_buf.at[slot], st_sem.at[slot])

        slope_copy = pltpu.make_async_copy(slopes_in, slopes, in_sem.at[5])
        slope_copy.start()
        state_copy(0, 0).start()
        small_copies = [pltpu.make_async_copy(src, dst, in_sem.at[n]) for n, (src, dst) in enumerate(
            ((tok_in, tok), (lin_gain_in, lin_gain), (out_gain_in, out_gain), (attn_gain_in, attn_gain), (rope_in, rope)))]
        for copy in small_copies:
            copy.start()
        weight_copies = [pltpu.make_async_copy(src, dst, w_sem.at[n]) for n, (src, dst) in enumerate(
            ((w_qkv, wv_qkv), (w_gate, wv_gate), (w_lo, wv_lo), (w_in, wv_in), (w_ao, wv_ao)))]
        for copy in weight_copies:
            copy.start()

        lane = lax.broadcasted_iota(jnp.int32, (1, LANES), 1)
        low_half = lane < head_dim

        def pair_slope(p):
            return jnp.where(low_half, jnp.full((1, LANES), slopes[2 * p], F32), jnp.full((1, LANES), slopes[2 * p + 1], F32))

        slope_copy.wait()
        offset = (shard_len * (sp_size - 1 - me)).astype(F32)
        decay = [jnp.exp(-pair_slope(p) * offset) for p in range(pairs)]

        def weigh_step(step, target):
            slot = lax.rem(step, 2)

            @pl.when(step + 1 < 2 * chips)
            def _():
                state_copy(step + 1, lax.rem(step + 1, 2)).start()

            state_copy(step, slot).wait()
            block = lax.rem(step, chips)
            for b in range(rows):
                for p in range(pairs):
                    packed = jnp.concatenate([st_buf[slot, b, 2 * p], st_buf[slot, b, 2 * p + 1]], axis=1)
                    target[block, b, p] = packed * decay[p]

        @pl.loop(0, chips)
        def _(step):
            weigh_step(step, p_out)

        pair_copy = remote(p_out, p_in, pair_sem.at[0], pair_sem.at[1], partner)
        pair_copy.start()

        @pl.loop(chips, 2 * chips)
        def _(step):
            weigh_step(step, acc)

        own_copies = [pltpu.make_async_copy(cache.at[pl.ds(me * rows, rows)], land.at[:, :, :, my_cols], own_sem.at[n])
                      for n, (cache, land) in enumerate(((k_in, k_land), (v_in, v_land)))]
        for copy in own_copies:
            copy.start()
        for n, swap in enumerate((k_swap, v_swap)):
            total_of(swap, (swap_sem.at[2 * n], swap_sem.at[2 * n + 1])).wait()
        partner_copies = [pltpu.make_async_copy(swap.at[pl.ds(chip * rows, rows)], land.at[:, :, :, partner_cols], own_sem.at[2 + n])
                          for n, (swap, land) in enumerate(((k_swap, k_land), (v_swap, v_land)))]
        for copy in partner_copies:
            copy.start()
        start_round(0, False)

        pair_copy.wait()

        @pl.loop(0, chips)
        def _(block):
            for b in range(rows):
                acc[block, b] = acc[block, b] + p_in[block, b]

        nexts = [(lax.rem(chip + dc, chips), {"sp": lax.rem(chip + dc, chips) * 2 + core}) for dc in (1, chips - 1)]
        far = lax.rem(chip + 2, chips)
        half = rows // 2
        parts = [pl.ds(0, half), pl.ds(half, half)]

        def rs_copy(n, src, dst, side):
            return remote(src, dst, rs_sem.at[n], rs_sem.at[n + 1], nexts[side][1])

        relay_copies = [rs_copy(0, acc.at[far, parts[side]], relay_in.at[side], side) for side in range(2)]
        rs_copies = [rs_copy(2, acc.at[nexts[side][0], parts[1 - side]], rs_in.at[side, parts[1 - side]], side) for side in range(2)]
        for copy in relay_copies + rs_copies:
            copy.start()
        start_round(1, False)

        def rms(vals):
            return vals * lax.rsqrt(jnp.mean(vals * vals, axis=-1, keepdims=True) + NORM_EPS)

        pad_rows = 8 - rows

        def pad8(vals):
            return jnp.concatenate([vals, jnp.zeros((pad_rows,) + vals.shape[1:], vals.dtype)], axis=0) if pad_rows else vals

        for copy in small_copies:
            copy.wait()
        tokens = pad8(tok[...].astype(F32))
        normed = (rms(tokens) * lin_gain[...]).astype(BF16)
        weight_copies[0].wait()

        def act(n):
            lin = jnp.dot(normed, wv_qkv[n], preferred_element_type=F32)
            return (lin * jax.nn.sigmoid(lin)).astype(BF16).astype(F32)

        query, key, value = act(0), act(1), act(2)
        weight_copies[1].wait()
        gate = jax.nn.sigmoid(jnp.dot(normed, wv_gate[...], preferred_element_type=F32))
        query_t = jnp.transpose(query)
        key_t = jnp.transpose(key)
        total_of(relay_in, (rs_sem.at[0], rs_sem.at[1])).wait()
        for side in range(2):
            block = nexts[side][0]
            for b in range(half):
                acc[block, side * half + b] = acc[block, side * half + b] + relay_in[side, b]
            rs_copy(2, acc.at[block, parts[side]], rs_in.at[side, parts[side]], side).start()
        start_round(2, True)
        start_round(2, False)
        o_s[...] = jnp.zeros_like(o_s)

        def column(cols, p, b):
            lo = cols[2 * p * head_dim:(2 * p + 1) * head_dim, b:b + 1]
            hi = cols[(2 * p + 1) * head_dim:(2 * p + 2) * head_dim, b:b + 1]
            return jnp.where(low_half, lo, hi)

        total_of(rs_in, (rs_sem.at[2], rs_sem.at[3])).wait()

        for p in range(pairs):
            lam = jnp.exp(-pair_slope(p))
            cols = slice(p * LANES, (p + 1) * LANES)
            for b in range(rows):
                moved = acc[chip, b, p] + rs_in[0, b, p] + rs_in[1, b, p]
                state = lam * moved + column(key_t, p, b) * value[b:b + 1, cols]
                o_s[b:b + 1, cols] = jnp.sum(column(query_t, p, b) * state, axis=0, keepdims=True)
                st_out[b, 2 * p] = state[:, :head_dim]
                st_out[b, 2 * p + 1] = state[:, head_dim:]

        def tp_sum(buf, vals, sems):
            buf[me_tp] = vals
            copies = []
            for dt in (2, 1, 3)[-(tp_size - 1):]:
                copies.append(remote(buf.at[me_tp], buf.at[me_tp], sems.at[0], sems.at[1], {"tp": lax.rem(me_tp + dt, tp_size)}))
            for copy in copies:
                copy.start()
            total_of(buf.at[pl.ds(0, len(copies))], (sems.at[0], sems.at[1])).wait()
            total = buf[0]
            for n in range(1, tp_size):
                total = total + buf[n]
            return total

        wait_for_tp()
        lin_attn = o_s[...]
        squares = jnp.broadcast_to(jnp.sum(lin_attn * lin_attn, axis=-1, keepdims=True), (8, LANES))
        square_sum = tp_sum(sq_x, squares, sq_sem)[:, :1]
        mixed = (lin_attn * lax.rsqrt(square_sum / hidden_width + NORM_EPS) * out_gain[...] * gate).astype(BF16)
        weight_copies[2].wait()
        lin_out = tp_sum(y_x, jnp.dot(mixed, wv_lo[...], preferred_element_type=F32), y_sem)
        hidden = (normed.astype(F32) + lin_out).astype(BF16).astype(F32)
        normed_two = (rms(hidden) * attn_gain[...]).astype(BF16)

        weight_copies[3].wait()
        proj = lax.dot_general(normed_two, wv_in[...], NT, preferred_element_type=F32).astype(BF16).astype(F32)
        cols_in = proj.shape[1]
        quarter = head_dim // 4
        rotated = proj * rope[0:1, :] + pltpu.roll(proj, quarter, 1) * rope[1:2, :] + pltpu.roll(proj, cols_in - quarter, 1) * rope[2:3, :]
        rotated = rotated.astype(BF16).astype(F32)

        def segment_at(kv, segment):
            start = (kv * segments + segment) * head_dim
            block = rotated[:, start // LANES * LANES:start // LANES * LANES + LANES]
            if start % LANES != kv * head_dim:
                block = pltpu.roll(block, head_dim, 1)
            return jnp.where(low_half if kv == 0 else ~low_half, block, 0.0)

        def packed_at(segment):
            return (segment_at(0, segment) + segment_at(1, segment))[:rows]

        key_rows, value_rows = packed_at(group), packed_at(group + 1)
        for i in range(group):
            q_s[i * rows:(i + 1) * rows, :] = packed_at(i)
            kn_s[i * rows:(i + 1) * rows, :] = key_rows
            vn_s[i * rows:(i + 1) * rows, :] = value_rows

        def spread(vals):
            return jnp.concatenate([jnp.where(low_half, vals, 0.0), jnp.where(low_half, 0.0, vals)], axis=0)

        q_x[me] = q_s[...].astype(BF16)
        for dc in steps:
            remote(q_x.at[me], q_x.at[me], q_sem.at[0], q_sem.at[1], {"sp": same_core(dc)}).start()
        remote(q_x.at[me], q_x.at[me], q_sem.at[2], q_sem.at[3], partner).start()
        for own in (True, False):
            start_round(3, own)
        for own in (True, False):
            start_round(4, own)

        def shard_copies(j, slot):
            return [pltpu.make_async_copy(cache.at[pl.ds(j * rows, rows)], buf.at[slot], kb_sem.at[n, slot])
                    for n, (cache, buf) in enumerate(((k_in, k_buf), (v_in, v_buf)))]

        for copy in shard_copies(0, 0):
            copy.start()

        rotated_t = jnp.transpose(rotated)
        lane16 = lax.broadcasted_iota(jnp.int32, (1, CACHE_EXTRA), 1)
        prompt_len = sp_size * shard_len
        for land, segment in ((k_land, group), (v_land, group + 1)):
            for kv in range(kv_dev):
                start = (kv * segments + segment) * head_dim
                for b in range(rows):
                    tail = jnp.where(lane16 == 0, rotated_t[start:start + head_dim, b:b + 1], 0.0)
                    land[b, kv, :, prompt_len:] = tail.astype(BF16)

        row_id = lax.broadcasted_iota(jnp.int32, (qrows, 1), 0)
        row_seq = lax.rem(row_id, rows)
        split = group * rows
        scale = head_dim ** -0.5

        total_of(q_x.at[pl.ds(0, chips - 1)], (q_sem.at[0], q_sem.at[1])).wait()
        for dc in (2, 1, 3):
            src = same_core(dc)
            remote(q_x.at[src], q_x.at[src], q_sem.at[2], q_sem.at[3], partner).start()
        total_of(q_x.at[pl.ds(0, chips)], (q_sem.at[2], q_sem.at[3])).wait()

        def write_partial(ref, out, peak, total):
            ref[:split] = out
            stats = jnp.transpose(jnp.where(low_half, peak, total))
            stats = jnp.concatenate([stats[:4], stats[head_dim:head_dim + 4]], axis=0)
            ref[split:] = jnp.concatenate([stats, jnp.zeros((8, LANES - qrows), F32)], axis=1)

        def read_partial(ref):
            stats = jnp.transpose(ref[split:])
            return ref[:split], stats[:qrows, 0:1], stats[:qrows, 4:5]

        def both_heads(column_vals):
            return jnp.where(low_half, column_vals[:split], column_vals[split:])

        @pl.loop(0, sp_size)
        def _(j):
            slot = lax.rem(j, 2)

            @pl.when(j + 1 < sp_size)
            def _():
                for copy in shard_copies(j + 1, lax.rem(j + 1, 2)):
                    copy.start()

            for copy in shard_copies(j, slot):
                copy.wait()
            queries = spread(q_x[j].astype(F32)).astype(BF16)
            scores = jnp.zeros((qrows, shard_len), F32)
            for b in range(rows):
                keys = k_buf[slot, b].reshape(kv_dev * head_dim, shard_len)
                scores = jnp.where(row_seq == b, jnp.dot(queries, keys, preferred_element_type=F32), scores)
            scores = scores * scale
            peak = jnp.max(scores, axis=-1, keepdims=True)
            probs = jnp.exp(scores - peak)
            total = jnp.sum(probs, axis=-1, keepdims=True)
            probs = probs.astype(BF16)
            out = jnp.zeros((qrows, LANES), F32)
            for b in range(rows):
                vals = v_buf[slot, b].reshape(kv_dev * head_dim, shard_len)
                out = jnp.where(row_seq == b, lax.dot_general(probs, vals, NT, preferred_element_type=F32), out)
            write_partial(pr_out.at[lax.rem(j, 2), j // 2], both_heads(out), peak, total)

        pr_swap = remote(pr_out.at[1 - core], pr_pair, pr_sem.at[0], pr_sem.at[1], partner)
        pr_swap.start()
        pr_swap.wait()

        @pl.loop(0, chips)
        def _(block):
            out_a, peak_a, total_a = read_partial(pr_out.at[core, block])
            out_b, peak_b, total_b = read_partial(pr_pair.at[block])
            peak = jnp.maximum(peak_a, peak_b)
            scale_a, scale_b = jnp.exp(peak_a - peak), jnp.exp(peak_b - peak)
            write_partial(pr_mine.at[block], out_a * both_heads(scale_a) + out_b * both_heads(scale_b), peak, total_a * scale_a + total_b * scale_b)

        for dc in (2, 1, 3):
            dst_chip = lax.rem(chip + dc, chips)
            remote(pr_mine.at[dst_chip], pr_in.at[chip], pr_sem.at[2], pr_sem.at[3], {"sp": dst_chip * 2 + core}).start()
        for own in (True, False):
            start_round(5, own)

        @pl.when(core == 1)
        def _():
            for own in (True, False):
                start_round(6, own)

        pr_in[chip] = pr_mine[chip]

        new_score = jnp.sum(spread(q_s[...] * kn_s[...]), axis=-1, keepdims=True) * scale

        total_of(pr_in.at[pl.ds(0, chips - 1)], (pr_sem.at[2], pr_sem.at[3])).wait()
        partials = [read_partial(pr_in.at[n]) for n in range(chips)]
        top = new_score
        for _, peak, _ in partials:
            top = jnp.maximum(top, peak)
        new_prob = jnp.exp(new_score - top)
        prob_sum = new_prob
        head = new_prob.astype(BF16).astype(F32) * spread(vn_s[...])
        for out, peak, total in partials:
            weight = jnp.exp(peak - top)
            prob_sum = prob_sum + weight * total
            head = head + weight * spread(out)
        head = (head / prob_sum).astype(BF16).astype(F32)

        ho_s[...] = jnp.zeros_like(ho_s)
        for n in range(0, kv_dev * group, 2):
            block = None
            for m in (n, n + 1):
                kv = m // group
                piece = head[m * rows:(m + 1) * rows]
                if kv != m % 2:
                    piece = pltpu.roll(piece, head_dim, 1)
                block = piece if block is None else block + piece
            ho_s[0:rows, n // 2 * LANES:(n // 2 + 1) * LANES] = block
        weight_copies[4].wait()
        attn_out = tp_sum(a_x, jnp.dot(ho_s[...].astype(BF16), wv_ao[...], preferred_element_type=F32), a_sem)
        hid_out[...] = (normed_two.astype(F32) + attn_out).astype(BF16)[:rows]

        for copy in own_copies:
            copy.wait()
        for copy in partner_copies:
            copy.wait()
        blocks = 2 * (chips - 1)
        total_of(v_in.at[pl.ds(0, blocks * rows)], (kv_send.at[1], kv_recv.at[1])).wait()

        @pl.when(core == 0)
        def _():
            total_of(k_in.at[pl.ds(0, blocks * (rows - 2))], (kv_send.at[0], kv_recv.at[0])).wait()

        @pl.when(core == 1)
        def _():
            total_of(k_in.at[pl.ds(0, blocks * (rows - 1))], (kv_send.at[0], kv_recv.at[0])).wait()

    dma = pltpu.SemaphoreType.DMA
    pl.run_scoped(decode_step, dma((6,)), dma((5,)), dma((2,)), dma((4,)), dma((2, 2)))


def last_kernel(dims, k_in, k_swap, _, k_last, k_send, k_recv, own_sem):
    chips, _, rows, _, _, _, _, shard_len = dims
    me = lax.axis_index("sp")
    chip = me // 2
    core = lax.rem(me, 2)

    def same_core(dc):
        return lax.rem(chip + dc, chips) * 2 + core

    barrier = pltpu.get_barrier_semaphore()
    for dc in (2, 1, 3):
        pl.semaphore_signal(barrier, inc=1, device_id={"sp": same_core(dc)}, device_id_type=MESH)
    pl.semaphore_wait(barrier, chips - 1)
    my_cols = pl.ds(pl.multiple_of(me * shard_len, LANES), shard_len)
    partner_cols = pl.ds(pl.multiple_of((chip * 2 + (1 - core)) * shard_len, LANES), shard_len)

    def move(count):
        def block(ref, index):
            return ref.at[pl.ds(index * rows + rows - count, count)]

        def remote(src, dst, device):
            return pltpu.make_async_remote_copy(src_ref=src, dst_ref=dst, send_sem=k_send, recv_sem=k_recv, device_id={"sp": device}, device_id_type=MESH)

        mine, partners = [k_last.at[pl.ds(2 - count, count), :, :, cols] for cols in (my_cols, partner_cols)]
        for piece in range(count):
            for dc, own in ((2, True), (1, True), (3, True), (2, False), (1, False), (3, False)):
                dst = same_core(dc)
                src = block(k_in, dst) if own else block(k_swap, lax.rem(chip + dc, chips))
                remote(src.at[piece], (mine if own else partners).at[piece], dst).start()
        own_copies = [pltpu.make_async_copy(block(k_in, me), mine, own_sem.at[0]), pltpu.make_async_copy(block(k_swap, chip), partners, own_sem.at[1])]
        for copy in own_copies:
            copy.start()
        for copy in own_copies:
            copy.wait()
        total = k_in.at[pl.ds(0, 2 * (chips - 1) * count)]
        remote(total, total, same_core(1)).wait()

    @pl.when(core == 0)
    def _():
        move(2)

    @pl.when(core == 1)
    def _():
        move(1)


def put_kernel(hid, st, k_land, v_land, hid_dst, st_dst, k_dst, v_dst, sems):
    rows, _, _, full_len = k_land.shape
    tail = pl.ds(full_len - CACHE_EXTRA, CACHE_EXTRA)
    core = lax.rem(lax.axis_index("sp"), 2)
    pairs = [(v_land.at[row], v_dst.at[row]) for row in range(rows)] + [(k_land.at[row], k_dst.at[row]) for row in range(rows - 2)]
    pairs += [(st, st_dst), (hid, hid_dst), (k_land.at[rows - 1, :, :, tail], k_dst.at[rows - 1, :, :, tail])]
    copies = [pltpu.make_async_copy(src, dst, sems.at[n]) for n, (src, dst) in enumerate(pairs)]
    for copy in copies:
        copy.start()
    row = rows - 2
    whole = pltpu.make_async_copy(k_land.at[row], k_dst.at[row], sems.at[len(copies)])
    part = pltpu.make_async_copy(k_land.at[row, :, :, tail], k_dst.at[row, :, :, tail], sems.at[len(copies)])

    @pl.when(core == 0)
    def _():
        part.start()
        part.wait()

    @pl.when(core == 1)
    def _():
        whole.start()
        whole.wait()

    for copy in copies:
        copy.wait()


def put_last_kernel(k_first, k_last, k_dst, sems):
    rows = k_dst.shape[0]
    cols = pl.ds(0, k_last.shape[-1])
    core = lax.rem(lax.axis_index("sp"), 2)
    last = pltpu.make_async_copy(k_last.at[1], k_dst.at[rows - 1, :, :, cols], sems.at[0])
    other = pltpu.make_async_copy(k_last.at[0], k_dst.at[rows - 2, :, :, cols], sems.at[1])
    last.start()

    @pl.when(core == 0)
    def _():
        other.start()
        other.wait()

    last.wait()


def solution(mesh):
    sp_size = mesh.shape['sp']
    tp_size = mesh.shape['tp']
    chips = sp_size // 2

    def device_step(tokens, states, k_cache, v_cache, slopes, lin_gain, w_lin_qkv, w_lin_gate, out_gain, w_lin_out, attn_gain, w_attn_in, w_attn_out):
        rows, model = tokens.shape
        kv_dev, shard_len, head_dim = k_cache.shape[1:]
        heads = slopes.shape[0]
        segments = w_attn_in.shape[2]
        group = segments - 2
        width = heads * head_dim
        pairs = heads // 2
        cols_in = kv_dev * segments * head_dim
        qrows = kv_dev * group * rows
        prompt_len = sp_size * shard_len
        full_len = prompt_len + CACHE_EXTRA
        dims = (chips, tp_size, rows, heads, head_dim, kv_dev, group, shard_len)
        rope = jnp.asarray(rope_tables(kv_dev, segments, group, head_dim, prompt_len))

        vmem = pl.BlockSpec(memory_space=pltpu.VMEM)
        anym = pl.BlockSpec(memory_space=pl.ANY)
        hbm = pl.BlockSpec(memory_space=pltpu.HBM)
        dma = pltpu.SemaphoreType.DMA

        def in_hbm(*arrays):
            return [pltpu.with_memory_space_constraint(array, pltpu.HBM) for array in arrays]

        land_shape = (rows, kv_dev, head_dim, full_len)
        out_types = [((rows, model), BF16), ((rows, heads, head_dim, head_dim), F32), (land_shape, BF16), (land_shape, BF16)]
        scratch = [
            pltpu.SMEM((heads,), F32),
            pltpu.VMEM((rows, model), BF16),
            pltpu.VMEM((1, model), F32),
            pltpu.VMEM((1, width), F32),
            pltpu.VMEM((1, model), F32),
            pltpu.VMEM((8, cols_in), F32),
            pltpu.VMEM((3, model, width), BF16),
            pltpu.VMEM((model, width), BF16),
            pltpu.VMEM((width, model), BF16),
            pltpu.VMEM((cols_in, model), BF16),
            pltpu.VMEM((width, model), BF16),
            pltpu.VMEM((2, rows, heads, head_dim, head_dim), F32),
            pltpu.VMEM((chips, rows, pairs, head_dim, LANES), F32),
            pltpu.VMEM((chips, rows, pairs, head_dim, LANES), F32),
            pltpu.VMEM((chips, rows, pairs, head_dim, LANES), F32),
            pltpu.VMEM((2, rows // 2, pairs, head_dim, LANES), F32),
            pltpu.VMEM((2, rows, pairs, head_dim, LANES), F32),
            pltpu.VMEM((tp_size, 8, LANES), F32),
            pltpu.VMEM((tp_size, 8, model), F32),
            pltpu.VMEM((tp_size, 8, model), F32),
            pltpu.VMEM((sp_size, group * rows, LANES), BF16),
            pltpu.VMEM((2, chips, group * rows + 8, LANES), F32),
            pltpu.VMEM((chips, group * rows + 8, LANES), F32),
            pltpu.VMEM((chips, group * rows + 8, LANES), F32),
            pltpu.VMEM((chips, group * rows + 8, LANES), F32),
            pltpu.VMEM((2, rows, kv_dev, head_dim, shard_len), BF16),
            pltpu.VMEM((2, rows, kv_dev, head_dim, shard_len), BF16),
            pltpu.VMEM((8, width), F32),
            pltpu.VMEM((group * rows, LANES), F32),
            pltpu.VMEM((group * rows, LANES), F32),
            pltpu.VMEM((group * rows, LANES), F32),
            pltpu.VMEM((8, width), F32),
            pltpu.SemaphoreType.REGULAR,
            dma((2,)),
            dma((4,)),
            dma((2,)),
            dma((2,)),
            dma((2,)),
            dma((4,)),
            dma((4,)),
            dma((2,)),
            dma((2,)),
            dma((4,)),
        ]
        k_cols, v_cols = jnp.transpose(k_cache, (0, 1, 3, 2)), jnp.transpose(v_cache, (0, 1, 3, 2))
        swap_type = jax.ShapeDtypeStruct((chips * rows, kv_dev, head_dim, shard_len), BF16)
        *landed, k_swap, v_swap = pl.pallas_call(
            functools.partial(step_kernel, dims),
            out_shape=[pltpu.VMEM(shape, dtype) for shape, dtype in out_types] + [swap_type] * 2,
            in_specs=[anym, anym, anym, anym, anym, anym] + [anym] * 8,
            out_specs=[vmem] * 4 + [anym] * 2,
            scratch_shapes=scratch,
            compiler_params=pltpu.CompilerParams(collective_id=0, has_side_effects=True, vmem_limit_bytes=40 * 2 ** 20),
        )(
            tokens, slopes, lin_gain.reshape(1, -1), out_gain.reshape(1, -1), attn_gain.reshape(1, -1), rope,
            states, k_cols, v_cols,
            jnp.transpose(w_lin_qkv, (1, 0, 2)), w_lin_gate, w_lin_out,
            jnp.transpose(w_attn_in, (1, 2, 3, 0)).reshape(cols_in, model), w_attn_out,
        )
        hidden_out, state_new, k_out, v_out = pl.pallas_call(
            put_kernel,
            out_shape=[jax.ShapeDtypeStruct(shape, dtype) for shape, dtype in out_types],
            in_specs=[vmem] * 4,
            out_specs=[anym] * 4,
            scratch_shapes=[dma((2 * rows + 2,))],
            compiler_params=pltpu.CompilerParams(vmem_limit_bytes=2 * 2 ** 20),
        )(*landed)
        last_rows = pl.pallas_call(
            functools.partial(last_kernel, dims),
            out_shape=pltpu.VMEM((2, kv_dev, head_dim, prompt_len), BF16),
            in_specs=[hbm] * 3,
            out_specs=vmem,
            scratch_shapes=[dma, dma, dma((2,))],
            compiler_params=pltpu.CompilerParams(collective_id=1, has_side_effects=True, vmem_limit_bytes=2 * 2 ** 20),
        )(*in_hbm(k_cols, k_swap, hidden_out))
        k_out = pl.pallas_call(
            put_last_kernel,
            out_shape=jax.ShapeDtypeStruct(land_shape, BF16),
            in_specs=[hbm, vmem],
            out_specs=hbm,
            scratch_shapes=[dma((2,))],
            input_output_aliases={0: 0},
            compiler_params=pltpu.CompilerParams(vmem_limit_bytes=2 * 2 ** 20),
        )(*in_hbm(k_out), last_rows)
        return hidden_out, state_new, jnp.transpose(k_out, (0, 1, 3, 2)), jnp.transpose(v_out, (0, 1, 3, 2))

    batch_spec = P(('dp', 'sp'), None)
    head_spec = P(('dp', 'sp'), 'tp', None, None)
    cache_spec = P('dp', 'tp', 'sp', None)
    in_specs = (batch_spec, P('sp', 'dp', 'tp', None, None), cache_spec, cache_spec, P('tp'), P(None), P(None, None, 'tp'), P(None, 'tp'), P('tp'), P('tp', None), P(None), P(None, 'tp', None, None), P('tp', None))
    out_specs = (batch_spec, head_spec, head_spec, head_spec)
    return jax.shard_map(device_step, mesh=mesh, in_specs=in_specs, out_specs=out_specs, check_vma=False)
```
